8 devices in a mesh: dp: 2 (over z, y), cp: 4 (over x, core).
Axes of the slice: x: 2, y: 2, z: 1, core: 2. Of those that a mesh axis runs over, the one named last changes fastest.
Arguments:
- queries: bfloat16 [128, 128, 128], P(('dp', 'cp')), parts along dimension 0
- key_new: bfloat16 [128, 8, 128], P(('dp', 'cp')), parts along dimension 0
- value_new: bfloat16 [128, 8, 128], P(('dp', 'cp')), parts along dimension 0
- key_cache: bfloat16 [24576, 8, 128], P(('dp', 'cp')), parts along dimension 0
- value_cache: bfloat16 [24576, 8, 128], P(('dp', 'cp')), parts along dimension 0
- prefix_len: int32 [2], P('dp'), parts along dimension 0
Outputs:
- output 1: bfloat16 [128, 128, 128], P(('dp', 'cp')), parts along dimension 0
- output 2: float32 [128, 128], P(('dp', 'cp')), parts along dimension 0
There are 2 independent parts. The reference program is written for one: setup_inputs(seed, part) draws one part's arguments, and reference() takes and returns one part's arrays. A program takes and returns all parts, laid end to end along the dimension named above; each array names one.
All inputs are finite; a program needn't handle non-finite values.
Results may differ from the reference program's by a relative error of at most 0.00879912.
Values are sent between devices in bfloat16 or wider.
A program may use at most 1 GiB of HBM per device.

```python
import math
import jax
import jax.numpy as jnp
from jax import lax

GROUP_SIZE = 4
NEW_DEV = 16
PREFIX_DEV = 3072
Q_HEADS = 128
KV_HEADS = 8
HEAD_DIM = 128
NEW_LEN = GROUP_SIZE * NEW_DEV
P_MAX = GROUP_SIZE * PREFIX_DEV
GROUP_RATIO = Q_HEADS // KV_HEADS


def setup_inputs(seed: int = 0, part: int = 0) -> dict:
    base_key = jax.random.fold_in(jax.random.key(seed), part)
    rand_keys = jax.random.split(base_key, 9)
    shift_scale = GROUP_SIZE ** 0.5
    new_boost = math.log(P_MAX / NEW_LEN) * 2.0 ** 0.5
    direction = jax.random.normal(rand_keys[0], (KV_HEADS, HEAD_DIM), jnp.float32)
    direction = direction / jnp.linalg.norm(direction, axis=-1, keepdims=True)
    q_mean = jnp.repeat(direction, GROUP_RATIO, axis=0) * HEAD_DIM ** 0.5
    q_noise = jax.random.normal(rand_keys[1], (NEW_LEN, Q_HEADS, HEAD_DIM), jnp.float32)
    queries = (q_noise + q_mean[None]) * 0.5 ** 0.5
    key_new = jax.random.normal(rand_keys[2], (NEW_LEN, KV_HEADS, HEAD_DIM), jnp.float32) + new_boost * direction[None]
    new_shift = jax.random.normal(rand_keys[3], (GROUP_SIZE, 1, KV_HEADS, HEAD_DIM), jnp.float32) * shift_scale
    value_new = jax.random.normal(rand_keys[4], (GROUP_SIZE, NEW_DEV, KV_HEADS, HEAD_DIM), jnp.float32) + new_shift
    key_cache = jax.random.normal(rand_keys[5], (P_MAX, KV_HEADS, HEAD_DIM), jnp.float32)
    cache_shift = jax.random.normal(rand_keys[6], (GROUP_SIZE, 1, KV_HEADS, HEAD_DIM), jnp.float32) * shift_scale
    value_cache = jax.random.normal(rand_keys[7], (GROUP_SIZE, PREFIX_DEV, KV_HEADS, HEAD_DIM), jnp.float32) + cache_shift
    prefix_len = jax.random.randint(rand_keys[8], (1,), (3 * P_MAX) // 4, P_MAX + 1, jnp.int32)
    return {
        'queries': queries.astype(jnp.bfloat16),
        'key_new': key_new.astype(jnp.bfloat16),
        'value_new': value_new.reshape(NEW_LEN, KV_HEADS, HEAD_DIM).astype(jnp.bfloat16),
        'key_cache': key_cache.astype(jnp.bfloat16),
        'value_cache': value_cache.reshape(P_MAX, KV_HEADS, HEAD_DIM).astype(jnp.bfloat16),
        'prefix_len': prefix_len,
    }


def reference(queries, key_new, value_new, key_cache, value_cache, prefix_len):
    prefix_end = prefix_len[0]
    key_pos = jnp.arange(P_MAX + NEW_LEN)
    logit_scale = HEAD_DIM ** -0.5

    def one_head(head_idx):
        kv_idx = head_idx // GROUP_RATIO
        keys_all = jnp.concatenate([lax.dynamic_index_in_dim(key_cache, kv_idx, axis=1, keepdims=False), lax.dynamic_index_in_dim(key_new, kv_idx, axis=1, keepdims=False)], axis=0).astype(jnp.float32)
        vals_all = jnp.concatenate([lax.dynamic_index_in_dim(value_cache, kv_idx, axis=1, keepdims=False), lax.dynamic_index_in_dim(value_new, kv_idx, axis=1, keepdims=False)], axis=0).astype(jnp.float32)
        q_head = lax.dynamic_index_in_dim(queries, head_idx, axis=1, keepdims=False).astype(jnp.float32).reshape(GROUP_SIZE, NEW_DEV, HEAD_DIM)

        def one_block(block_args):
            q_rows, row_start = block_args
            scores = jnp.dot(q_rows, keys_all.T) * logit_scale
            q_pos = row_start + jnp.arange(NEW_DEV)
            visible = jnp.where(key_pos[None, :] < P_MAX, key_pos[None, :] < prefix_end, key_pos[None, :] - P_MAX <= q_pos[:, None])
            scores = jnp.where(visible, scores, -jnp.inf)
            row_max = jnp.max(scores, axis=-1)
            exp_scores = jnp.exp(scores - row_max[:, None])
            row_sum = jnp.sum(exp_scores, axis=-1)
            prob_bf = exp_scores.astype(jnp.bfloat16).astype(jnp.float32)
            block_out = jnp.dot(prob_bf, vals_all) / row_sum[:, None]
            return block_out.astype(jnp.bfloat16), row_max + jnp.log(row_sum)

        head_out, head_lse = lax.map(one_block, (q_head, jnp.arange(GROUP_SIZE) * NEW_DEV))
        return head_out.reshape(NEW_LEN, HEAD_DIM), head_lse.reshape(NEW_LEN)

    all_out, all_lse = lax.map(one_head, jnp.arange(Q_HEADS))
    return jnp.transpose(all_out, (1, 0, 2)), jnp.transpose(all_lse)
```

```python
import functools
import math

import jax
import jax.numpy as jnp
from jax import lax
from jax.experimental import pallas as pl
from jax.experimental.pallas import tpu as pltpu
from jax.sharding import PartitionSpec as P

MESH = pl.DeviceIdType.MESH
BIG = 1e30
TK = 256
PREP = 128
BF = jnp.bfloat16
F32 = jnp.float32


def attend_kernel(q_hbm, kn_hbm, vn_hbm, kc_hbm, vc_hbm, plen_ref, out_hbm, lse_hbm,
                  raw_k, raw_v, new_k, new_v, kbuf, vbuf, bias, qraw, qt, s0, s1, m0, m1,
                  st_o, st_m, st_l, ps, psl, pr, prl, fo, fl,
                  raw_sem, new_sem, q_send, q_recv, kv_send, k_recv, v_recv, p_send, p_recv, f_send, f_recv):
    tok, kvh, ratio, dim = q_hbm.shape
    cache = kc_hbm.shape[0] // kvh
    half = kvh // 2
    rows = tok * ratio
    n_raw = raw_sem.shape[1]
    raw_pos = cache // n_raw
    chunks = cache // TK
    scale2 = dim ** -0.5 * math.log2(math.e)

    me = lax.axis_index('cp')
    core = lax.rem(me, 2)
    chip2 = me - core
    mate = chip2 + 1 - core
    far = lax.rem(chip2 + 2, 4) + core
    far_other = lax.rem(chip2 + 2, 4) + 1 - core

    def raw_copy(j):
        sl = pl.ds(j * raw_pos * kvh, raw_pos * kvh)
        return (pltpu.make_async_copy(kc_hbm.at[sl], raw_k.at[sl], raw_sem.at[0, j]),
                pltpu.make_async_copy(vc_hbm.at[sl], raw_v.at[sl], raw_sem.at[1, j]))

    def own_q(h):
        return pltpu.make_async_copy(q_hbm.at[:, half * core + h], qraw.at[h], q_recv.at[h])

    for j in range(n_raw):
        a, b = raw_copy(j)
        a.start()
        b.start()
    new_copies = (pltpu.make_async_copy(kn_hbm, new_k, new_sem.at[0]),
                  pltpu.make_async_copy(vn_hbm, new_v, new_sem.at[1]))
    for cp in new_copies:
        cp.start()
    for h in range(half):
        own_q(h).start()

    barrier = pltpu.get_barrier_semaphore()
    for peer in (mate, far, far_other):
        pl.semaphore_signal(barrier, inc=1, device_id={'cp': peer}, device_id_type=MESH)

    ones_row = jnp.where(lax.broadcasted_iota(jnp.int32, (dim, rows), 0) == 0, 1.0, 0.0).astype(BF)

    @pl.loop(0, 4 * half)
    def _(j):
        qt[j, pl.ds(dim, dim), :] = ones_row
        st_o[j] = jnp.zeros((dim, rows), F32)
        st_m[j] = jnp.full((1, rows), -1e38, F32)
        st_l[j] = jnp.zeros((1, rows), F32)

    pl.semaphore_wait(barrier, 3)

    def q_copy(k, h):
        peer, base = ((far, 2 * half), (far_other, 3 * half), (mate, half))[k]
        peer_core = (core, 1 - core, 1 - core)[k]
        return pltpu.make_async_remote_copy(
            src_ref=q_hbm.at[:, half * peer_core + h], dst_ref=qraw.at[base + h],
            send_sem=q_send.at[k * half + h], recv_sem=q_recv.at[base + h],
            device_id={'cp': peer}, device_id_type=MESH)

    for k in range(3):
        for h in range(half):
            q_copy(k, h).start()

    visible_len = plen_ref[0]
    for f, owner in enumerate((me, mate)):
        @pl.loop(0, chunks)
        def _(j):
            lane = lax.broadcasted_iota(jnp.int32, (TK, dim), 1)
            pos = owner * cache + j * TK + lax.broadcasted_iota(jnp.int32, (TK, dim), 0)
            hidden = jnp.logical_and(lane == 0, pos >= visible_len)
            bias[f, pl.ds(pl.multiple_of(j * TK, TK), TK), :] = jnp.where(hidden, -BIG, 0.0).astype(BF)

    for cp in new_copies:
        cp.wait()
    kt = pltpu.einshape('phd->hpd', new_k[...].reshape(tok, kvh, dim))
    vt = pltpu.einshape('phd->hpd', new_v[...].reshape(tok, kvh, dim))
    for h in range(kvh):
        kbuf[h, pl.ds(cache, tok), :] = kt[h]
        vpad = jnp.concatenate([vt[h].astype(F32), jnp.zeros((dim - tok, dim), F32)], axis=0)
        vbuf[h, :, pl.ds(cache, dim)] = vpad.T.astype(BF)
    for j in range(n_raw):
        for cp in raw_copy(j):
            cp.wait()

        @pl.loop(0, raw_pos // PREP)
        def _(i):
            base = pl.multiple_of(j * raw_pos + i * PREP, PREP)
            src = pl.ds(pl.multiple_of(base * kvh, PREP * kvh), PREP * kvh)
            xk = pltpu.einshape('phd->hpd', raw_k[src, :].reshape(PREP, kvh, dim))
            xv = pltpu.einshape('phd->hpd', raw_v[src, :].reshape(PREP, kvh, dim))
            for h in range(kvh):
                kbuf[h, pl.ds(base, PREP), :] = xk[h]
                vbuf[h, :, pl.ds(base, PREP)] = xv[h].T

    def kv_copies(h):
        src = half * (1 - core) + h
        return tuple(
            pltpu.make_async_remote_copy(
                src_ref=buf.at[src], dst_ref=buf.at[kvh + h], send_sem=kv_send.at[w, h], recv_sem=recv.at[h],
                device_id={'cp': mate}, device_id_type=MESH)
            for w, (buf, recv) in enumerate(((kbuf, k_recv), (vbuf, v_recv))))

    for h in range(half):
        for cp in kv_copies(h):
            cp.start()

    def item(s):
        second = lax.div(s, 4 * half)
        slot = lax.rem(s + second * 2 * half, 4 * half)
        h = lax.rem(slot, half)
        kv = jnp.where(second == 1, kvh + h, half * core + h)
        owner = jnp.where(second == 1, mate, me)
        src = lax.div(slot, half)
        home = jnp.where(src == 0, me, jnp.where(src == 1, mate, jnp.where(src == 2, far, far_other)))
        return second, slot, kv, owner, home

    def load_q(slot):
        qt[slot, pl.ds(0, dim), :] = qraw[slot].reshape(rows, dim).T

    def qk_tile(kv, f, c, qv):
        sl = pl.ds(c * TK, TK)
        lhs = jnp.concatenate([kbuf[kv, sl, :], bias[f, sl, :]], axis=1)
        return jnp.dot(lhs, qv, preferred_element_type=F32)

    def qk_new(kv, owner, home, qv):
        lhs = jnp.concatenate([kbuf[kv, pl.ds(cache, tok), :], jnp.zeros((tok, dim), BF)], axis=1)
        st = jnp.dot(lhs, qv, preferred_element_type=F32)
        key = owner * tok + lax.broadcasted_iota(jnp.int32, (tok, rows), 0)
        query = home * tok + lax.broadcasted_iota(jnp.int32, (tok, rows), 1) // ratio
        return jnp.where(key <= query, st, -BIG)

    def fold_max(mx, st):
        t = jnp.max(st.reshape(st.shape[0] // 8, 8, rows), axis=0)
        return t if mx is None else jnp.maximum(mx, t)

    def first_scores():
        f, slot, kv, owner, home = item(0)
        qv = qt[slot]
        mx = None
        for c in range(chunks):
            st = qk_tile(kv, f, c, qv)
            s0[pl.ds(c * TK, TK), :] = st
            mx = fold_max(mx, st)
        st = qk_new(kv, owner, home, qv)
        s0[pl.ds(cache, tok), :] = st
        m0[...] = fold_max(mx, st)

    def step(s, sc, sn, mc, mn):
        nxt = lax.rem(s + 1, 8 * half)
        f_n, slot_n, kv_n, owner_n, home_n = item(nxt)
        _, slot, kv, _, _ = item(s)

        ahead = s + 2

        @pl.when(jnp.logical_and(ahead >= half, ahead < 4 * half))
        def _():
            pltpu.make_async_copy(qraw.at[ahead], qraw.at[ahead], q_recv.at[ahead]).wait()

        @pl.when(jnp.logical_and(nxt >= 4 * half, nxt < 5 * half))
        def _():
            h = nxt - 4 * half
            pltpu.make_async_copy(kbuf.at[kvh + h], kbuf.at[kvh + h], k_recv.at[h]).wait()
            pltpu.make_async_copy(vbuf.at[kvh + h], vbuf.at[kvh + h], v_recv.at[h]).wait()

        qv = qt[slot_n]
        m_old = st_m[slot]
        m = jnp.maximum(m_old, jnp.max(mc[...], axis=0, keepdims=True) * scale2)
        decay = jnp.exp2(m_old - m)
        mx = None
        l8 = jnp.zeros((8, rows), F32)
        o = None
        for c in range(chunks):
            sl = pl.ds(c * TK, TK)
            st = qk_tile(kv_n, f_n, c, qv)
            p = jnp.exp2(sc[sl, :] * scale2 - m)
            sn[sl, :] = st
            mx = fold_max(mx, st)
            l8 = l8 + jnp.sum(p.reshape(TK // 8, 8, rows), axis=0)
            t = jnp.dot(vbuf[kv, :, sl], p.astype(BF), preferred_element_type=F32)
            o = t if o is None else o + t
        st = qk_new(kv_n, owner_n, home_n, qv)
        sl = pl.ds(cache, tok)
        p = jnp.exp2(sc[sl, :] * scale2 - m)
        sn[sl, :] = st
        mn[...] = fold_max(mx, st)
        l8 = l8 + jnp.sum(p.reshape(tok // 8, 8, rows), axis=0)
        pb = jnp.concatenate([p.astype(BF), jnp.zeros((dim - tok, rows), BF)], axis=0)
        o = o + jnp.dot(vbuf[kv, :, pl.ds(cache, dim)], pb, preferred_element_type=F32)
        st_o[slot] = st_o[slot] * decay + o
        st_l[slot] = st_l[slot] * decay + jnp.sum(l8, axis=0, keepdims=True)
        st_m[slot] = m
        load_q(jnp.minimum(ahead, 4 * half - 1))

    def partial_copies(u):
        return (pltpu.make_async_remote_copy(
                    src_ref=ps.at[u], dst_ref=pr.at[u], send_sem=p_send.at[0, u], recv_sem=p_recv.at[0, u],
                    device_id={'cp': far}, device_id_type=MESH),
                pltpu.make_async_remote_copy(
                    src_ref=psl.at[u], dst_ref=prl.at[u], send_sem=p_send.at[1, u], recv_sem=p_recv.at[1, u],
                    device_id={'cp': far}, device_id_type=MESH))

    def own_out(u):
        hh = half * core + u
        return (pltpu.make_async_copy(fo.at[u], out_hbm.at[:, hh], f_send.at[0, u]),
                pltpu.make_async_copy(fl.at[u], lse_hbm.at[hh], f_send.at[1, u]))

    def mate_out(u):
        hh = half * core + u - half
        return (pltpu.make_async_remote_copy(
                    src_ref=fo.at[u], dst_ref=out_hbm.at[:, hh], send_sem=f_send.at[0, u],
                    recv_sem=f_recv.at[0, u - half], device_id={'cp': mate}, device_id_type=MESH),
                pltpu.make_async_remote_copy(
                    src_ref=fl.at[u], dst_ref=lse_hbm.at[hh], send_sem=f_send.at[1, u],
                    recv_sem=f_recv.at[1, u - half], device_id={'cp': mate}, device_id_type=MESH))

    def finish(s):
        @pl.when(jnp.logical_and(s >= 4 * half, s < 6 * half))
        def _():
            u = s - 4 * half
            slot = u + 2 * half
            l = st_l[slot]
            ps[u] = (st_o[slot] * (1.0 / l)).astype(BF)
            psl[u] = st_m[slot] + jnp.log2(l)
            for cp in partial_copies(u):
                cp.start()

        @pl.when(s >= 6 * half)
        def _():
            u = s - 6 * half
            for cp in partial_copies(u):
                cp.wait_recv()
            m_a, m_b = st_m[u], prl[u]
            m = jnp.maximum(m_a, m_b)
            a, b = jnp.exp2(m_a - m), jnp.exp2(m_b - m)
            l = st_l[u] * a + b
            inv = 1.0 / l
            o = st_o[u] * (a * inv) + pr[u].astype(F32) * (b * inv)
            fo[u] = o.T.astype(BF).reshape(tok, ratio, dim)
            fl[u] = (m + jnp.log2(l)) * math.log(2.0)

            @pl.when(u < half)
            def _():
                for cp in own_out(u):
                    cp.start()

            @pl.when(u >= half)
            def _():
                for cp in mate_out(u):
                    cp.start()

    for h in range(half):
        own_q(h).wait()
    load_q(0)
    load_q(1)
    first_scores()

    @pl.loop(0, 4 * half)
    def _(i):
        step(2 * i, s0, s1, m0, m1)
        finish(2 * i)
        step(2 * i + 1, s1, s0, m1, m0)
        finish(2 * i + 1)

    for k in range(3):
        for h in range(half):
            q_copy(k, h).wait_send()
    for h in range(half):
        for cp in kv_copies(h):
            cp.wait_send()
    for u in range(2 * half):
        for cp in partial_copies(u):
            cp.wait_send()
    for u in range(half):
        for cp in own_out(u):
            cp.wait()
        for cp in mate_out(u + half):
            cp.wait_send()
            cp.wait_recv()


def solution(mesh):
    tok_spec = P(('dp', 'cp'))

    def local(queries, key_new, value_new, key_cache, value_cache, prefix_len):
        tok, heads, dim = queries.shape
        cache, kvh = key_cache.shape[:2]
        ratio = heads // kvh
        half = kvh // 2
        rows = tok * ratio
        n_raw = 6
        dma = pltpu.SemaphoreType.DMA
        hbm = pl.BlockSpec(memory_space=pl.ANY)
        scratch = [
            pltpu.VMEM((cache * kvh, dim), BF),
            pltpu.VMEM((cache * kvh, dim), BF),
            pltpu.VMEM((tok * kvh, dim), BF),
            pltpu.VMEM((tok * kvh, dim), BF),
            pltpu.VMEM((kvh + half, cache + tok, dim), BF),
            pltpu.VMEM((kvh + half, dim, cache + dim), BF),
            pltpu.VMEM((2, cache, dim), BF),
            pltpu.VMEM((4 * half, tok, ratio, dim), BF),
            pltpu.VMEM((4 * half, 2 * dim, rows), BF),
            pltpu.VMEM((cache + tok, rows), F32),
            pltpu.VMEM((cache + tok, rows), F32),
            pltpu.VMEM((8, rows), F32),
            pltpu.VMEM((8, rows), F32),
            pltpu.VMEM((4 * half, dim, rows), F32),
            pltpu.VMEM((4 * half, 1, rows), F32),
            pltpu.VMEM((4 * half, 1, rows), F32),
            pltpu.VMEM((2 * half, dim, rows), BF),
            pltpu.VMEM((2 * half, 1, rows), F32),
            pltpu.VMEM((2 * half, dim, rows), BF),
            pltpu.VMEM((2 * half, 1, rows), F32),
            pltpu.VMEM((2 * half, tok, ratio, dim), BF),
            pltpu.VMEM((2 * half, 1, rows), F32),
            dma((2, n_raw)), dma((2,)), dma((3 * half,)), dma((4 * half,)), dma((2, half)), dma((half,)), dma((half,)),
            dma((2, 2 * half)), dma((2, 2 * half)), dma((2, 2 * half)), dma((2, half)),
        ]
        flops = 4 * heads * tok * 4 * cache * dim
        out, lse = pl.pallas_call(
            attend_kernel,
            out_shape=(jax.ShapeDtypeStruct((tok, kvh, ratio, dim), BF), jax.ShapeDtypeStruct((kvh, 1, rows), F32)),
            in_specs=[hbm] * 5 + [pl.BlockSpec(memory_space=pltpu.SMEM)],
            out_specs=(hbm, hbm),
            scratch_shapes=scratch,
            compiler_params=pltpu.CompilerParams(collective_id=0, has_side_effects=True, vmem_limit_bytes=63 * 2 ** 20),
            cost_estimate=pl.CostEstimate(flops=flops, bytes_accessed=4 * cache * kvh * dim, transcendentals=heads * tok * 4 * cache),
            name='attend',
        )(queries.reshape(tok, kvh, ratio, dim), key_new.reshape(tok * kvh, dim), value_new.reshape(tok * kvh, dim),
          key_cache.reshape(cache * kvh, dim), value_cache.reshape(cache * kvh, dim), prefix_len)
        row_lse = lse.reshape(kvh, tok, ratio).transpose(1, 0, 2).reshape(tok, heads)
        return out.reshape(tok, heads, dim), row_lse

    return jax.shard_map(local, mesh=mesh, in_specs=(tok_spec, tok_spec, tok_spec, tok_spec, tok_spec, P('dp')),
                         out_specs=(tok_spec, tok_spec), check_vma=False)
```

```python
import functools
import math

import jax
import jax.numpy as jnp
from jax import lax
from jax.experimental import pallas as pl
from jax.experimental.pallas import tpu as pltpu
from jax.sharding import PartitionSpec as P

MESH = pl.DeviceIdType.MESH
BIG = 1e30
TK = 256
PREP = 128
BF = jnp.bfloat16
F32 = jnp.float32


def attend_kernel(q_hbm, kn_hbm, vn_hbm, kc_hbm, vc_hbm, plen_ref, out_hbm, lse_hbm,
                  raw_k, raw_v, new_k, new_v, kbuf, vbuf, bias, qraw, qt, s_even, s_odd, m_even, m_odd,
                  st_o, st_m, st_l, ps, psl, pr, prl, fo, fl,
                  raw_sem, new_sem, q_send, q_recv, kv_send, k_recv, v_recv, p_send, p_recv, f_send, f_recv):
    tok, kvh, ratio, dim = q_hbm.shape
    cache = kc_hbm.shape[0] // kvh
    half = kvh // 2
    rows = tok * ratio
    n_raw = raw_sem.shape[1]
    raw_pos = cache // n_raw
    chunks = cache // TK
    scale2 = dim ** -0.5 * math.log2(math.e)

    me = lax.axis_index('cp')
    core = lax.rem(me, 2)
    chip2 = me - core
    mate = chip2 + 1 - core
    far = lax.rem(chip2 + 2, 4) + core
    far_other = lax.rem(chip2 + 2, 4) + 1 - core

    def raw_copy(j):
        sl = pl.ds(j * raw_pos * kvh, raw_pos * kvh)
        return (pltpu.make_async_copy(kc_hbm.at[sl], raw_k.at[sl], raw_sem.at[0, j]),
                pltpu.make_async_copy(vc_hbm.at[sl], raw_v.at[sl], raw_sem.at[1, j]))

    def own_q(h):
        return pltpu.make_async_copy(q_hbm.at[:, half * core + h], qraw.at[h], q_recv.at[h])

    for j in range(n_raw):
        a, b = raw_copy(j)
        a.start()
        b.start()
    new_copies = (pltpu.make_async_copy(kn_hbm, new_k, new_sem.at[0]),
                  pltpu.make_async_copy(vn_hbm, new_v, new_sem.at[1]))
    for cp in new_copies:
        cp.start()
    for h in range(half):
        own_q(h).start()

    barrier = pltpu.get_barrier_semaphore()
    for peer in (mate, far, far_other):
        pl.semaphore_signal(barrier, inc=1, device_id={'cp': peer}, device_id_type=MESH)

    ones_row = jnp.where(lax.broadcasted_iota(jnp.int32, (dim, rows), 0) == 0, 1.0, 0.0).astype(BF)

    @pl.loop(0, 4 * half)
    def _(j):
        qt[j, pl.ds(dim, dim), :] = ones_row
        st_o[j] = jnp.zeros((dim, rows), F32)
        st_m[j] = jnp.full((1, rows), -1e38, F32)
        st_l[j] = jnp.zeros((1, rows), F32)

    pl.semaphore_wait(barrier, 3)

    def q_copy(k, h):
        peer, base = ((far, 2 * half), (far_other, 3 * half), (mate, half))[k]
        peer_core = (core, 1 - core, 1 - core)[k]
        return pltpu.make_async_remote_copy(
            src_ref=q_hbm.at[:, half * peer_core + h], dst_ref=qraw.at[base + h],
            send_sem=q_send.at[k * half + h], recv_sem=q_recv.at[base + h],
            device_id={'cp': peer}, device_id_type=MESH)

    for k in range(3):
        for h in range(half):
            q_copy(k, h).start()

    visible_len = plen_ref[0]
    for f, owner in enumerate((me, mate)):
        @pl.loop(0, chunks)
        def _(j):
            lane = lax.broadcasted_iota(jnp.int32, (TK, dim), 1)
            pos = owner * cache + j * TK + lax.broadcasted_iota(jnp.int32, (TK, dim), 0)
            hidden = jnp.logical_and(lane == 0, pos >= visible_len)
            bias[f, pl.ds(pl.multiple_of(j * TK, TK), TK), :] = jnp.where(hidden, -BIG, 0.0).astype(BF)

    for cp in new_copies:
        cp.wait()
    kt = pltpu.einshape('phd->hpd', new_k[...].reshape(tok, kvh, dim))
    vt = pltpu.einshape('phd->hpd', new_v[...].reshape(tok, kvh, dim))
    for h in range(kvh):
        kbuf[h, pl.ds(cache, tok), :] = kt[h]
        vpad = jnp.concatenate([vt[h].astype(F32), jnp.zeros((dim - tok, dim), F32)], axis=0)
        vbuf[h, :, pl.ds(cache, dim)] = vpad.T.astype(BF)
    for j in range(n_raw):
        for cp in raw_copy(j):
            cp.wait()

        @pl.loop(0, raw_pos // PREP)
        def _(i):
            base = pl.multiple_of(j * raw_pos + i * PREP, PREP)
            src = pl.ds(pl.multiple_of(base * kvh, PREP * kvh), PREP * kvh)
            xk = pltpu.einshape('phd->hpd', raw_k[src, :].reshape(PREP, kvh, dim))
            xv = pltpu.einshape('phd->hpd', raw_v[src, :].reshape(PREP, kvh, dim))
            for h in range(kvh):
                kbuf[h, pl.ds(base, PREP), :] = xk[h]
                vbuf[h, :, pl.ds(base, PREP)] = xv[h].T

    def kv_copies(h):
        src = half * (1 - core) + h
        return tuple(
            pltpu.make_async_remote_copy(
                src_ref=buf.at[src], dst_ref=buf.at[kvh + h], send_sem=kv_send.at[w, h], recv_sem=recv.at[h],
                device_id={'cp': mate}, device_id_type=MESH)
            for w, (buf, recv) in enumerate(((kbuf, k_recv), (vbuf, v_recv))))

    for h in range(half):
        for cp in kv_copies(h):
            cp.start()

    n_pairs = 4 * half

    def pair(i):
        second = lax.div(i, 2 * half)
        j = i - second * 2 * half
        late = lax.rem(2 * j + half, 2 * half) + jnp.where(j < half, 2 * half, 0)
        slot = jnp.where(second == 1, late, 2 * j)
        h = lax.rem(slot, half)
        kv = jnp.where(second == 1, kvh + h, half * core + h)
        owner = jnp.where(second == 1, mate, me)
        src = lax.div(slot, half)
        home = jnp.where(src == 0, me, jnp.where(src == 1, mate, jnp.where(src == 2, far, far_other)))
        return second, slot, kv, owner, home

    def load_q(slot):
        qt[slot, pl.ds(0, dim), :] = qraw[slot].reshape(rows, dim).T

    def qk_tile(kv, f, c, qv):
        sl = pl.ds(c * TK, TK)
        lhs = jnp.concatenate([kbuf[kv, sl, :], bias[f, sl, :]], axis=1)
        return jnp.dot(lhs, qv, preferred_element_type=F32)

    def qk_new(kv, owner, home, qv):
        lhs = jnp.concatenate([kbuf[kv, pl.ds(cache, tok), :], jnp.zeros((tok, dim), BF)], axis=1)
        st = jnp.dot(lhs, qv, preferred_element_type=F32)
        key = owner * tok + lax.broadcasted_iota(jnp.int32, (tok, rows), 0)
        query = home * tok + lax.broadcasted_iota(jnp.int32, (tok, rows), 1) // ratio
        return jnp.where(key <= query, st, -BIG)

    def fold_max(mx, st):
        t = jnp.max(st.reshape(st.shape[0] // 8, 8, rows), axis=0)
        return t if mx is None else jnp.maximum(mx, t)

    def first_scores():
        f, slot, kv, owner, home = pair(0)
        for e in range(2):
            qv = qt[slot + e]
            mx = None
            for c in range(chunks):
                st = qk_tile(kv + e, f, c, qv)
                s_even[e][pl.ds(c * TK, TK), :] = st
                mx = fold_max(mx, st)
            st = qk_new(kv + e, owner, home, qv)
            s_even[e][pl.ds(cache, tok), :] = st
            m_even[e][...] = fold_max(mx, st)

    def region(i, sc, sn, mc, mn):
        nxt = lax.rem(i + 1, n_pairs)
        f_n, slot_n, kv_n, owner_n, home_n = pair(nxt)
        _, slot, kv, _, _ = pair(i)
        ahead = 2 * i + 4

        @pl.when(jnp.logical_and(ahead >= half, ahead < 4 * half))
        def _():
            for e in range(2):
                pltpu.make_async_copy(qraw.at[ahead + e], qraw.at[ahead + e], q_recv.at[ahead + e]).wait()

        @pl.when(jnp.logical_and(nxt >= 2 * half, nxt < 2 * half + half // 2))
        def _():
            for e in range(2):
                h = 2 * (nxt - 2 * half) + e
                pltpu.make_async_copy(kbuf.at[kvh + h], kbuf.at[kvh + h], k_recv.at[h]).wait()
                pltpu.make_async_copy(vbuf.at[kvh + h], vbuf.at[kvh + h], v_recv.at[h]).wait()

        qv, m, decay, mx, l8, o = [], [], [], [None] * 2, [], [None] * 2
        for e in range(2):
            qv.append(qt[slot_n + e])
            m_old = st_m[slot + e]
            m.append(jnp.maximum(m_old, jnp.max(mc[e][...], axis=0, keepdims=True) * scale2))
            decay.append(jnp.exp2(m_old - m[e]))
            l8.append(jnp.zeros((8, rows), F32))
        for c in range(chunks):
            sl = pl.ds(c * TK, TK)
            for e in range(2):
                st = qk_tile(kv_n + e, f_n, c, qv[e])
                p = jnp.exp2(sc[e][sl, :] * scale2 - m[e])
                sn[e][sl, :] = st
                mx[e] = fold_max(mx[e], st)
                l8[e] = l8[e] + jnp.sum(p.reshape(TK // 8, 8, rows), axis=0)
                t = jnp.dot(vbuf[kv + e, :, sl], p.astype(BF), preferred_element_type=F32)
                o[e] = t if o[e] is None else o[e] + t
        sl = pl.ds(cache, tok)
        for e in range(2):
            st = qk_new(kv_n + e, owner_n, home_n, qv[e])
            p = jnp.exp2(sc[e][sl, :] * scale2 - m[e])
            sn[e][sl, :] = st
            mn[e][...] = fold_max(mx[e], st)
            l8[e] = l8[e] + jnp.sum(p.reshape(tok // 8, 8, rows), axis=0)
            pb = jnp.concatenate([p.astype(BF), jnp.zeros((dim - tok, rows), BF)], axis=0)
            o[e] = o[e] + jnp.dot(vbuf[kv + e, :, pl.ds(cache, dim)], pb, preferred_element_type=F32)
        for e in range(2):
            st_o[slot + e] = st_o[slot + e] * decay[e] + o[e]
            st_l[slot + e] = st_l[slot + e] * decay[e] + jnp.sum(l8[e], axis=0, keepdims=True)
            st_m[slot + e] = m[e]
            load_q(jnp.minimum(ahead, 4 * half - 2) + e)

    def partial_copies(u):
        return (pltpu.make_async_remote_copy(
                    src_ref=ps.at[u], dst_ref=pr.at[u], send_sem=p_send.at[0, u], recv_sem=p_recv.at[0, u],
                    device_id={'cp': far}, device_id_type=MESH),
                pltpu.make_async_remote_copy(
                    src_ref=psl.at[u], dst_ref=prl.at[u], send_sem=p_send.at[1, u], recv_sem=p_recv.at[1, u],
                    device_id={'cp': far}, device_id_type=MESH))

    def own_out(u):
        hh = half * core + u
        return (pltpu.make_async_copy(fo.at[u], out_hbm.at[:, hh], f_send.at[0, u]),
                pltpu.make_async_copy(fl.at[u], lse_hbm.at[hh], f_send.at[1, u]))

    def mate_out(u):
        hh = half * core + u - half
        return (pltpu.make_async_remote_copy(
                    src_ref=fo.at[u], dst_ref=out_hbm.at[:, hh], send_sem=f_send.at[0, u],
                    recv_sem=f_recv.at[0, u - half], device_id={'cp': mate}, device_id_type=MESH),
                pltpu.make_async_remote_copy(
                    src_ref=fl.at[u], dst_ref=lse_hbm.at[hh], send_sem=f_send.at[1, u],
                    recv_sem=f_recv.at[1, u - half], device_id={'cp': mate}, device_id_type=MESH))

    def finish(i):
        _, slot, _, _, _ = pair(i)

        @pl.when(jnp.logical_and(i >= 2 * half, i < 3 * half))
        def _():
            u = slot - 2 * half
            for e in range(2):
                l = st_l[slot + e]
                ps[u + e] = (st_o[slot + e] * (1.0 / l)).astype(BF)
                psl[u + e] = st_m[slot + e] + jnp.log2(l)
            for e in range(2):
                for cp in partial_copies(u + e):
                    cp.start()

        @pl.when(i >= 3 * half)
        def _():
            u = slot
            for e in range(2):
                for cp in partial_copies(u + e):
                    cp.wait_recv()
            for e in range(2):
                m_a, m_b = st_m[u + e], prl[u + e]
                m = jnp.maximum(m_a, m_b)
                a, b = jnp.exp2(m_a - m), jnp.exp2(m_b - m)
                l = st_l[u + e] * a + b
                inv = 1.0 / l
                o = st_o[u + e] * (a * inv) + pr[u + e].astype(F32) * (b * inv)
                fo[u + e] = o.T.astype(BF).reshape(tok, ratio, dim)
                fl[u + e] = (m + jnp.log2(l)) * math.log(2.0)

            @pl.when(u < half)
            def _():
                for e in range(2):
                    for cp in own_out(u + e):
                        cp.start()

            @pl.when(u >= half)
            def _():
                for e in range(2):
                    for cp in mate_out(u + e):
                        cp.start()

    for h in range(half):
        own_q(h).wait()
    for h in range(half):
        load_q(h)
    first_scores()

    @pl.loop(0, n_pairs // 2)
    def _(i):
        region(2 * i, s_even, s_odd, m_even, m_odd)
        finish(2 * i)
        region(2 * i + 1, s_odd, s_even, m_odd, m_even)
        finish(2 * i + 1)

    for k in range(3):
        for h in range(half):
            q_copy(k, h).wait_send()
    for h in range(half):
        for cp in kv_copies(h):
            cp.wait_send()
    for u in range(2 * half):
        for cp in partial_copies(u):
            cp.wait_send()
    for u in range(half):
        for cp in own_out(u):
            cp.wait()
        for cp in mate_out(u + half):
            cp.wait_send()
            cp.wait_recv()


def place_kernel(out_ref, lse_ref, out_hbm, lse_out, buf, sem):
    kvh, _, rows = lse_ref.shape
    tok, heads = lse_out.shape
    ratio = heads // kvh
    parts = sem.shape[1]
    step = tok // parts
    reads = [pltpu.make_async_copy(out_ref.at[pl.ds(j * step, step)], buf.at[pl.ds(j * step, step)], sem.at[0, j]) for j in range(parts)]
    writes = [pltpu.make_async_copy(buf.at[pl.ds(j * step, step)], out_hbm.at[pl.ds(j * step, step)], sem.at[1, j]) for j in range(parts)]
    for cp in reads:
        cp.start()
    x = lse_ref[...].reshape(kvh, rows)
    lane = lax.broadcasted_iota(jnp.int32, (kvh, heads), 1) // ratio
    head = lax.broadcasted_iota(jnp.int32, (kvh, heads), 0)
    per = heads // ratio
    blocks = [pltpu.roll(x[:, b * heads:(b + 1) * heads], 0, 1, stride=ratio, stride_axis=0) for b in range(tok // per)]
    for t in range(tok):
        turned = pltpu.roll(blocks[t // per], (heads - (t % per) * ratio) % heads, 1)
        lse_out[pl.ds(t, 1), :] = jnp.sum(jnp.where(lane == head, turned, 0.0), axis=0, keepdims=True)
    for r, w in zip(reads, writes):
        r.wait()
        w.start()
    for w in writes:
        w.wait()


def solution(mesh):
    tok_spec = P(('dp', 'cp'))

    def local(queries, key_new, value_new, key_cache, value_cache, prefix_len):
        tok, heads, dim = queries.shape
        cache, kvh = key_cache.shape[:2]
        ratio = heads // kvh
        half = kvh // 2
        rows = tok * ratio
        n_raw = 6
        dma = pltpu.SemaphoreType.DMA
        hbm = pl.BlockSpec(memory_space=pl.ANY)
        scratch = [
            pltpu.VMEM((cache * kvh, dim), BF),
            pltpu.VMEM((cache * kvh, dim), BF),
            pltpu.VMEM((tok * kvh, dim), BF),
            pltpu.VMEM((tok * kvh, dim), BF),
            pltpu.VMEM((kvh + half, cache + tok, dim), BF),
            pltpu.VMEM((kvh + half, dim, cache + dim), BF),
            pltpu.VMEM((2, cache, dim), BF),
            pltpu.VMEM((4 * half, tok, ratio, dim), BF),
            pltpu.VMEM((4 * half, 2 * dim, rows), BF),
            (pltpu.VMEM((cache + tok, rows), F32),) * 2,
            (pltpu.VMEM((cache + tok, rows), F32),) * 2,
            (pltpu.VMEM((8, rows), F32),) * 2,
            (pltpu.VMEM((8, rows), F32),) * 2,
            pltpu.VMEM((4 * half, dim, rows), F32),
            pltpu.VMEM((4 * half, 1, rows), F32),
            pltpu.VMEM((4 * half, 1, rows), F32),
            pltpu.VMEM((2 * half, dim, rows), BF),
            pltpu.VMEM((2 * half, 1, rows), F32),
            pltpu.VMEM((2 * half, dim, rows), BF),
            pltpu.VMEM((2 * half, 1, rows), F32),
            pltpu.VMEM((2 * half, tok, ratio, dim), BF),
            pltpu.VMEM((2 * half, 1, rows), F32),
            dma((2, n_raw)), dma((2,)), dma((3 * half,)), dma((4 * half,)), dma((2, half)), dma((half,)), dma((half,)),
            dma((2, 2 * half)), dma((2, 2 * half)), dma((2, 2 * half)), dma((2, half)),
        ]
        flops = 4 * heads * tok * 4 * cache * dim
        out, lse = pl.pallas_call(
            attend_kernel,
            out_shape=(jax.ShapeDtypeStruct((tok, kvh, ratio, dim), BF), jax.ShapeDtypeStruct((kvh, 1, rows), F32)),
            in_specs=[hbm] * 5 + [pl.BlockSpec(memory_space=pltpu.SMEM)],
            out_specs=(hbm, hbm),
            scratch_shapes=scratch,
            compiler_params=pltpu.CompilerParams(collective_id=0, has_side_effects=True, vmem_limit_bytes=63 * 2 ** 20),
            cost_estimate=pl.CostEstimate(flops=flops, bytes_accessed=4 * cache * kvh * dim, transcendentals=heads * tok * 4 * cache),
            name='attend',
        )(queries.reshape(tok, kvh, ratio, dim), key_new.reshape(tok * kvh, dim), value_new.reshape(tok * kvh, dim),
          key_cache.reshape(cache * kvh, dim), value_cache.reshape(cache * kvh, dim), prefix_len)
        vmem = pl.BlockSpec(memory_space=pltpu.VMEM)
        out, row_lse = pl.pallas_call(
            place_kernel,
            out_shape=(jax.ShapeDtypeStruct((tok, heads, dim), BF), jax.ShapeDtypeStruct((tok, heads), F32)),
            in_specs=[hbm, vmem],
            out_specs=(hbm, vmem),
            scratch_shapes=[pltpu.VMEM((tok, heads, dim), BF), dma((2, 4))],
            name='place',
        )(out.reshape(tok, heads, dim), lse)
        return out, row_lse

    return jax.shard_map(local, mesh=mesh, in_specs=(tok_spec, tok_spec, tok_spec, tok_spec, tok_spec, P('dp')),
                         out_specs=(tok_spec, tok_spec), check_vma=False)
```

```python
import functools
import math

import jax
import jax.numpy as jnp
from jax import lax
from jax.experimental import pallas as pl
from jax.experimental.pallas import tpu as pltpu
from jax.sharding import PartitionSpec as P

MESH = pl.DeviceIdType.MESH
BIG = 1e30
TK = 256
PREP = 128
BF = jnp.bfloat16
F32 = jnp.float32


def attend_kernel(q_hbm, kn_hbm, vn_hbm, kc_hbm, vc_hbm, plen_ref, out_ref, lse_ref,
                  raw_k, raw_v, new_k, new_v, kbuf, vbuf, bias, qraw, qt, s_even, s_odd, m_even, m_odd,
                  st_o, st_m, st_l, ps, psl, pr, prl, fo, fl,
                  raw_sem, new_sem, q_send, q_recv, kv_send, k_recv, v_recv, p_send, p_recv, f_send, f_recv):
    tok, kvh, ratio, dim = q_hbm.shape
    cache = kc_hbm.shape[0] // kvh
    half = kvh // 2
    rows = tok * ratio
    n_raw = raw_sem.shape[1]
    raw_pos = cache // n_raw
    chunks = cache // TK
    scale2 = dim ** -0.5 * math.log2(math.e)

    me = lax.axis_index('cp')
    core = lax.rem(me, 2)
    chip2 = me - core
    mate = chip2 + 1 - core
    far = lax.rem(chip2 + 2, 4) + core
    far_other = lax.rem(chip2 + 2, 4) + 1 - core

    def raw_copy(j):
        sl = pl.ds(j * raw_pos * kvh, raw_pos * kvh)
        return (pltpu.make_async_copy(kc_hbm.at[sl], raw_k.at[sl], raw_sem.at[0, j]),
                pltpu.make_async_copy(vc_hbm.at[sl], raw_v.at[sl], raw_sem.at[1, j]))

    def own_q(h):
        return pltpu.make_async_copy(q_hbm.at[:, half * core + h], qraw.at[h], q_recv.at[h])

    for j in range(n_raw):
        a, b = raw_copy(j)
        a.start()
        b.start()
    new_copies = (pltpu.make_async_copy(kn_hbm, new_k, new_sem.at[0]),
                  pltpu.make_async_copy(vn_hbm, new_v, new_sem.at[1]))
    for cp in new_copies:
        cp.start()
    for h in range(half):
        own_q(h).start()

    barrier = pltpu.get_barrier_semaphore()
    for peer in (mate, far, far_other):
        pl.semaphore_signal(barrier, inc=1, device_id={'cp': peer}, device_id_type=MESH)

    ones_row = jnp.where(lax.broadcasted_iota(jnp.int32, (dim, rows), 0) == 0, 1.0, 0.0).astype(BF)

    @pl.loop(0, 4 * half)
    def _(j):
        qt[j, pl.ds(dim, dim), :] = ones_row
        st_o[j] = jnp.zeros((dim, rows), F32)
        st_m[j] = jnp.full((1, rows), -1e38, F32)
        st_l[j] = jnp.zeros((1, rows), F32)

    pl.semaphore_wait(barrier, 3)

    def q_copy(k, h):
        peer, base = ((far, 2 * half), (far_other, 3 * half), (mate, half))[k]
        peer_core = (core, 1 - core, 1 - core)[k]
        return pltpu.make_async_remote_copy(
            src_ref=q_hbm.at[:, half * peer_core + h], dst_ref=qraw.at[base + h],
            send_sem=q_send.at[k * half + h], recv_sem=q_recv.at[base + h],
            device_id={'cp': peer}, device_id_type=MESH)

    for k in range(3):
        for h in range(half):
            q_copy(k, h).start()

    visible_len = plen_ref[0]
    for f, owner in enumerate((me, mate)):
        @pl.loop(0, chunks)
        def _(j):
            lane = lax.broadcasted_iota(jnp.int32, (TK, dim), 1)
            pos = owner * cache + j * TK + lax.broadcasted_iota(jnp.int32, (TK, dim), 0)
            hidden = jnp.logical_and(lane == 0, pos >= visible_len)
            bias[f, pl.ds(pl.multiple_of(j * TK, TK), TK), :] = jnp.where(hidden, -BIG, 0.0).astype(BF)

    for cp in new_copies:
        cp.wait()
    kt = pltpu.einshape('phd->hpd', new_k[...].reshape(tok, kvh, dim))
    vt = pltpu.einshape('phd->hpd', new_v[...].reshape(tok, kvh, dim))
    for h in range(kvh):
        kbuf[h, pl.ds(cache, tok), :] = kt[h]
        vpad = jnp.concatenate([vt[h].astype(F32), jnp.zeros((dim - tok, dim), F32)], axis=0)
        vbuf[h, :, pl.ds(cache, dim)] = vpad.T.astype(BF)
    for j in range(n_raw):
        for cp in raw_copy(j):
            cp.wait()

        @pl.loop(0, raw_pos // PREP)
        def _(i):
            base = pl.multiple_of(j * raw_pos + i * PREP, PREP)
            src = pl.ds(pl.multiple_of(base * kvh, PREP * kvh), PREP * kvh)
            xk = pltpu.einshape('phd->hpd', raw_k[src, :].reshape(PREP, kvh, dim))
            xv = pltpu.einshape('phd->hpd', raw_v[src, :].reshape(PREP, kvh, dim))
            for h in range(kvh):
                kbuf[h, pl.ds(base, PREP), :] = xk[h]
                vbuf[h, :, pl.ds(base, PREP)] = xv[h].T

    def kv_copies(h):
        src = half * (1 - core) + h
        return tuple(
            pltpu.make_async_remote_copy(
                src_ref=buf.at[src], dst_ref=buf.at[kvh + h], send_sem=kv_send.at[w, h], recv_sem=recv.at[h],
                device_id={'cp': mate}, device_id_type=MESH)
            for w, (buf, recv) in enumerate(((kbuf, k_recv), (vbuf, v_recv))))

    for h in range(half):
        for cp in kv_copies(h):
            cp.start()

    n_pairs = 4 * half

    def pair(i):
        q = half // 2
        late = lax.rem(2 * (i - 3 * q - 1) + half, 2 * half) + 2 * half
        last = lax.rem(2 * (i - 6 * q) + half, 2 * half)
        slot = jnp.where(i < q + 1, 2 * i,
               jnp.where(i < 3 * q + 1, 2 * half + 2 * (i - q - 1),
               jnp.where(i < 5 * q + 1, late,
               jnp.where(i < 6 * q, 2 * i - 8 * q, last))))
        second = jnp.where(jnp.logical_or(jnp.logical_and(i >= 3 * q + 1, i < 5 * q + 1), i >= 6 * q), 1, 0)
        h = lax.rem(slot, half)
        kv = jnp.where(second == 1, kvh + h, half * core + h)
        owner = jnp.where(second == 1, mate, me)
        src = lax.div(slot, half)
        home = jnp.where(src == 0, me, jnp.where(src == 1, mate, jnp.where(src == 2, far, far_other)))
        return second, slot, kv, owner, home

    def load_q(slot):
        qt[slot, pl.ds(0, dim), :] = qraw[slot].reshape(rows, dim).T

    def qk_tile(kv, f, c, qv):
        sl = pl.ds(c * TK, TK)
        lhs = jnp.concatenate([kbuf[kv, sl, :], bias[f, sl, :]], axis=1)
        return jnp.dot(lhs, qv, preferred_element_type=F32)

    def qk_new(kv, owner, home, qv):
        lhs = jnp.concatenate([kbuf[kv, pl.ds(cache, tok), :], jnp.zeros((tok, dim), BF)], axis=1)
        st = jnp.dot(lhs, qv, preferred_element_type=F32)
        key = owner * tok + lax.broadcasted_iota(jnp.int32, (tok, rows), 0)
        query = home * tok + lax.broadcasted_iota(jnp.int32, (tok, rows), 1) // ratio
        return jnp.where(key <= query, st, -BIG)

    def fold_max(mx, st):
        t = jnp.max(st.reshape(st.shape[0] // 8, 8, rows), axis=0)
        return t if mx is None else jnp.maximum(mx, t)

    def first_scores():
        f, slot, kv, owner, home = pair(0)
        for e in range(2):
            qv = qt[slot + e]
            mx = None
            for c in range(chunks):
                st = qk_tile(kv + e, f, c, qv)
                s_even[e][pl.ds(c * TK, TK), :] = st
                mx = fold_max(mx, st)
            st = qk_new(kv + e, owner, home, qv)
            s_even[e][pl.ds(cache, tok), :] = st
            m_even[e][...] = fold_max(mx, st)

    def region(i, sc, sn, mc, mn):
        nxt = lax.rem(i + 1, n_pairs)
        f_n, slot_n, kv_n, owner_n, home_n = pair(nxt)
        _, slot, kv, _, _ = pair(i)
        q = half // 2
        later = jnp.minimum(i + 2, n_pairs - 1)
        ahead = pair(later)[1]

        @pl.when(jnp.logical_or(i + 2 == 6 * q - 1, jnp.logical_and(i + 2 >= q, i + 2 < 3 * q + 1)))
        def _():
            for e in range(2):
                pltpu.make_async_copy(qraw.at[ahead + e], qraw.at[ahead + e], q_recv.at[ahead + e]).wait()

        @pl.when(jnp.logical_and(nxt >= 3 * q + 1, nxt < 4 * q + 1))
        def _():
            for e in range(2):
                h = 2 * (nxt - 3 * q - 1) + e
                pltpu.make_async_copy(kbuf.at[kvh + h], kbuf.at[kvh + h], k_recv.at[h]).wait()
                pltpu.make_async_copy(vbuf.at[kvh + h], vbuf.at[kvh + h], v_recv.at[h]).wait()

        qv, m, decay, mx, l8, o = [], [], [], [None] * 2, [], [None] * 2
        for e in range(2):
            qv.append(qt[slot_n + e])
            m_old = st_m[slot + e]
            m.append(jnp.maximum(m_old, jnp.max(mc[e][...], axis=0, keepdims=True) * scale2))
            decay.append(jnp.exp2(m_old - m[e]))
            l8.append(jnp.zeros((8, rows), F32))
        for c in range(chunks):
            sl = pl.ds(c * TK, TK)
            for e in range(2):
                st = qk_tile(kv_n + e, f_n, c, qv[e])
                p = jnp.exp2(sc[e][sl, :] * scale2 - m[e])
                sn[e][sl, :] = st
                mx[e] = fold_max(mx[e], st)
                l8[e] = l8[e] + jnp.sum(p.reshape(TK // 8, 8, rows), axis=0)
                t = jnp.dot(vbuf[kv + e, :, sl], p.astype(BF), preferred_element_type=F32)
                o[e] = t if o[e] is None else o[e] + t
        sl = pl.ds(cache, tok)
        for e in range(2):
            st = qk_new(kv_n + e, owner_n, home_n, qv[e])
            p = jnp.exp2(sc[e][sl, :] * scale2 - m[e])
            sn[e][sl, :] = st
            mn[e][...] = fold_max(mx[e], st)
            l8[e] = l8[e] + jnp.sum(p.reshape(tok // 8, 8, rows), axis=0)
            pb = jnp.concatenate([p.astype(BF), jnp.zeros((dim - tok, rows), BF)], axis=0)
            o[e] = o[e] + jnp.dot(vbuf[kv + e, :, pl.ds(cache, dim)], pb, preferred_element_type=F32)
        for e in range(2):
            st_o[slot + e] = st_o[slot + e] * decay[e] + o[e]
            st_l[slot + e] = st_l[slot + e] * decay[e] + jnp.sum(l8[e], axis=0, keepdims=True)
            st_m[slot + e] = m[e]
            load_q(ahead + e)

    def partial_copies(u):
        return (pltpu.make_async_remote_copy(
                    src_ref=ps.at[u], dst_ref=pr.at[u], send_sem=p_send.at[0, u], recv_sem=p_recv.at[0, u],
                    device_id={'cp': far}, device_id_type=MESH),
                pltpu.make_async_remote_copy(
                    src_ref=psl.at[u], dst_ref=prl.at[u], send_sem=p_send.at[1, u], recv_sem=p_recv.at[1, u],
                    device_id={'cp': far}, device_id_type=MESH))

    def mate_out(u):
        hh = half * core + u - half
        return (pltpu.make_async_remote_copy(
                    src_ref=fo.at[u - half], dst_ref=out_ref.at[:, hh], send_sem=f_send.at[0, u - half],
                    recv_sem=f_recv.at[0, u - half], device_id={'cp': mate}, device_id_type=MESH),
                pltpu.make_async_remote_copy(
                    src_ref=fl.at[u - half], dst_ref=lse_ref.at[hh], send_sem=f_send.at[1, u - half],
                    recv_sem=f_recv.at[1, u - half], device_id={'cp': mate}, device_id_type=MESH))

    def finish(i):
        _, slot, _, _, _ = pair(i)

        q = half // 2

        @pl.when(jnp.logical_and(i >= 3 * q + 1, i < 5 * q + 1))
        def _():
            u = slot - 2 * half
            for e in range(2):
                l = st_l[slot + e]
                ps[u + e] = (st_o[slot + e] * (1.0 / l)).astype(BF)
                psl[u + e] = st_m[slot + e] + jnp.log2(l)
            for e in range(2):
                for cp in partial_copies(u + e):
                    cp.start()

        @pl.when(i >= 6 * q)
        def _():
            u = slot
            for e in range(2):
                for cp in partial_copies(u + e):
                    cp.wait_recv()
            done = []
            for e in range(2):
                m_a, m_b = st_m[u + e], prl[u + e]
                m = jnp.maximum(m_a, m_b)
                a, b = jnp.exp2(m_a - m), jnp.exp2(m_b - m)
                l = st_l[u + e] * a + b
                inv = 1.0 / l
                o = st_o[u + e] * (a * inv) + pr[u + e].astype(F32) * (b * inv)
                done.append((o.T.astype(BF).reshape(tok, ratio, dim), (m + jnp.log2(l)) * math.log(2.0)))

            @pl.when(u < half)
            def _():
                for e in range(2):
                    out_ref[:, half * core + u + e] = done[e][0]
                    lse_ref[half * core + u + e] = done[e][1]

            @pl.when(u >= half)
            def _():
                for e in range(2):
                    fo[u - half + e] = done[e][0]
                    fl[u - half + e] = done[e][1]
                for e in range(2):
                    for cp in mate_out(u + e):
                        cp.start()

    for h in range(half):
        own_q(h).wait()
    for h in range(half):
        load_q(h)
    first_scores()

    @pl.loop(0, n_pairs // 2)
    def _(i):
        region(2 * i, s_even, s_odd, m_even, m_odd)
        finish(2 * i)
        region(2 * i + 1, s_odd, s_even, m_odd, m_even)
        finish(2 * i + 1)

    for k in range(3):
        for h in range(half):
            q_copy(k, h).wait_send()
    for h in range(half):
        for cp in kv_copies(h):
            cp.wait_send()
    for u in range(2 * half):
        for cp in partial_copies(u):
            cp.wait_send()
    for u in range(half):
        for cp in mate_out(u + half):
            cp.wait_send()
            cp.wait_recv()


def place_kernel(out_ref, lse_ref, out_hbm, lse_hbm, lse_buf, sem):
    kvh, _, rows = lse_ref.shape
    tok, heads = lse_buf.shape
    ratio = heads // kvh
    write = pltpu.make_async_copy(out_ref, out_hbm, sem.at[0])
    write.start()
    x = lse_ref[...].reshape(kvh, rows)
    lane = lax.broadcasted_iota(jnp.int32, (kvh, heads), 1) // ratio
    head = lax.broadcasted_iota(jnp.int32, (kvh, heads), 0)
    per = heads // ratio
    blocks = [pltpu.roll(x[:, b * heads:(b + 1) * heads], 0, 1, stride=ratio, stride_axis=0) for b in range(tok // per)]
    for t in range(tok):
        turned = pltpu.roll(blocks[t // per], (heads - (t % per) * ratio) % heads, 1)
        lse_buf[pl.ds(t, 1), :] = jnp.sum(jnp.where(lane == head, turned, 0.0), axis=0, keepdims=True)
    lse_write = pltpu.make_async_copy(lse_buf, lse_hbm, sem.at[1])
    lse_write.start()
    write.wait()
    lse_write.wait()


def solution(mesh):
    tok_spec = P(('dp', 'cp'))

    def local(queries, key_new, value_new, key_cache, value_cache, prefix_len):
        tok, heads, dim = queries.shape
        cache, kvh = key_cache.shape[:2]
        ratio = heads // kvh
        half = kvh // 2
        rows = tok * ratio
        n_raw = 6
        dma = pltpu.SemaphoreType.DMA
        hbm = pl.BlockSpec(memory_space=pltpu.HBM)
        vmem = pl.BlockSpec(memory_space=pltpu.VMEM)
        scratch = [
            pltpu.VMEM((cache * kvh, dim), BF),
            pltpu.VMEM((cache * kvh, dim), BF),
            pltpu.VMEM((tok * kvh, dim), BF),
            pltpu.VMEM((tok * kvh, dim), BF),
            pltpu.VMEM((kvh + half, cache + tok, dim), BF),
            pltpu.VMEM((kvh + half, dim, cache + dim), BF),
            pltpu.VMEM((2, cache, dim), BF),
            pltpu.VMEM((4 * half, tok, ratio, dim), BF),
            pltpu.VMEM((4 * half, 2 * dim, rows), BF),
            (pltpu.VMEM((cache + tok, rows), F32),) * 2,
            (pltpu.VMEM((cache + tok, rows), F32),) * 2,
            (pltpu.VMEM((8, rows), F32),) * 2,
            (pltpu.VMEM((8, rows), F32),) * 2,
            pltpu.VMEM((4 * half, dim, rows), F32),
            pltpu.VMEM((4 * half, 1, rows), F32),
            pltpu.VMEM((4 * half, 1, rows), F32),
            pltpu.VMEM((2 * half, dim, rows), BF),
            pltpu.VMEM((2 * half, 1, rows), F32),
            pltpu.VMEM((2 * half, dim, rows), BF),
            pltpu.VMEM((2 * half, 1, rows), F32),
            pltpu.VMEM((half, tok, ratio, dim), BF),
            pltpu.VMEM((half, 1, rows), F32),
            dma((2, n_raw)), dma((2,)), dma((3 * half,)), dma((4 * half,)), dma((2, half)), dma((half,)), dma((half,)),
            dma((2, 2 * half)), dma((2, 2 * half)), dma((2, half)), dma((2, half)),
        ]
        flops = 4 * heads * tok * 4 * cache * dim
        out, lse = pl.pallas_call(
            attend_kernel,
            out_shape=(pltpu.VMEM((tok, kvh, ratio, dim), BF), pltpu.VMEM((kvh, 1, rows), F32)),
            in_specs=[hbm] * 5 + [pl.BlockSpec(memory_space=pltpu.SMEM)],
            out_specs=(vmem, vmem),
            scratch_shapes=scratch,
            compiler_params=pltpu.CompilerParams(collective_id=0, has_side_effects=True, vmem_limit_bytes=60 * 2 ** 20),
            cost_estimate=pl.CostEstimate(flops=flops, bytes_accessed=4 * cache * kvh * dim, transcendentals=heads * tok * 4 * cache),
            name='attend',
        )(queries.reshape(tok, kvh, ratio, dim), key_new.reshape(tok * kvh, dim), value_new.reshape(tok * kvh, dim),
          key_cache.reshape(cache * kvh, dim), value_cache.reshape(cache * kvh, dim), prefix_len)
        out, row_lse = pl.pallas_call(
            place_kernel,
            out_shape=(jax.ShapeDtypeStruct((tok, heads, dim), BF), jax.ShapeDtypeStruct((tok, heads), F32)),
            in_specs=[vmem, vmem],
            out_specs=(hbm, hbm),
            scratch_shapes=[pltpu.VMEM((tok, heads), F32), dma((2,))],
            compiler_params=pltpu.CompilerParams(vmem_limit_bytes=2 * 2 ** 20),
            name='place',
        )(out.reshape(tok, heads, dim), lse)
        return out, row_lse

    return jax.shard_map(local, mesh=mesh, in_specs=(tok_spec, tok_spec, tok_spec, tok_spec, tok_spec, P('dp')),
                         out_specs=(tok_spec, tok_spec), check_vma=False)
```

```python
import functools
import math

import jax
import jax.numpy as jnp
from jax import lax
from jax.experimental import pallas as pl
from jax.experimental.pallas import tpu as pltpu
from jax.sharding import PartitionSpec as P

MESH = pl.DeviceIdType.MESH
BIG = 1e30
TK = 256
PREP = 128
BF = jnp.bfloat16
SEQ = ((0, 0), (2, 0), (4, 0), (12, 0), (14, 0), (12, 1), (8, 0), (14, 1),
       (10, 0), (8, 1), (10, 1), (6, 0), (4, 1), (6, 1), (0, 1), (2, 1))
F32 = jnp.float32


def _packed(part):
    v = sum((slot // 2 + 8 * second) << (4 * k) for k, (slot, second) in enumerate(part))
    return v - (1 << 32) if v >= 1 << 31 else v


ORDER = (_packed(SEQ[:8]), _packed(SEQ[8:]))
Q_PAIRS = tuple(SEQ.index((s, 0)) for s in range(4, 16, 2))
KV_PAIRS = tuple(next(k for k, (s, f) in enumerate(SEQ) if f and s % 4 == h) for h in (0, 2))
R_PAIRS = tuple(k for k, (s, f) in enumerate(SEQ) if f and s >= 8)
L_PAIRS = tuple(k for k, (s, f) in enumerate(SEQ) if f and s < 8)


def among(i, ks):
    hit = i == ks[0]
    for k in ks[1:]:
        hit = jnp.logical_or(hit, i == k)
    return hit


def attend_kernel(q_hbm, kn_hbm, vn_hbm, kc_hbm, vc_hbm, plen_ref, out_ref, lse_ref,
                  raw_k, raw_v, new_k, new_v, kbuf, vbuf, bias, qraw, qt, sbuf, mbuf,
                  st_o, st_m, st_l, ps, psl, pr, prl, fo, fl,
                  raw_sem, new_sem, q_send, q_recv, kv_send, k_recv, v_recv, p_send, p_recv, f_send, f_recv):
    tok, kvh, ratio, dim = q_hbm.shape
    cache = kc_hbm.shape[0] // kvh
    half = kvh // 2
    rows = tok * ratio
    n_raw = raw_sem.shape[1]
    raw_pos = cache // n_raw
    chunks = cache // TK
    scale2 = dim ** -0.5 * math.log2(math.e)

    me = lax.axis_index('cp')
    core = lax.rem(me, 2)
    chip2 = me - core
    mate = chip2 + 1 - core
    far = lax.rem(chip2 + 2, 4) + core
    far_other = lax.rem(chip2 + 2, 4) + 1 - core

    def raw_copy(j):
        sl = pl.ds(j * raw_pos * kvh, raw_pos * kvh)
        return (pltpu.make_async_copy(kc_hbm.at[sl], raw_k.at[sl], raw_sem.at[0, j]),
                pltpu.make_async_copy(vc_hbm.at[sl], raw_v.at[sl], raw_sem.at[1, j]))

    def own_q(h):
        return pltpu.make_async_copy(q_hbm.at[:, half * core + h], qraw.at[h], q_recv.at[h])

    for j in range(n_raw):
        a, b = raw_copy(j)
        a.start()
        b.start()
    new_copies = (pltpu.make_async_copy(kn_hbm, new_k, new_sem.at[0]),
                  pltpu.make_async_copy(vn_hbm, new_v, new_sem.at[1]))
    for cp in new_copies:
        cp.start()
    for h in range(half):
        own_q(h).start()

    barrier = pltpu.get_barrier_semaphore()
    for peer in (mate, far, far_other):
        pl.semaphore_signal(barrier, inc=1, device_id={'cp': peer}, device_id_type=MESH)

    ones_row = jnp.where(lax.broadcasted_iota(jnp.int32, (dim, rows), 0) == 0, 1.0, 0.0).astype(BF)

    @pl.loop(0, 4 * half)
    def _(j):
        qt[j, pl.ds(dim, dim), :] = ones_row
        st_o[j] = jnp.zeros((dim, rows), F32)
        st_m[j] = jnp.full((1, rows), -1e38, F32)
        st_l[j] = jnp.zeros((1, rows), F32)

    pl.semaphore_wait(barrier, 3)

    def q_copy(k, h):
        peer, base = ((far_other, 3 * half), (far, 2 * half), (mate, half))[k]
        peer_core = (1 - core, core, 1 - core)[k]
        return pltpu.make_async_remote_copy(
            src_ref=q_hbm.at[:, half * peer_core + h], dst_ref=qraw.at[base + h],
            send_sem=q_send.at[k * half + h], recv_sem=q_recv.at[base + h],
            device_id={'cp': peer}, device_id_type=MESH)

    for k in range(3):
        for h in range(half):
            q_copy(k, h).start()

    visible_len = plen_ref[0]
    for f, owner in enumerate((me, mate)):
        @pl.loop(0, chunks)
        def _(j):
            lane = lax.broadcasted_iota(jnp.int32, (TK, dim), 1)
            pos = owner * cache + j * TK + lax.broadcasted_iota(jnp.int32, (TK, dim), 0)
            hidden = jnp.logical_and(lane == 0, pos >= visible_len)
            bias[f, pl.ds(pl.multiple_of(j * TK, TK), TK), :] = jnp.where(hidden, -BIG, 0.0).astype(BF)

    for cp in new_copies:
        cp.wait()
    kt = pltpu.einshape('phd->hpd', new_k[...].reshape(tok, kvh, dim))
    vt = pltpu.einshape('phd->hpd', new_v[...].reshape(tok, kvh, dim))
    for h in range(kvh):
        kbuf[h, pl.ds(cache, tok), :] = kt[h]
        vpad = jnp.concatenate([vt[h].astype(F32), jnp.zeros((dim - tok, dim), F32)], axis=0)
        vbuf[h, :, pl.ds(cache, dim)] = vpad.T.astype(BF)
    def kv_parts(h, lo, n):
        src = half * (1 - core) + h
        to = dict(device_id={'cp': mate}, device_id_type=MESH)
        k_rows, v_lanes = pl.ds(lo, min(n, cache + tok - lo)), pl.ds(lo, n)
        return (pltpu.make_async_remote_copy(
                    src_ref=kbuf.at[src, k_rows], dst_ref=kbuf.at[kvh + h, k_rows],
                    send_sem=kv_send.at[0, h], recv_sem=k_recv.at[h], **to),
                pltpu.make_async_remote_copy(
                    src_ref=vbuf.at[src, :, v_lanes], dst_ref=vbuf.at[kvh + h, :, v_lanes],
                    send_sem=kv_send.at[1, h], recv_sem=v_recv.at[h], **to))

    def kv_start(lo, n):
        for h in range(half):
            for cp in kv_parts(h, lo, n):
                cp.start()

    for j in range(n_raw):
        for cp in raw_copy(j):
            cp.wait()

        @pl.loop(0, raw_pos // PREP)
        def _(i):
            base = pl.multiple_of(j * raw_pos + i * PREP, PREP)
            src = pl.ds(pl.multiple_of(base * kvh, PREP * kvh), PREP * kvh)
            xk = pltpu.einshape('phd->hpd', raw_k[src, :].reshape(PREP, kvh, dim))
            xv = pltpu.einshape('phd->hpd', raw_v[src, :].reshape(PREP, kvh, dim))
            for h in range(kvh):
                kbuf[h, pl.ds(base, PREP), :] = xk[h]
                vbuf[h, :, pl.ds(base, PREP)] = xv[h].T

        if j == 0:
            kv_start(cache, dim)
        else:
            kv_start((j - 1) * raw_pos, raw_pos)

    n_pairs = 4 * half

    def pair(i):
        code = lax.shift_right_logical(jnp.where(i < 8, ORDER[0], ORDER[1]), 4 * lax.rem(i, 8))
        slot = 2 * jnp.bitwise_and(code, 7)
        second = lax.div(jnp.bitwise_and(code, 15), 8)
        h = lax.rem(slot, half)
        kv = jnp.where(second == 1, kvh + h, half * core + h)
        owner = jnp.where(second == 1, mate, me)
        src = lax.div(slot, half)
        home = jnp.where(src == 0, me, jnp.where(src == 1, mate, jnp.where(src == 2, far, far_other)))
        return second, slot, kv, owner, home

    def load_q(slot):
        qt[slot, pl.ds(0, dim), :] = qraw[slot].reshape(rows, dim).T

    def qk_tile(kv, f, c, qv):
        sl = pl.ds(c * TK, TK)
        lhs = jnp.concatenate([kbuf[kv, sl, :], bias[f, sl, :]], axis=1)
        return jnp.dot(lhs, qv, preferred_element_type=F32)

    def qk_new(kv, owner, home, qv):
        lhs = jnp.concatenate([kbuf[kv, pl.ds(cache, tok), :], jnp.zeros((tok, dim), BF)], axis=1)
        st = jnp.dot(lhs, qv, preferred_element_type=F32)
        key = owner * tok + lax.broadcasted_iota(jnp.int32, (tok, rows), 0)
        query = home * tok + lax.broadcasted_iota(jnp.int32, (tok, rows), 1) // ratio
        return jnp.where(key <= query, st, -BIG)

    def fold_max(mx, st):
        t = jnp.max(st.reshape(st.shape[0] // 8, 8, rows), axis=0)
        return t if mx is None else jnp.maximum(mx, t)

    def first_scores():
        f, slot, kv, owner, home = pair(0)
        for e in range(2):
            qv = qt[slot + e]
            mx = None
            for c in range(chunks):
                st = qk_tile(kv + e, f, c, qv)
                sbuf[e][pl.ds(c * TK, TK), :] = st
                mx = fold_max(mx, st)
            st = qk_new(kv + e, owner, home, qv)
            sbuf[e][pl.ds(cache, tok), :] = st
            mbuf[e][...] = fold_max(mx, st)

    def wait_inputs(i):
        _, slot, kv, _, _ = pair(i)

        @pl.when(among(i, Q_PAIRS))
        def _():
            for e in range(2):
                pltpu.make_async_copy(qraw.at[slot + e], qraw.at[slot + e], q_recv.at[slot + e]).wait()

    def wait_kv(i):
        _, slot, kv, _, _ = pair(i)

        @pl.when(among(i, KV_PAIRS))
        def _():
            for e in range(2):
                pltpu.make_async_copy(kbuf.at[kv + e], kbuf.at[kv + e], k_recv.at[kv + e - kvh]).wait()
                pltpu.make_async_copy(vbuf.at[kv + e], vbuf.at[kv + e], v_recv.at[kv + e - kvh]).wait()

    def region(r):
        cur = [2 * r, 2 * r + 1, jnp.minimum(2 * r + 2, n_pairs - 1), jnp.minimum(2 * r + 3, n_pairs - 1)]
        wait_inputs(2 * r + 2)
        wait_inputs(2 * r + 3)
        wait_kv(2 * r + 1)
        wait_kv(2 * r + 2)
        info = [pair(c) for c in cur]
        units = [tuple(x + e if k in (1, 2) else x for k, x in enumerate(info[p])) for p in range(3) for e in range(2)]
        for e in range(2):
            load_q(info[2][1] + e)
        m_old = [st_m[units[e][1]] for e in range(4)]
        for e in range(4):
            _, slot, kv, _, _ = units[e]
            f_n, slot_n, kv_n, owner_n, home_n = units[e + 2]
            n = (e + 2) % 4
            qv = qt[slot_n]
            m = jnp.maximum(m_old[e], jnp.max(mbuf[e][...], axis=0, keepdims=True) * scale2)
            decay = jnp.exp2(m_old[e] - m)
            mx, o, l8 = None, None, jnp.zeros((8, rows), F32)
            for c in range(chunks):
                sl = pl.ds(c * TK, TK)
                st = qk_tile(kv_n, f_n, c, qv)
                p = jnp.exp2(sbuf[e][sl, :] * scale2 - m)
                sbuf[n][sl, :] = st
                mx = fold_max(mx, st)
                l8 = l8 + jnp.sum(p.reshape(TK // 8, 8, rows), axis=0)
                t = jnp.dot(vbuf[kv, :, sl], p.astype(BF), preferred_element_type=F32)
                o = t if o is None else o + t
            sl = pl.ds(cache, tok)
            st = qk_new(kv_n, owner_n, home_n, qv)
            p = jnp.exp2(sbuf[e][sl, :] * scale2 - m)
            sbuf[n][sl, :] = st
            mbuf[n][...] = fold_max(mx, st)
            l8 = l8 + jnp.sum(p.reshape(tok // 8, 8, rows), axis=0)
            pb = jnp.concatenate([p.astype(BF), jnp.zeros((dim - tok, rows), BF)], axis=0)
            o = o + jnp.dot(vbuf[kv, :, pl.ds(cache, dim)], pb, preferred_element_type=F32)
            st_o[slot] = st_o[slot] * decay + o
            st_l[slot] = st_l[slot] * decay + jnp.sum(l8, axis=0, keepdims=True)
            st_m[slot] = m
        for e in range(2):
            load_q(info[3][1] + e)

    def partial_copies(u):
        return (pltpu.make_async_remote_copy(
                    src_ref=ps.at[u], dst_ref=pr.at[u], send_sem=p_send.at[0, u], recv_sem=p_recv.at[0, u],
                    device_id={'cp': far}, device_id_type=MESH),
                pltpu.make_async_remote_copy(
                    src_ref=psl.at[u], dst_ref=prl.at[u], send_sem=p_send.at[1, u], recv_sem=p_recv.at[1, u],
                    device_id={'cp': far}, device_id_type=MESH))

    def mate_out(u):
        hh = half * core + u - half
        return (pltpu.make_async_remote_copy(
                    src_ref=fo.at[u - half], dst_ref=out_ref.at[:, hh], send_sem=f_send.at[0, u - half],
                    recv_sem=f_recv.at[0, u - half], device_id={'cp': mate}, device_id_type=MESH),
                pltpu.make_async_remote_copy(
                    src_ref=fl.at[u - half], dst_ref=lse_ref.at[hh], send_sem=f_send.at[1, u - half],
                    recv_sem=f_recv.at[1, u - half], device_id={'cp': mate}, device_id_type=MESH))

    def finish(i):
        _, slot, _, _, _ = pair(i)

        @pl.when(among(i, R_PAIRS))
        def _():
            u = slot - 2 * half
            for e in range(2):
                l = st_l[slot + e]
                ps[u + e] = (st_o[slot + e] * (1.0 / l)).astype(BF)
                psl[u + e] = st_m[slot + e] + jnp.log2(l)
            for e in range(2):
                for cp in partial_copies(u + e):
                    cp.start()

        @pl.when(among(i, L_PAIRS))
        def _():
            u = slot
            for e in range(2):
                for cp in partial_copies(u + e):
                    cp.wait_recv()
            done = []
            for e in range(2):
                m_a, m_b = st_m[u + e], prl[u + e]
                m = jnp.maximum(m_a, m_b)
                a, b = jnp.exp2(m_a - m), jnp.exp2(m_b - m)
                l = st_l[u + e] * a + b
                inv = 1.0 / l
                o = st_o[u + e] * (a * inv) + pr[u + e].astype(F32) * (b * inv)
                done.append((o.T.astype(BF).reshape(tok, ratio, dim), (m + jnp.log2(l)) * math.log(2.0)))

            @pl.when(u < half)
            def _():
                for e in range(2):
                    out_ref[:, half * core + u + e] = done[e][0]
                    lse_ref[half * core + u + e] = done[e][1]

            @pl.when(u >= half)
            def _():
                for e in range(2):
                    fo[u - half + e] = done[e][0]
                    fl[u - half + e] = done[e][1]
                for e in range(2):
                    for cp in mate_out(u + e):
                        cp.start()

    for h in range(half):
        own_q(h).wait()
    for h in range(half):
        load_q(h)
    first_scores()
    kv_start(cache - raw_pos, raw_pos)

    @pl.loop(0, n_pairs // 2)
    def _(r):
        region(r)
        finish(2 * r)
        finish(2 * r + 1)

    for k in range(3):
        for h in range(half):
            q_copy(k, h).wait_send()
    for h in range(half):
        pltpu.make_async_copy(kbuf.at[h], kbuf.at[h], kv_send.at[0, h]).wait()
        pltpu.make_async_copy(vbuf.at[h], vbuf.at[h], kv_send.at[1, h]).wait()
    for u in range(2 * half):
        for cp in partial_copies(u):
            cp.wait_send()
    for u in range(half):
        for cp in mate_out(u + half):
            cp.wait_send()
            cp.wait_recv()


def place_kernel(out_ref, lse_ref, out_hbm, lse_hbm, lse_buf, sem):
    kvh, _, rows = lse_ref.shape
    tok, heads = lse_buf.shape
    ratio = heads // kvh
    write = pltpu.make_async_copy(out_ref, out_hbm, sem.at[0])
    write.start()
    x = lse_ref[...].reshape(kvh, rows)
    lane = lax.broadcasted_iota(jnp.int32, (kvh, heads), 1) // ratio
    head = lax.broadcasted_iota(jnp.int32, (kvh, heads), 0)
    per = heads // ratio
    blocks = [pltpu.roll(x[:, b * heads:(b + 1) * heads], 0, 1, stride=ratio, stride_axis=0) for b in range(tok // per)]
    for t in range(tok):
        turned = pltpu.roll(blocks[t // per], (heads - (t % per) * ratio) % heads, 1)
        lse_buf[pl.ds(t, 1), :] = jnp.sum(jnp.where(lane == head, turned, 0.0), axis=0, keepdims=True)
    lse_write = pltpu.make_async_copy(lse_buf, lse_hbm, sem.at[1])
    lse_write.start()
    write.wait()
    lse_write.wait()


def solution(mesh):
    tok_spec = P(('dp', 'cp'))

    def local(queries, key_new, value_new, key_cache, value_cache, prefix_len):
        tok, heads, dim = queries.shape
        cache, kvh = key_cache.shape[:2]
        ratio = heads // kvh
        half = kvh // 2
        rows = tok * ratio
        n_raw = 6
        dma = pltpu.SemaphoreType.DMA
        hbm = pl.BlockSpec(memory_space=pltpu.HBM)
        vmem = pl.BlockSpec(memory_space=pltpu.VMEM)
        scratch = [
            pltpu.VMEM((cache * kvh, dim), BF),
            pltpu.VMEM((cache * kvh, dim), BF),
            pltpu.VMEM((tok * kvh, dim), BF),
            pltpu.VMEM((tok * kvh, dim), BF),
            pltpu.VMEM((kvh + half, cache + tok, dim), BF),
            pltpu.VMEM((kvh + half, dim, cache + dim), BF),
            pltpu.VMEM((2, cache, dim), BF),
            pltpu.VMEM((4 * half, tok, ratio, dim), BF),
            pltpu.VMEM((4 * half, 2 * dim, rows), BF),
            (pltpu.VMEM((cache + tok, rows), F32),) * 4,
            (pltpu.VMEM((8, rows), F32),) * 4,
            pltpu.VMEM((4 * half, dim, rows), F32),
            pltpu.VMEM((4 * half, 1, rows), F32),
            pltpu.VMEM((4 * half, 1, rows), F32),
            pltpu.VMEM((2 * half, dim, rows), BF),
            pltpu.VMEM((2 * half, 1, rows), F32),
            pltpu.VMEM((2 * half, dim, rows), BF),
            pltpu.VMEM((2 * half, 1, rows), F32),
            pltpu.VMEM((half, tok, ratio, dim), BF),
            pltpu.VMEM((half, 1, rows), F32),
            dma((2, n_raw)), dma((2,)), dma((3 * half,)), dma((4 * half,)), dma((2, half)), dma((half,)), dma((half,)),
            dma((2, 2 * half)), dma((2, 2 * half)), dma((2, half)), dma((2, half)),
        ]
        flops = 4 * heads * tok * 4 * cache * dim
        out, lse = pl.pallas_call(
            attend_kernel,
            out_shape=(pltpu.VMEM((tok, kvh, ratio, dim), BF), pltpu.VMEM((kvh, 1, rows), F32)),
            in_specs=[hbm] * 5 + [pl.BlockSpec(memory_space=pltpu.SMEM)],
            out_specs=(vmem, vmem),
            scratch_shapes=scratch,
            compiler_params=pltpu.CompilerParams(collective_id=0, has_side_effects=True, vmem_limit_bytes=60 * 2 ** 20),
            cost_estimate=pl.CostEstimate(flops=flops, bytes_accessed=4 * cache * kvh * dim, transcendentals=heads * tok * 4 * cache),
            name='attend',
        )(queries.reshape(tok, kvh, ratio, dim), key_new.reshape(tok * kvh, dim), value_new.reshape(tok * kvh, dim),
          key_cache.reshape(cache * kvh, dim), value_cache.reshape(cache * kvh, dim), prefix_len)
        out, row_lse = pl.pallas_call(
            place_kernel,
            out_shape=(jax.ShapeDtypeStruct((tok, heads, dim), BF), jax.ShapeDtypeStruct((tok, heads), F32)),
            in_specs=[vmem, vmem],
            out_specs=(hbm, hbm),
            scratch_shapes=[pltpu.VMEM((tok, heads), F32), dma((2,))],
            compiler_params=pltpu.CompilerParams(vmem_limit_bytes=2 * 2 ** 20),
            name='place',
        )(out.reshape(tok, heads, dim), lse)
        return out, row_lse

    return jax.shard_map(local, mesh=mesh, in_specs=(tok_spec, tok_spec, tok_spec, tok_spec, tok_spec, P('dp')),
                         out_specs=(tok_spec, tok_spec), check_vma=False)
```

```python
import functools
import math

import jax
import jax.numpy as jnp
from jax import lax
from jax.experimental import pallas as pl
from jax.experimental.pallas import tpu as pltpu
from jax.sharding import PartitionSpec as P

MESH = pl.DeviceIdType.MESH
BIG = 1e30
TK = 256
PREP = 128
BF = jnp.bfloat16
SEQ = ((0, 0), (2, 0), (4, 0), (12, 0), (14, 0), (12, 1), (8, 0), (14, 1),
       (10, 0), (8, 1), (10, 1), (6, 0), (4, 1), (6, 1), (0, 1), (2, 1))
F32 = jnp.float32


def _packed(part):
    v = sum((slot // 2 + 8 * second) << (4 * k) for k, (slot, second) in enumerate(part))
    return v - (1 << 32) if v >= 1 << 31 else v


ORDER = (_packed(SEQ[:8]), _packed(SEQ[8:]))
Q_PAIRS = tuple(SEQ.index((s, 0)) for s in range(4, 16, 2))
KV_PAIRS = tuple(next(k for k, (s, f) in enumerate(SEQ) if f and s % 4 == h) for h in (0, 2))
R_PAIRS = tuple(k for k, (s, f) in enumerate(SEQ) if f and s >= 8)
L_PAIRS = tuple(k for k, (s, f) in enumerate(SEQ) if f and s < 8)


def among(i, ks):
    hit = i == ks[0]
    for k in ks[1:]:
        hit = jnp.logical_or(hit, i == k)
    return hit


def attend_kernel(q_hbm, kn_hbm, vn_hbm, kc_hbm, vc_hbm, plen_ref, out_ref, lse_ref,
                  raw_k, raw_v, new_k, new_v, kbuf, vbuf, bias, qraw, qt, sbuf, mbuf,
                  st_o, st_m, st_l, ps, psl, pr, prl, fo, fl,
                  raw_sem, new_sem, q_send, q_recv, kv_send, k_recv, v_recv, p_send, p_recv, f_send, f_recv):
    tok, kvh, ratio, dim = q_hbm.shape
    cache = kc_hbm.shape[0] // kvh
    half = kvh // 2
    rows = tok * ratio
    n_raw = raw_sem.shape[1]
    raw_pos = cache // n_raw
    chunks = cache // TK
    scale2 = dim ** -0.5 * math.log2(math.e)

    me = lax.axis_index('cp')
    core = lax.rem(me, 2)
    chip2 = me - core
    mate = chip2 + 1 - core
    far = lax.rem(chip2 + 2, 4) + core
    far_other = lax.rem(chip2 + 2, 4) + 1 - core

    def raw_copy(j):
        sl = pl.ds(j * raw_pos * kvh, raw_pos * kvh)
        return (pltpu.make_async_copy(kc_hbm.at[sl], raw_k.at[sl], raw_sem.at[0, j]),
                pltpu.make_async_copy(vc_hbm.at[sl], raw_v.at[sl], raw_sem.at[1, j]))

    def own_q(h):
        return pltpu.make_async_copy(q_hbm.at[:, half * core + h], qraw.at[h], q_recv.at[h])

    for j in range(n_raw):
        a, b = raw_copy(j)
        a.start()
        b.start()
    new_copies = (pltpu.make_async_copy(kn_hbm, new_k, new_sem.at[0]),
                  pltpu.make_async_copy(vn_hbm, new_v, new_sem.at[1]))
    for cp in new_copies:
        cp.start()
    for h in range(half):
        own_q(h).start()

    barrier = pltpu.get_barrier_semaphore()
    for peer in (mate, far, far_other):
        pl.semaphore_signal(barrier, inc=1, device_id={'cp': peer}, device_id_type=MESH)

    ones_row = jnp.where(lax.broadcasted_iota(jnp.int32, (dim, rows), 0) == 0, 1.0, 0.0).astype(BF)

    @pl.loop(0, 4 * half)
    def _(j):
        qt[j, pl.ds(dim, dim), :] = ones_row
        st_o[j] = jnp.zeros((dim, rows), F32)
        st_m[j] = jnp.full((1, rows), -1e38, F32)
        st_l[j] = jnp.zeros((1, rows), F32)

    pl.semaphore_wait(barrier, 3)

    def q_copy(k, h):
        peer, base = ((far_other, 3 * half), (far, 2 * half), (mate, half))[k]
        peer_core = (1 - core, core, 1 - core)[k]
        return pltpu.make_async_remote_copy(
            src_ref=q_hbm.at[:, half * peer_core + h], dst_ref=qraw.at[base + h],
            send_sem=q_send.at[k * half + h], recv_sem=q_recv.at[base + h],
            device_id={'cp': peer}, device_id_type=MESH)

    for k in range(3):
        for h in range(half):
            q_copy(k, h).start()

    visible_len = plen_ref[0]
    for f, owner in enumerate((me, mate)):
        @pl.loop(0, chunks)
        def _(j):
            lane = lax.broadcasted_iota(jnp.int32, (TK, dim), 1)
            pos = owner * cache + j * TK + lax.broadcasted_iota(jnp.int32, (TK, dim), 0)
            hidden = jnp.logical_and(lane == 0, pos >= visible_len)
            bias[f, pl.ds(pl.multiple_of(j * TK, TK), TK), :] = jnp.where(hidden, -BIG, 0.0).astype(BF)

    for cp in new_copies:
        cp.wait()
    kt = pltpu.einshape('phd->hpd', new_k[...].reshape(tok, kvh, dim))
    vt = pltpu.einshape('phd->hpd', new_v[...].reshape(tok, kvh, dim))
    for h in range(kvh):
        kbuf[h, pl.ds(cache, tok), :] = kt[h]
        vpad = jnp.concatenate([vt[h].astype(F32), jnp.zeros((dim - tok, dim), F32)], axis=0)
        vbuf[h, :, pl.ds(cache, dim)] = vpad.T.astype(BF)
    def kv_parts(h, lo, n):
        src = half * (1 - core) + h
        to = dict(device_id={'cp': mate}, device_id_type=MESH)
        k_rows, v_lanes = pl.ds(lo, min(n, cache + tok - lo)), pl.ds(lo, n)
        return (pltpu.make_async_remote_copy(
                    src_ref=kbuf.at[src, k_rows], dst_ref=kbuf.at[kvh + h, k_rows],
                    send_sem=kv_send.at[0, h], recv_sem=k_recv.at[h], **to),
                pltpu.make_async_remote_copy(
                    src_ref=vbuf.at[src, :, v_lanes], dst_ref=vbuf.at[kvh + h, :, v_lanes],
                    send_sem=kv_send.at[1, h], recv_sem=v_recv.at[h], **to))

    def kv_start(lo, n):
        for h in range(half):
            for cp in kv_parts(h, lo, n):
                cp.start()

    for j in range(n_raw):
        for cp in raw_copy(j):
            cp.wait()

        @pl.loop(0, raw_pos // PREP)
        def _(i):
            base = pl.multiple_of(j * raw_pos + i * PREP, PREP)
            src = pl.ds(pl.multiple_of(base * kvh, PREP * kvh), PREP * kvh)
            xk = pltpu.einshape('phd->hpd', raw_k[src, :].reshape(PREP, kvh, dim))
            xv = pltpu.einshape('phd->hpd', raw_v[src, :].reshape(PREP, kvh, dim))
            for h in range(kvh):
                kbuf[h, pl.ds(base, PREP), :] = xk[h]
                vbuf[h, :, pl.ds(base, PREP)] = xv[h].T

        if j == 0:
            kv_start(cache, dim)
        else:
            kv_start((j - 1) * raw_pos, raw_pos)

    n_pairs = 4 * half

    def pair(i):
        code = lax.shift_right_logical(jnp.where(i < 8, ORDER[0], ORDER[1]), 4 * lax.rem(i, 8))
        slot = 2 * jnp.bitwise_and(code, 7)
        second = lax.div(jnp.bitwise_and(code, 15), 8)
        h = lax.rem(slot, half)
        kv = jnp.where(second == 1, kvh + h, half * core + h)
        owner = jnp.where(second == 1, mate, me)
        src = lax.div(slot, half)
        home = jnp.where(src == 0, me, jnp.where(src == 1, mate, jnp.where(src == 2, far, far_other)))
        return second, slot, kv, owner, home

    def load_q(slot):
        qt[slot, pl.ds(0, dim), :] = qraw[slot].reshape(rows, dim).T

    def qk_tile(kv, f, c, qv):
        sl = pl.ds(c * TK, TK)
        lhs = jnp.concatenate([kbuf[kv, sl, :], bias[f, sl, :]], axis=1)
        return jnp.dot(lhs, qv, preferred_element_type=F32)

    def qk_new(kv, owner, home, qv):
        lhs = jnp.concatenate([kbuf[kv, pl.ds(cache, tok), :], jnp.zeros((tok, dim), BF)], axis=1)
        st = jnp.dot(lhs, qv, preferred_element_type=F32)
        key = owner * tok + lax.broadcasted_iota(jnp.int32, (tok, rows), 0)
        query = home * tok + lax.broadcasted_iota(jnp.int32, (tok, rows), 1) // ratio
        return jnp.where(key <= query, st, -BIG)

    def fold_max(mx, st):
        t = jnp.max(st.reshape(st.shape[0] // 8, 8, rows), axis=0)
        return t if mx is None else jnp.maximum(mx, t)

    def first_scores():
        f, slot, kv, owner, home = pair(0)
        for e in range(2):
            qv = qt[slot + e]
            mx = None
            for c in range(chunks):
                st = qk_tile(kv + e, f, c, qv)
                sbuf[e][pl.ds(c * TK, TK), :] = st
                mx = fold_max(mx, st)
            st = qk_new(kv + e, owner, home, qv)
            sbuf[e][pl.ds(cache, tok), :] = st
            mbuf[e][...] = fold_max(mx, st)

    def region(i, sc, sn, mc, mn):
        nxt = lax.rem(i + 1, n_pairs)
        f_n, slot_n, kv_n, owner_n, home_n = pair(nxt)
        _, slot, kv, _, _ = pair(i)
        later = jnp.minimum(i + 2, n_pairs - 1)
        ahead = pair(later)[1]

        @pl.when(among(i + 2, Q_PAIRS))
        def _():
            for e in range(2):
                pltpu.make_async_copy(qraw.at[ahead + e], qraw.at[ahead + e], q_recv.at[ahead + e]).wait()

        @pl.when(among(i + 1, KV_PAIRS))
        def _():
            for e in range(2):
                pltpu.make_async_copy(kbuf.at[kv_n + e], kbuf.at[kv_n + e], k_recv.at[kv_n + e - kvh]).wait()
                pltpu.make_async_copy(vbuf.at[kv_n + e], vbuf.at[kv_n + e], v_recv.at[kv_n + e - kvh]).wait()

        qv, m, decay, mx, l8, o = [], [], [], [None] * 2, [], [None] * 2
        for e in range(2):
            qv.append(qt[slot_n + e])
            m_old = st_m[slot + e]
            m.append(jnp.maximum(m_old, jnp.max(mc[e][...], axis=0, keepdims=True) * scale2))
            decay.append(jnp.exp2(m_old - m[e]))
            l8.append(jnp.zeros((8, rows), F32))
        for c in range(chunks):
            sl = pl.ds(c * TK, TK)
            for e in range(2):
                st = qk_tile(kv_n + e, f_n, c, qv[e])
                p = jnp.exp2(sc[e][sl, :] * scale2 - m[e])
                sn[e][sl, :] = st
                mx[e] = fold_max(mx[e], st)
                l8[e] = l8[e] + jnp.sum(p.reshape(TK // 8, 8, rows), axis=0)
                t = jnp.dot(vbuf[kv + e, :, sl], p.astype(BF), preferred_element_type=F32)
                o[e] = t if o[e] is None else o[e] + t
        sl = pl.ds(cache, tok)
        for e in range(2):
            st = qk_new(kv_n + e, owner_n, home_n, qv[e])
            p = jnp.exp2(sc[e][sl, :] * scale2 - m[e])
            sn[e][sl, :] = st
            mn[e][...] = fold_max(mx[e], st)
            l8[e] = l8[e] + jnp.sum(p.reshape(tok // 8, 8, rows), axis=0)
            pb = jnp.concatenate([p.astype(BF), jnp.zeros((dim - tok, rows), BF)], axis=0)
            o[e] = o[e] + jnp.dot(vbuf[kv + e, :, pl.ds(cache, dim)], pb, preferred_element_type=F32)
        for e in range(2):
            st_o[slot + e] = st_o[slot + e] * decay[e] + o[e]
            st_l[slot + e] = st_l[slot + e] * decay[e] + jnp.sum(l8[e], axis=0, keepdims=True)
            st_m[slot + e] = m[e]
            load_q(ahead + e)

    def partial_copies(u):
        return (pltpu.make_async_remote_copy(
                    src_ref=ps.at[u], dst_ref=pr.at[u], send_sem=p_send.at[0, u], recv_sem=p_recv.at[0, u],
                    device_id={'cp': far}, device_id_type=MESH),
                pltpu.make_async_remote_copy(
                    src_ref=psl.at[u], dst_ref=prl.at[u], send_sem=p_send.at[1, u], recv_sem=p_recv.at[1, u],
                    device_id={'cp': far}, device_id_type=MESH))

    def mate_out(u):
        hh = half * core + u - half
        return (pltpu.make_async_remote_copy(
                    src_ref=fo.at[u - half], dst_ref=out_ref.at[:, hh], send_sem=f_send.at[0, u - half],
                    recv_sem=f_recv.at[0, u - half], device_id={'cp': mate}, device_id_type=MESH),
                pltpu.make_async_remote_copy(
                    src_ref=fl.at[u - half], dst_ref=lse_ref.at[hh], send_sem=f_send.at[1, u - half],
                    recv_sem=f_recv.at[1, u - half], device_id={'cp': mate}, device_id_type=MESH))

    def finish(i):
        _, slot, _, _, _ = pair(i)

        @pl.when(among(i, R_PAIRS))
        def _():
            u = slot - 2 * half
            for e in range(2):
                l = st_l[slot + e]
                ps[u + e] = (st_o[slot + e] * (1.0 / l)).astype(BF)
                psl[u + e] = st_m[slot + e] + jnp.log2(l)
            for e in range(2):
                for cp in partial_copies(u + e):
                    cp.start()

        @pl.when(among(i, L_PAIRS))
        def _():
            u = slot
            for e in range(2):
                for cp in partial_copies(u + e):
                    cp.wait_recv()
            done = []
            for e in range(2):
                m_a, m_b = st_m[u + e], prl[u + e]
                m = jnp.maximum(m_a, m_b)
                a, b = jnp.exp2(m_a - m), jnp.exp2(m_b - m)
                l = st_l[u + e] * a + b
                inv = 1.0 / l
                o = st_o[u + e] * (a * inv) + pr[u + e].astype(F32) * (b * inv)
                done.append((o.T.astype(BF).reshape(tok, ratio, dim), (m + jnp.log2(l)) * math.log(2.0)))

            @pl.when(u < half)
            def _():
                for e in range(2):
                    out_ref[:, half * core + u + e] = done[e][0]
                    lse_ref[half * core + u + e] = done[e][1]

            @pl.when(u >= half)
            def _():
                for e in range(2):
                    fo[u - half + e] = done[e][0]
                    fl[u - half + e] = done[e][1]
                for e in range(2):
                    for cp in mate_out(u + e):
                        cp.start()

    for h in range(half):
        own_q(h).wait()
    for h in range(half):
        load_q(h)
    first_scores()
    kv_start(cache - raw_pos, raw_pos)

    @pl.loop(0, n_pairs // 2)
    def _(i):
        region(2 * i, sbuf[:2], sbuf[2:], mbuf[:2], mbuf[2:])
        finish(2 * i)
        region(2 * i + 1, sbuf[2:], sbuf[:2], mbuf[2:], mbuf[:2])
        finish(2 * i + 1)

    for k in range(3):
        for h in range(half):
            q_copy(k, h).wait_send()
    for h in range(half):
        pltpu.make_async_copy(kbuf.at[h], kbuf.at[h], kv_send.at[0, h]).wait()
        pltpu.make_async_copy(vbuf.at[h], vbuf.at[h], kv_send.at[1, h]).wait()
    for u in range(2 * half):
        for cp in partial_copies(u):
            cp.wait_send()
    for u in range(half):
        for cp in mate_out(u + half):
            cp.wait_send()
            cp.wait_recv()


def place_kernel(out_ref, lse_ref, out_hbm, lse_hbm, lse_buf, sem):
    kvh, _, rows = lse_ref.shape
    tok, heads = lse_buf.shape
    ratio = heads // kvh
    write = pltpu.make_async_copy(out_ref, out_hbm, sem.at[0])
    write.start()
    x = lse_ref[...].reshape(kvh, rows)
    lane = lax.broadcasted_iota(jnp.int32, (kvh, heads), 1) // ratio
    head = lax.broadcasted_iota(jnp.int32, (kvh, heads), 0)
    per = heads // ratio
    blocks = [pltpu.roll(x[:, b * heads:(b + 1) * heads], 0, 1, stride=ratio, stride_axis=0) for b in range(tok // per)]
    for t in range(tok):
        turned = pltpu.roll(blocks[t // per], (heads - (t % per) * ratio) % heads, 1)
        lse_buf[pl.ds(t, 1), :] = jnp.sum(jnp.where(lane == head, turned, 0.0), axis=0, keepdims=True)
    lse_write = pltpu.make_async_copy(lse_buf, lse_hbm, sem.at[1])
    lse_write.start()
    write.wait()
    lse_write.wait()


def solution(mesh):
    tok_spec = P(('dp', 'cp'))

    def local(queries, key_new, value_new, key_cache, value_cache, prefix_len):
        tok, heads, dim = queries.shape
        cache, kvh = key_cache.shape[:2]
        ratio = heads // kvh
        half = kvh // 2
        rows = tok * ratio
        n_raw = 6
        dma = pltpu.SemaphoreType.DMA
        hbm = pl.BlockSpec(memory_space=pltpu.HBM)
        vmem = pl.BlockSpec(memory_space=pltpu.VMEM)
        scratch = [
            pltpu.VMEM((cache * kvh, dim), BF),
            pltpu.VMEM((cache * kvh, dim), BF),
            pltpu.VMEM((tok * kvh, dim), BF),
            pltpu.VMEM((tok * kvh, dim), BF),
            pltpu.VMEM((kvh + half, cache + tok, dim), BF),
            pltpu.VMEM((kvh + half, dim, cache + dim), BF),
            pltpu.VMEM((2, cache, dim), BF),
            pltpu.VMEM((4 * half, tok, ratio, dim), BF),
            pltpu.VMEM((4 * half, 2 * dim, rows), BF),
            (pltpu.VMEM((cache + tok, rows), F32),) * 4,
            (pltpu.VMEM((8, rows), F32),) * 4,
            pltpu.VMEM((4 * half, dim, rows), F32),
            pltpu.VMEM((4 * half, 1, rows), F32),
            pltpu.VMEM((4 * half, 1, rows), F32),
            pltpu.VMEM((2 * half, dim, rows), BF),
            pltpu.VMEM((2 * half, 1, rows), F32),
            pltpu.VMEM((2 * half, dim, rows), BF),
            pltpu.VMEM((2 * half, 1, rows), F32),
            pltpu.VMEM((half, tok, ratio, dim), BF),
            pltpu.VMEM((half, 1, rows), F32),
            dma((2, n_raw)), dma((2,)), dma((3 * half,)), dma((4 * half,)), dma((2, half)), dma((half,)), dma((half,)),
            dma((2, 2 * half)), dma((2, 2 * half)), dma((2, half)), dma((2, half)),
        ]
        flops = 4 * heads * tok * 4 * cache * dim
        out, lse = pl.pallas_call(
            attend_kernel,
            out_shape=(pltpu.VMEM((tok, kvh, ratio, dim), BF), pltpu.VMEM((kvh, 1, rows), F32)),
            in_specs=[hbm] * 5 + [pl.BlockSpec(memory_space=pltpu.SMEM)],
            out_specs=(vmem, vmem),
            scratch_shapes=scratch,
            compiler_params=pltpu.CompilerParams(collective_id=0, has_side_effects=True, vmem_limit_bytes=60 * 2 ** 20),
            cost_estimate=pl.CostEstimate(flops=flops, bytes_accessed=4 * cache * kvh * dim, transcendentals=heads * tok * 4 * cache),
            name='attend',
        )(queries.reshape(tok, kvh, ratio, dim), key_new.reshape(tok * kvh, dim), value_new.reshape(tok * kvh, dim),
          key_cache.reshape(cache * kvh, dim), value_cache.reshape(cache * kvh, dim), prefix_len)
        out, row_lse = pl.pallas_call(
            place_kernel,
            out_shape=(jax.ShapeDtypeStruct((tok, heads, dim), BF), jax.ShapeDtypeStruct((tok, heads), F32)),
            in_specs=[vmem, vmem],
            out_specs=(hbm, hbm),
            scratch_shapes=[pltpu.VMEM((tok, heads), F32), dma((2,))],
            compiler_params=pltpu.CompilerParams(vmem_limit_bytes=2 * 2 ** 20),
            name='place',
        )(out.reshape(tok, heads, dim), lse)
        return out, row_lse

    return jax.shard_map(local, mesh=mesh, in_specs=(tok_spec, tok_spec, tok_spec, tok_spec, tok_spec, P('dp')),
                         out_specs=(tok_spec, tok_spec), check_vma=False)
```

```python
import functools
import math

import jax
import jax.numpy as jnp
from jax import lax
from jax.experimental import pallas as pl
from jax.experimental.pallas import tpu as pltpu
from jax.sharding import PartitionSpec as P

MESH = pl.DeviceIdType.MESH
BIG = 1e30
TK = 256
BF = jnp.bfloat16
SEQ = ((0, 0), (2, 0), (4, 0), (12, 0), (14, 0), (12, 1), (8, 0), (14, 1),
       (10, 0), (8, 1), (10, 1), (6, 0), (4, 1), (6, 1), (0, 1), (2, 1))
F32 = jnp.float32


def _packed(part):
    v = sum((slot // 2 + 8 * second) << (4 * k) for k, (slot, second) in enumerate(part))
    return v - (1 << 32) if v >= 1 << 31 else v


ORDER = (_packed(SEQ[:8]), _packed(SEQ[8:]))
Q_PAIRS = tuple(SEQ.index((s, 0)) for s in range(4, 16, 2))
KV_PAIRS = tuple(next(k for k, (s, f) in enumerate(SEQ) if f and s % 4 == h) for h in (0, 2))
R_PAIRS = tuple(k for k, (s, f) in enumerate(SEQ) if f and s >= 8)
L_PAIRS = tuple(k for k, (s, f) in enumerate(SEQ) if f and s < 8)


def among(i, ks):
    hit = i == ks[0]
    for k in ks[1:]:
        hit = jnp.logical_or(hit, i == k)
    return hit


def attend_kernel(q_hbm, kn_hbm, vn_hbm, kc_hbm, vc_hbm, plen_hbm, out_ref, lse_ref,
                  raw_k, raw_v, new_k, new_v, kbuf, vbuf, bias, qraw, qt, pick, plen, sbuf, mbuf,
                  st_o, st_m, st_l, ps, psl, pr, prl, fo, fl,
                  raw_sem, new_sem, q_send, q_recv, kv_send, k_recv, v_recv, p_send, p_recv, f_send, f_recv):
    tok, kvh, ratio, dim = q_hbm.shape
    cache = kc_hbm.shape[0] // kvh
    half = kvh // 2
    rows = tok * ratio
    n_raw = raw_sem.shape[1]
    raw_pos = cache // n_raw
    chunks = cache // TK
    scale2 = dim ** -0.5 * math.log2(math.e)

    me = lax.axis_index('cp')
    core = lax.rem(me, 2)
    chip2 = me - core
    mate = chip2 + 1 - core
    far = lax.rem(chip2 + 2, 4) + core
    far_other = lax.rem(chip2 + 2, 4) + 1 - core

    def raw_copy(j):
        sl = pl.ds(j * raw_pos * kvh, raw_pos * kvh)
        return (pltpu.make_async_copy(kc_hbm.at[sl], raw_k.at[sl], raw_sem.at[0, j]),
                pltpu.make_async_copy(vc_hbm.at[sl], raw_v.at[sl], raw_sem.at[1, j]))

    def own_q(h):
        return pltpu.make_async_copy(q_hbm.at[:, half * core + h], qraw.at[h], q_recv.at[h])

    for j in range(n_raw):
        a, b = raw_copy(j)
        a.start()
        b.start()
    plen_copy = pltpu.make_async_copy(plen_hbm, plen, new_sem.at[2])
    plen_copy.start()
    new_copies = (pltpu.make_async_copy(kn_hbm, new_k, new_sem.at[0]),
                  pltpu.make_async_copy(vn_hbm, new_v, new_sem.at[1]))
    for cp in new_copies:
        cp.start()
    for h in range(half):
        own_q(h).start()

    barrier = pltpu.get_barrier_semaphore()
    for peer in (mate, far, far_other):
        pl.semaphore_signal(barrier, inc=1, device_id={'cp': peer}, device_id_type=MESH)

    pick[...] = jnp.where(lax.broadcasted_iota(jnp.int32, (dim, rows), 0) == 0, 1.0, 0.0).astype(BF)
    for e in range(2):
        mbuf[e][...] = jnp.full((8, rows), -3e38, F32)

    pl.semaphore_wait(barrier, 3)

    def q_copy(k, h):
        peer, base = ((far_other, 3 * half), (far, 2 * half), (mate, half))[k]
        peer_core = (1 - core, core, 1 - core)[k]
        return pltpu.make_async_remote_copy(
            src_ref=q_hbm.at[:, half * peer_core + h], dst_ref=qraw.at[base + h],
            send_sem=q_send.at[k * half + h], recv_sem=q_recv.at[base + h],
            device_id={'cp': peer}, device_id_type=MESH)

    for k in range(3):
        for h in range(half):
            q_copy(k, h).start()

    plen_copy.wait()
    visible_len = plen[0]
    for f, owner in enumerate((me, mate)):
        @pl.loop(0, chunks)
        def _(j):
            lane = lax.broadcasted_iota(jnp.int32, (TK, dim), 1)
            pos = owner * cache + j * TK + lax.broadcasted_iota(jnp.int32, (TK, dim), 0)
            hidden = jnp.logical_and(lane == 0, pos >= visible_len)
            bias[f, pl.ds(pl.multiple_of(j * TK, TK), TK), :] = jnp.where(hidden, -BIG, 0.0).astype(BF)

    for cp in new_copies:
        cp.wait()
    kt = pltpu.einshape('phd->hpd', new_k[...].reshape(tok, kvh, dim))
    vt = pltpu.einshape('phd->hpd', new_v[...].reshape(tok, kvh, dim))
    for h in range(kvh):
        kbuf[h, pl.ds(cache, tok), :] = kt[h]
        vpad = jnp.concatenate([vt[h].astype(F32), jnp.zeros((dim - tok, dim), F32)], axis=0)
        vbuf[h, :, pl.ds(cache, dim)] = vpad.T.astype(BF)
    def kv_parts(h, lo, n):
        src = half * (1 - core) + h
        to = dict(device_id={'cp': mate}, device_id_type=MESH)
        k_rows, v_lanes = pl.ds(lo, tok if n == dim else n), pl.ds(lo, n)
        return (pltpu.make_async_remote_copy(
                    src_ref=kbuf.at[src, k_rows], dst_ref=kbuf.at[kvh + h, k_rows],
                    send_sem=kv_send.at[0, h], recv_sem=k_recv.at[h], **to),
                pltpu.make_async_remote_copy(
                    src_ref=vbuf.at[src, :, v_lanes], dst_ref=vbuf.at[kvh + h, :, v_lanes],
                    send_sem=kv_send.at[1, h], recv_sem=v_recv.at[h], **to))

    def kv_start(lo, n):
        for h in range(half):
            for cp in kv_parts(h, lo, n):
                cp.start()

    n_pairs = 4 * half

    def pair(i):
        code = lax.shift_right_logical(jnp.where(i < 8, ORDER[0], ORDER[1]), 4 * lax.rem(i, 8))
        slot = 2 * jnp.bitwise_and(code, 7)
        second = lax.div(jnp.bitwise_and(code, 15), 8)
        h = lax.rem(slot, half)
        kv = jnp.where(second == 1, kvh + h, half * core + h)
        owner = jnp.where(second == 1, mate, me)
        src = lax.div(slot, half)
        home = jnp.where(src == 0, me, jnp.where(src == 1, mate, jnp.where(src == 2, far, far_other)))
        return second, slot, kv, owner, home

    def load_q(slot):
        qt[slot] = qraw[slot].reshape(rows, dim).T

    def score_rhs(slot):
        return jnp.concatenate([qt[slot], pick[...]], axis=0)

    def qk_tile(kv, f, c, qv):
        sl = pl.ds(c * TK if isinstance(c, int) else pl.multiple_of(c * TK, TK), TK)
        lhs = jnp.concatenate([kbuf[kv, sl, :], bias[f, sl, :]], axis=1)
        return jnp.dot(lhs, qv, preferred_element_type=F32)

    def qk_new(kv, owner, home, qv):
        lhs = jnp.concatenate([kbuf[kv, pl.ds(cache, tok), :], jnp.zeros((tok, dim), BF)], axis=1)
        st = jnp.dot(lhs, qv, preferred_element_type=F32)
        key = owner * tok + lax.broadcasted_iota(jnp.int32, (tok, rows), 0)
        query = home * tok + lax.broadcasted_iota(jnp.int32, (tok, rows), 1) // ratio
        return jnp.where(key <= query, st, -BIG)

    def fold_max(mx, st):
        t = jnp.max(st.reshape(st.shape[0] // 8, 8, rows), axis=0)
        return t if mx is None else jnp.maximum(mx, t)

    def prepare(c):
        base = pl.multiple_of(c * TK, TK)
        src = pl.ds(pl.multiple_of(base * kvh, TK * kvh), TK * kvh)
        xk = pltpu.einshape('phd->hpd', raw_k[src, :].reshape(TK, kvh, dim))
        xv = pltpu.einshape('phd->hpd', raw_v[src, :].reshape(TK, kvh, dim))
        for h in range(kvh):
            kbuf[h, pl.ds(base, TK), :] = xk[h]
            vbuf[h, :, pl.ds(base, TK)] = xv[h].T

    f_0, slot_0, kv_0, owner_0, home_0 = pair(0)

    def first_scores(c):
        for e in range(2):
            st = qk_tile(kv_0 + e, f_0, c, score_rhs(slot_0 + e))
            sbuf[e][pl.ds(pl.multiple_of(c * TK, TK), TK), :] = st
            mbuf[e][...] = fold_max(mbuf[e][...], st)

    per_raw = raw_pos // TK
    for h in range(half):
        own_q(h).wait()
    for h in range(half):
        load_q(h)
    for cp in raw_copy(0):
        cp.wait()
    kv_start(cache, dim)
    prepare(0)

    @pl.loop(1, chunks)
    def _(c):
        @pl.when(lax.rem(c, per_raw) == 0)
        def _():
            j = lax.div(c, per_raw)
            for cp in raw_copy(j):
                cp.wait()

            @pl.when(j >= 2)
            def _():
                kv_start(pl.multiple_of((j - 2) * raw_pos, raw_pos), raw_pos)

        first_scores(c - 1)
        prepare(c)

    kv_start(cache - 2 * raw_pos, raw_pos)
    first_scores(chunks - 1)
    for e in range(2):
        st = qk_new(kv_0 + e, owner_0, home_0, score_rhs(slot_0 + e))
        sbuf[e][pl.ds(cache, tok), :] = st
        mbuf[e][...] = fold_max(mbuf[e][...], st)
    kv_start(cache - raw_pos, raw_pos)

    def region(i, sc, sn, mc, mn, more=True):
        nxt = lax.rem(i + 1, n_pairs)
        f_n, slot_n, kv_n, owner_n, home_n = pair(nxt)
        second, slot, kv, _, _ = pair(i)
        later = jnp.minimum(i + 2, n_pairs - 1)
        ahead = pair(later)[1]

        @pl.when(among(i + 2, Q_PAIRS))
        def _():
            for e in range(2):
                pltpu.make_async_copy(qraw.at[ahead + e], qraw.at[ahead + e], q_recv.at[ahead + e]).wait()

        @pl.when(among(i + 1, KV_PAIRS))
        def _():
            for e in range(2):
                pltpu.make_async_copy(kbuf.at[kv_n + e], kbuf.at[kv_n + e], k_recv.at[kv_n + e - kvh]).wait()
                pltpu.make_async_copy(vbuf.at[kv_n + e], vbuf.at[kv_n + e], v_recv.at[kv_n + e - kvh]).wait()

        qv, m, decay, mx, l8, o = [], [], [], [None] * 2, [], [None] * 2
        for e in range(2):
            qv.append(score_rhs(slot_n + e) if more else None)
            m_old = jnp.where(second == 1, st_m[slot + e], -1e38)
            m.append(jnp.maximum(m_old, jnp.max(mc[e][...], axis=0, keepdims=True) * scale2))
            decay.append(jnp.exp2(m_old - m[e]))
            l8.append(jnp.zeros((8, rows), F32))
        for c in range(chunks):
            sl = pl.ds(c * TK, TK)
            for e in range(2):
                st = qk_tile(kv_n + e, f_n, c, qv[e]) if more else None
                p = jnp.exp2(sc[e][sl, :] * scale2 - m[e])
                if more:
                    sn[e][sl, :] = st
                    mx[e] = fold_max(mx[e], st)
                l8[e] = l8[e] + jnp.sum(p.reshape(TK // 8, 8, rows), axis=0)
                t = jnp.dot(vbuf[kv + e, :, sl], p.astype(BF), preferred_element_type=F32)
                o[e] = t if o[e] is None else o[e] + t
        sl = pl.ds(cache, tok)
        for e in range(2):
            p = jnp.exp2(sc[e][sl, :] * scale2 - m[e])
            if more:
                st = qk_new(kv_n + e, owner_n, home_n, qv[e])
                sn[e][sl, :] = st
                mn[e][...] = fold_max(mx[e], st)
            l8[e] = l8[e] + jnp.sum(p.reshape(tok // 8, 8, rows), axis=0)
            pb = jnp.concatenate([p.astype(BF), jnp.zeros((dim - tok, rows), BF)], axis=0)
            o[e] = o[e] + jnp.dot(vbuf[kv + e, :, pl.ds(cache, dim)], pb, preferred_element_type=F32)
        for e in range(2):
            st_o[slot + e] = jnp.where(second == 1, st_o[slot + e] * decay[e], 0.0) + o[e]
            st_l[slot + e] = jnp.where(second == 1, st_l[slot + e] * decay[e], 0.0) + jnp.sum(l8[e], axis=0, keepdims=True)
            st_m[slot + e] = m[e]
            if more:
                load_q(ahead + e)

    def partial_copies(u):
        return (pltpu.make_async_remote_copy(
                    src_ref=ps.at[u], dst_ref=pr.at[u], send_sem=p_send.at[0, u], recv_sem=p_recv.at[0, u],
                    device_id={'cp': far}, device_id_type=MESH),
                pltpu.make_async_remote_copy(
                    src_ref=psl.at[u], dst_ref=prl.at[u], send_sem=p_send.at[1, u], recv_sem=p_recv.at[1, u],
                    device_id={'cp': far}, device_id_type=MESH))

    def mate_out(u):
        hh = half * core + u - half
        return (pltpu.make_async_remote_copy(
                    src_ref=fo.at[u - half], dst_ref=out_ref.at[:, hh], send_sem=f_send.at[0, u - half],
                    recv_sem=f_recv.at[0, u - half], device_id={'cp': mate}, device_id_type=MESH),
                pltpu.make_async_remote_copy(
                    src_ref=fl.at[u - half], dst_ref=lse_ref.at[hh], send_sem=f_send.at[1, u - half],
                    recv_sem=f_recv.at[1, u - half], device_id={'cp': mate}, device_id_type=MESH))

    def finish(i):
        _, slot, _, _, _ = pair(i)

        @pl.when(among(i, R_PAIRS))
        def _():
            u = slot - 2 * half
            for e in range(2):
                l = st_l[slot + e]
                ps[u + e] = (st_o[slot + e] * (1.0 / l)).astype(BF)
                psl[u + e] = st_m[slot + e] + jnp.log2(l)
            for e in range(2):
                for cp in partial_copies(u + e):
                    cp.start()

        @pl.when(among(i, L_PAIRS))
        def _():
            u = slot
            for e in range(2):
                for cp in partial_copies(u + e):
                    cp.wait_recv()
            done = []
            for e in range(2):
                m_a, m_b = st_m[u + e], prl[u + e]
                m = jnp.maximum(m_a, m_b)
                a, b = jnp.exp2(m_a - m), jnp.exp2(m_b - m)
                l = st_l[u + e] * a + b
                inv = 1.0 / l
                o = st_o[u + e] * (a * inv) + pr[u + e].astype(F32) * (b * inv)
                done.append((o.T.astype(BF).reshape(tok, ratio, dim), (m + jnp.log2(l)) * math.log(2.0)))

            @pl.when(u < half)
            def _():
                for e in range(2):
                    out_ref[:, half * core + u + e] = done[e][0]
                    lse_ref[half * core + u + e] = done[e][1]

            @pl.when(u >= half)
            def _():
                for e in range(2):
                    fo[u - half + e] = done[e][0]
                    fl[u - half + e] = done[e][1]
                for e in range(2):
                    for cp in mate_out(u + e):
                        cp.start()

    def two(i, more):
        region(2 * i, sbuf[:2], sbuf[2:], mbuf[:2], mbuf[2:])
        finish(2 * i)
        region(2 * i + 1, sbuf[2:], sbuf[:2], mbuf[2:], mbuf[:2], more)
        finish(2 * i + 1)

    @pl.loop(0, n_pairs // 2 - 1)
    def _(i):
        two(i, True)

    two(jnp.int32(n_pairs // 2 - 1), False)

    for k in range(3):
        for h in range(half):
            q_copy(k, h).wait_send()
    for h in range(half):
        pltpu.make_async_copy(kbuf.at[h], kbuf.at[h], kv_send.at[0, h]).wait()
        pltpu.make_async_copy(vbuf.at[h], vbuf.at[h], kv_send.at[1, h]).wait()
    for u in range(2 * half):
        for cp in partial_copies(u):
            cp.wait_send()
    for u in range(half):
        for cp in mate_out(u + half):
            cp.wait_send()
            cp.wait_recv()


def place_kernel(out_ref, lse_ref, out_hbm, lse_hbm, lse_buf, sem):
    kvh, _, rows = lse_ref.shape
    tok, heads = lse_buf.shape
    ratio = heads // kvh
    write = pltpu.make_async_copy(out_ref, out_hbm, sem.at[0])
    write.start()
    x = lse_ref[...].reshape(kvh, rows)
    lane = lax.broadcasted_iota(jnp.int32, (kvh, heads), 1) // ratio
    head = lax.broadcasted_iota(jnp.int32, (kvh, heads), 0)
    per = heads // ratio
    blocks = [pltpu.roll(x[:, b * heads:(b + 1) * heads], 0, 1, stride=ratio, stride_axis=0) for b in range(tok // per)]
    for t in range(tok):
        turned = pltpu.roll(blocks[t // per], (heads - (t % per) * ratio) % heads, 1)
        lse_buf[pl.ds(t, 1), :] = jnp.sum(jnp.where(lane == head, turned, 0.0), axis=0, keepdims=True)
    lse_write = pltpu.make_async_copy(lse_buf, lse_hbm, sem.at[1])
    lse_write.start()
    write.wait()
    lse_write.wait()


def solution(mesh):
    tok_spec = P(('dp', 'cp'))

    def local(queries, key_new, value_new, key_cache, value_cache, prefix_len):
        tok, heads, dim = queries.shape
        cache, kvh = key_cache.shape[:2]
        ratio = heads // kvh
        half = kvh // 2
        rows = tok * ratio
        n_raw = 6
        dma = pltpu.SemaphoreType.DMA
        hbm = pl.BlockSpec(memory_space=pltpu.HBM)
        vmem = pl.BlockSpec(memory_space=pltpu.VMEM)
        scratch = [
            pltpu.VMEM((cache * kvh, dim), BF),
            pltpu.VMEM((cache * kvh, dim), BF),
            pltpu.VMEM((tok * kvh, dim), BF),
            pltpu.VMEM((tok * kvh, dim), BF),
            pltpu.VMEM((kvh + half, cache + tok, dim), BF),
            pltpu.VMEM((kvh + half, dim, cache + dim), BF),
            pltpu.VMEM((2, cache, dim), BF),
            pltpu.VMEM((4 * half, tok, ratio, dim), BF),
            pltpu.VMEM((4 * half, dim, rows), BF),
            pltpu.VMEM((dim, rows), BF),
            pltpu.SMEM((1,), jnp.int32),
            (pltpu.VMEM((cache + tok, rows), F32),) * 4,
            (pltpu.VMEM((8, rows), F32),) * 4,
            pltpu.VMEM((4 * half, dim, rows), F32),
            pltpu.VMEM((4 * half, 1, rows), F32),
            pltpu.VMEM((4 * half, 1, rows), F32),
            pltpu.VMEM((2 * half, dim, rows), BF),
            pltpu.VMEM((2 * half, 1, rows), F32),
            pltpu.VMEM((2 * half, dim, rows), BF),
            pltpu.VMEM((2 * half, 1, rows), F32),
            pltpu.VMEM((half, tok, ratio, dim), BF),
            pltpu.VMEM((half, 1, rows), F32),
            dma((2, n_raw)), dma((3,)), dma((3 * half,)), dma((4 * half,)), dma((2, half)), dma((half,)), dma((half,)),
            dma((2, 2 * half)), dma((2, 2 * half)), dma((2, half)), dma((2, half)),
        ]
        flops = 4 * heads * tok * 4 * cache * dim
        out, lse = pl.pallas_call(
            attend_kernel,
            out_shape=(pltpu.VMEM((tok, kvh, ratio, dim), BF), pltpu.VMEM((kvh, 1, rows), F32)),
            in_specs=[hbm] * 6,
            out_specs=(vmem, vmem),
            scratch_shapes=scratch,
            compiler_params=pltpu.CompilerParams(collective_id=0, has_side_effects=True, vmem_limit_bytes=60 * 2 ** 20),
            cost_estimate=pl.CostEstimate(flops=flops, bytes_accessed=4 * cache * kvh * dim, transcendentals=heads * tok * 4 * cache),
            name='attend',
        )(queries.reshape(tok, kvh, ratio, dim), key_new.reshape(tok * kvh, dim), value_new.reshape(tok * kvh, dim),
          key_cache.reshape(cache * kvh, dim), value_cache.reshape(cache * kvh, dim), prefix_len)
        out, row_lse = pl.pallas_call(
            place_kernel,
            out_shape=(jax.ShapeDtypeStruct((tok, heads, dim), BF), jax.ShapeDtypeStruct((tok, heads), F32)),
            in_specs=[vmem, vmem],
            out_specs=(hbm, hbm),
            scratch_shapes=[pltpu.VMEM((tok, heads), F32), dma((2,))],
            compiler_params=pltpu.CompilerParams(vmem_limit_bytes=2 * 2 ** 20),
            name='place',
        )(out.reshape(tok, heads, dim), lse)
        return out, row_lse

    return jax.shard_map(local, mesh=mesh, in_specs=(tok_spec, tok_spec, tok_spec, tok_spec, tok_spec, P('dp')),
                         out_specs=(tok_spec, tok_spec), check_vma=False)
```

```python
import functools
import math

import jax
import jax.numpy as jnp
from jax import lax
from jax.experimental import pallas as pl
from jax.experimental.pallas import tpu as pltpu
from jax.sharding import PartitionSpec as P

MESH = pl.DeviceIdType.MESH
BIG = 1e30
TK = 256
BF = jnp.bfloat16
SEQ = ((0, 0), (2, 0), (4, 0), (12, 0), (14, 0), (8, 0), (12, 1), (10, 0),
       (14, 1), (8, 1), (10, 1), (6, 0), (4, 1), (6, 1), (0, 1), (2, 1))
F32 = jnp.float32


def _packed(part):
    v = sum((slot // 2 + 8 * second) << (4 * k) for k, (slot, second) in enumerate(part))
    return v - (1 << 32) if v >= 1 << 31 else v


ORDER = (_packed(SEQ[:8]), _packed(SEQ[8:]))
Q_PAIRS = tuple(SEQ.index((s, 0)) for s in range(4, 16, 2))
KV_PAIRS = tuple(next(k for k, (s, f) in enumerate(SEQ) if f and s % 4 == h) for h in (0, 2))
R_PAIRS = tuple(k for k, (s, f) in enumerate(SEQ) if f and s >= 8)
L_PAIRS = tuple(k for k, (s, f) in enumerate(SEQ) if f and s < 8)


def among(i, ks):
    hit = i == ks[0]
    for k in ks[1:]:
        hit = jnp.logical_or(hit, i == k)
    return hit


def attend_kernel(q_hbm, kn_hbm, vn_hbm, kc_hbm, vc_hbm, plen_hbm, out_ref, lse_ref,
                  raw_k, raw_v, new_k, new_v, kbuf, vbuf, bias, qraw, qt, pick, plen, sbuf, mbuf,
                  st_o, st_m, st_l, ps, psl, pr, prl, fo, fl,
                  raw_sem, new_sem, q_send, q_recv, kv_send, k_recv, v_recv, p_send, p_recv, f_send, f_recv):
    tok, kvh, ratio, dim = q_hbm.shape
    cache = kc_hbm.shape[0] // kvh
    half = kvh // 2
    rows = tok * ratio
    n_raw = raw_sem.shape[1]
    raw_pos = cache // n_raw
    chunks = cache // TK
    scale2 = dim ** -0.5 * math.log2(math.e)

    me = lax.axis_index('cp')
    core = lax.rem(me, 2)
    chip2 = me - core
    mate = chip2 + 1 - core
    far = lax.rem(chip2 + 2, 4) + core
    far_other = lax.rem(chip2 + 2, 4) + 1 - core

    def raw_copy(j):
        sl = pl.ds(j * raw_pos * kvh, raw_pos * kvh)
        return (pltpu.make_async_copy(kc_hbm.at[sl], raw_k.at[sl], raw_sem.at[0, j]),
                pltpu.make_async_copy(vc_hbm.at[sl], raw_v.at[sl], raw_sem.at[1, j]))

    def own_q(h):
        return pltpu.make_async_copy(q_hbm.at[:, half * core + h], qraw.at[h], q_recv.at[h])

    for j in range(n_raw):
        a, b = raw_copy(j)
        a.start()
        b.start()
    plen_copy = pltpu.make_async_copy(plen_hbm, plen, new_sem.at[2])
    plen_copy.start()
    new_copies = (pltpu.make_async_copy(kn_hbm, new_k, new_sem.at[0]),
                  pltpu.make_async_copy(vn_hbm, new_v, new_sem.at[1]))
    for cp in new_copies:
        cp.start()
    for h in range(half):
        own_q(h).start()

    barrier = pltpu.get_barrier_semaphore()
    for peer in (mate, far, far_other):
        pl.semaphore_signal(barrier, inc=1, device_id={'cp': peer}, device_id_type=MESH)

    pick[...] = jnp.where(lax.broadcasted_iota(jnp.int32, (dim, rows), 0) == 0, 1.0, 0.0).astype(BF)
    for e in range(2):
        mbuf[e][...] = jnp.full((8, rows), -3e38, F32)

    pl.semaphore_wait(barrier, 3)

    def q_copy(k, h):
        peer, base = ((far_other, 3 * half), (far, 2 * half), (mate, half))[k]
        peer_core = (1 - core, core, 1 - core)[k]
        return pltpu.make_async_remote_copy(
            src_ref=q_hbm.at[:, half * peer_core + h], dst_ref=qraw.at[base + h],
            send_sem=q_send.at[k * half + h], recv_sem=q_recv.at[base + h],
            device_id={'cp': peer}, device_id_type=MESH)

    for k in range(3):
        for h in range(half):
            q_copy(k, h).start()

    plen_copy.wait()
    visible_len = plen[0]
    for f, owner in enumerate((me, mate)):
        @pl.loop(0, chunks)
        def _(j):
            lane = lax.broadcasted_iota(jnp.int32, (TK, dim), 1)
            pos = owner * cache + j * TK + lax.broadcasted_iota(jnp.int32, (TK, dim), 0)
            hidden = jnp.logical_and(lane == 0, pos >= visible_len)
            bias[f, pl.ds(pl.multiple_of(j * TK, TK), TK), :] = jnp.where(hidden, -BIG, 0.0).astype(BF)

    for cp in new_copies:
        cp.wait()
    kt = pltpu.einshape('phd->hpd', new_k[...].reshape(tok, kvh, dim))
    vt = pltpu.einshape('phd->hpd', new_v[...].reshape(tok, kvh, dim))
    for h in range(kvh):
        kbuf[h, pl.ds(cache, tok), :] = kt[h]
        vpad = jnp.concatenate([vt[h].astype(F32), jnp.zeros((dim - tok, dim), F32)], axis=0)
        vbuf[h, :, pl.ds(cache, dim)] = vpad.T.astype(BF)
    def kv_parts(h, lo, n):
        src = half * (1 - core) + h
        to = dict(device_id={'cp': mate}, device_id_type=MESH)
        k_rows, v_lanes = pl.ds(lo, tok if n == dim else n), pl.ds(lo, n)
        return (pltpu.make_async_remote_copy(
                    src_ref=kbuf.at[src, k_rows], dst_ref=kbuf.at[kvh + h, k_rows],
                    send_sem=kv_send.at[0, h], recv_sem=k_recv.at[h], **to),
                pltpu.make_async_remote_copy(
                    src_ref=vbuf.at[src, :, v_lanes], dst_ref=vbuf.at[kvh + h, :, v_lanes],
                    send_sem=kv_send.at[1, h], recv_sem=v_recv.at[h], **to))

    def kv_start(lo, n):
        for h in range(half):
            for cp in kv_parts(h, lo, n):
                cp.start()

    n_pairs = 4 * half

    def pair(i):
        code = lax.shift_right_logical(jnp.where(i < 8, ORDER[0], ORDER[1]), 4 * lax.rem(i, 8))
        slot = 2 * jnp.bitwise_and(code, 7)
        second = lax.div(jnp.bitwise_and(code, 15), 8)
        h = lax.rem(slot, half)
        kv = jnp.where(second == 1, kvh + h, half * core + h)
        owner = jnp.where(second == 1, mate, me)
        src = lax.div(slot, half)
        home = jnp.where(src == 0, me, jnp.where(src == 1, mate, jnp.where(src == 2, far, far_other)))
        return second, slot, kv, owner, home

    def load_q(slot):
        qt[slot] = qraw[slot].reshape(rows, dim).T

    def score_rhs(slot):
        return jnp.concatenate([qt[slot], pick[...]], axis=0)

    def qk_tile(kv, f, c, qv):
        sl = pl.ds(c * TK if isinstance(c, int) else pl.multiple_of(c * TK, TK), TK)
        lhs = jnp.concatenate([kbuf[kv, sl, :], bias[f, sl, :]], axis=1)
        return jnp.dot(lhs, qv, preferred_element_type=F32)

    def qk_new(kv, owner, home, qv):
        lhs = jnp.concatenate([kbuf[kv, pl.ds(cache, tok), :], jnp.zeros((tok, dim), BF)], axis=1)
        st = jnp.dot(lhs, qv, preferred_element_type=F32)
        key = owner * tok + lax.broadcasted_iota(jnp.int32, (tok, rows), 0)
        query = home * tok + lax.broadcasted_iota(jnp.int32, (tok, rows), 1) // ratio
        return jnp.where(key <= query, st, -BIG)

    def fold_max(mx, st):
        t = jnp.max(st.reshape(st.shape[0] // 8, 8, rows), axis=0)
        return t if mx is None else jnp.maximum(mx, t)

    def prepare(c):
        base = pl.multiple_of(c * TK, TK)
        src = pl.ds(pl.multiple_of(base * kvh, TK * kvh), TK * kvh)
        xk = pltpu.einshape('phd->hpd', raw_k[src, :].reshape(TK, kvh, dim))
        xv = pltpu.einshape('phd->hpd', raw_v[src, :].reshape(TK, kvh, dim))
        for h in range(kvh):
            kbuf[h, pl.ds(base, TK), :] = xk[h]
            vbuf[h, :, pl.ds(base, TK)] = xv[h].T

    f_0, slot_0, kv_0, owner_0, home_0 = pair(0)

    def first_scores(c):
        for e in range(2):
            st = qk_tile(kv_0 + e, f_0, c, score_rhs(slot_0 + e))
            sbuf[e][pl.ds(pl.multiple_of(c * TK, TK), TK), :] = st
            mbuf[e][...] = fold_max(mbuf[e][...], st)

    per_raw = raw_pos // TK
    for h in range(half):
        own_q(h).wait()
    for h in range(half):
        load_q(h)
    for cp in raw_copy(0):
        cp.wait()
    kv_start(cache, dim)
    prepare(0)

    @pl.loop(1, chunks)
    def _(c):
        @pl.when(lax.rem(c, per_raw) == 0)
        def _():
            j = lax.div(c, per_raw)
            for cp in raw_copy(j):
                cp.wait()

            @pl.when(j >= 2)
            def _():
                kv_start(pl.multiple_of((j - 2) * raw_pos, raw_pos), raw_pos)

        first_scores(c - 1)
        prepare(c)

    kv_start(cache - 2 * raw_pos, raw_pos)
    first_scores(chunks - 1)
    for e in range(2):
        st = qk_new(kv_0 + e, owner_0, home_0, score_rhs(slot_0 + e))
        sbuf[e][pl.ds(cache, tok), :] = st
        mbuf[e][...] = fold_max(mbuf[e][...], st)
    kv_start(cache - raw_pos, raw_pos)

    def region(i, sc, sn, mc, mn, more=True):
        nxt = lax.rem(i + 1, n_pairs)
        f_n, slot_n, kv_n, owner_n, home_n = pair(nxt)
        second, slot, kv, _, _ = pair(i)
        later = jnp.minimum(i + 2, n_pairs - 1)
        ahead = pair(later)[1]

        @pl.when(among(i + 2, Q_PAIRS))
        def _():
            for e in range(2):
                pltpu.make_async_copy(qraw.at[ahead + e], qraw.at[ahead + e], q_recv.at[ahead + e]).wait()

        @pl.when(among(i + 1, KV_PAIRS))
        def _():
            for e in range(2):
                pltpu.make_async_copy(kbuf.at[kv_n + e], kbuf.at[kv_n + e], k_recv.at[kv_n + e - kvh]).wait()
                pltpu.make_async_copy(vbuf.at[kv_n + e], vbuf.at[kv_n + e], v_recv.at[kv_n + e - kvh]).wait()

        qv, m, decay, mx, l8, o = [], [], [], [None] * 2, [], [None] * 2
        for e in range(2):
            qv.append(score_rhs(slot_n + e) if more else None)
            m_old = jnp.where(second == 1, st_m[slot + e], -1e38)
            m.append(jnp.maximum(m_old, jnp.max(mc[e][...], axis=0, keepdims=True) * scale2))
            decay.append(jnp.exp2(m_old - m[e]))
            l8.append(jnp.zeros((8, rows), F32))
        for c in range(chunks):
            sl = pl.ds(c * TK, TK)
            for e in range(2):
                st = qk_tile(kv_n + e, f_n, c, qv[e]) if more else None
                p = jnp.exp2(sc[e][sl, :] * scale2 - m[e])
                if more:
                    sn[e][sl, :] = st
                    mx[e] = fold_max(mx[e], st)
                l8[e] = l8[e] + jnp.sum(p.reshape(TK // 8, 8, rows), axis=0)
                t = jnp.dot(vbuf[kv + e, :, sl], p.astype(BF), preferred_element_type=F32)
                o[e] = t if o[e] is None else o[e] + t
        sl = pl.ds(cache, tok)
        for e in range(2):
            p = jnp.exp2(sc[e][sl, :] * scale2 - m[e])
            if more:
                st = qk_new(kv_n + e, owner_n, home_n, qv[e])
                sn[e][sl, :] = st
                mn[e][...] = fold_max(mx[e], st)
            l8[e] = l8[e] + jnp.sum(p.reshape(tok // 8, 8, rows), axis=0)
            pb = jnp.concatenate([p.astype(BF), jnp.zeros((dim - tok, rows), BF)], axis=0)
            o[e] = o[e] + jnp.dot(vbuf[kv + e, :, pl.ds(cache, dim)], pb, preferred_element_type=F32)
        for e in range(2):
            st_o[slot + e] = jnp.where(second == 1, st_o[slot + e] * decay[e], 0.0) + o[e]
            st_l[slot + e] = jnp.where(second == 1, st_l[slot + e] * decay[e], 0.0) + jnp.sum(l8[e], axis=0, keepdims=True)
            st_m[slot + e] = m[e]
            if more:
                load_q(ahead + e)

    def partial_copies(u):
        return (pltpu.make_async_remote_copy(
                    src_ref=ps.at[u], dst_ref=pr.at[u], send_sem=p_send.at[0, u], recv_sem=p_recv.at[0, u],
                    device_id={'cp': far}, device_id_type=MESH),
                pltpu.make_async_remote_copy(
                    src_ref=psl.at[u], dst_ref=prl.at[u], send_sem=p_send.at[1, u], recv_sem=p_recv.at[1, u],
                    device_id={'cp': far}, device_id_type=MESH))

    def mate_out(u):
        hh = half * core + u - half
        return (pltpu.make_async_remote_copy(
                    src_ref=fo.at[u - half], dst_ref=out_ref.at[:, hh], send_sem=f_send.at[0, u - half],
                    recv_sem=f_recv.at[0, u - half], device_id={'cp': mate}, device_id_type=MESH),
                pltpu.make_async_remote_copy(
                    src_ref=fl.at[u - half], dst_ref=lse_ref.at[hh], send_sem=f_send.at[1, u - half],
                    recv_sem=f_recv.at[1, u - half], device_id={'cp': mate}, device_id_type=MESH))

    def finish(i):
        _, slot, _, _, _ = pair(i)

        @pl.when(among(i, R_PAIRS))
        def _():
            u = slot - 2 * half
            for e in range(2):
                l = st_l[slot + e]
                ps[u + e] = (st_o[slot + e] * (1.0 / l)).astype(BF)
                psl[u + e] = st_m[slot + e] + jnp.log2(l)
            for e in range(2):
                for cp in partial_copies(u + e):
                    cp.start()

        @pl.when(among(i, L_PAIRS))
        def _():
            u = slot
            for e in range(2):
                for cp in partial_copies(u + e):
                    cp.wait_recv()
            done = []
            for e in range(2):
                m_a, m_b = st_m[u + e], prl[u + e]
                m = jnp.maximum(m_a, m_b)
                a, b = jnp.exp2(m_a - m), jnp.exp2(m_b - m)
                l = st_l[u + e] * a + b
                inv = 1.0 / l
                o = st_o[u + e] * (a * inv) + pr[u + e].astype(F32) * (b * inv)
                done.append((o.T.astype(BF).reshape(tok, ratio, dim), (m + jnp.log2(l)) * math.log(2.0)))

            @pl.when(u < half)
            def _():
                for e in range(2):
                    out_ref[:, half * core + u + e] = done[e][0]
                    lse_ref[half * core + u + e] = done[e][1]

            @pl.when(u >= half)
            def _():
                for e in range(2):
                    fo[u - half + e] = done[e][0]
                    fl[u - half + e] = done[e][1]
                for e in range(2):
                    for cp in mate_out(u + e):
                        cp.start()

    def two(i, more):
        region(2 * i, sbuf[:2], sbuf[2:], mbuf[:2], mbuf[2:])
        finish(2 * i)
        region(2 * i + 1, sbuf[2:], sbuf[:2], mbuf[2:], mbuf[:2], more)
        finish(2 * i + 1)

    @pl.loop(0, n_pairs // 2 - 1)
    def _(i):
        two(i, True)

    two(jnp.int32(n_pairs // 2 - 1), False)

    for k in range(3):
        for h in range(half):
            q_copy(k, h).wait_send()
    for h in range(half):
        pltpu.make_async_copy(kbuf.at[h], kbuf.at[h], kv_send.at[0, h]).wait()
        pltpu.make_async_copy(vbuf.at[h], vbuf.at[h], kv_send.at[1, h]).wait()
    for u in range(2 * half):
        for cp in partial_copies(u):
            cp.wait_send()
    for u in range(half):
        for cp in mate_out(u + half):
            cp.wait_send()
            cp.wait_recv()


def place_kernel(out_ref, lse_ref, out_hbm, lse_hbm, lse_buf, sem):
    kvh, _, rows = lse_ref.shape
    tok, heads = lse_buf.shape
    ratio = heads // kvh
    write = pltpu.make_async_copy(out_ref, out_hbm, sem.at[0])
    write.start()
    x = lse_ref[...].reshape(kvh, rows)
    lane = lax.broadcasted_iota(jnp.int32, (kvh, heads), 1) // ratio
    head = lax.broadcasted_iota(jnp.int32, (kvh, heads), 0)
    per = heads // ratio
    blocks = [pltpu.roll(x[:, b * heads:(b + 1) * heads], 0, 1, stride=ratio, stride_axis=0) for b in range(tok // per)]
    for t in range(tok):
        turned = pltpu.roll(blocks[t // per], (heads - (t % per) * ratio) % heads, 1)
        lse_buf[pl.ds(t, 1), :] = jnp.sum(jnp.where(lane == head, turned, 0.0), axis=0, keepdims=True)
    lse_write = pltpu.make_async_copy(lse_buf, lse_hbm, sem.at[1])
    lse_write.start()
    write.wait()
    lse_write.wait()


def solution(mesh):
    tok_spec = P(('dp', 'cp'))

    def local(queries, key_new, value_new, key_cache, value_cache, prefix_len):
        tok, heads, dim = queries.shape
        cache, kvh = key_cache.shape[:2]
        ratio = heads // kvh
        half = kvh // 2
        rows = tok * ratio
        n_raw = 6
        dma = pltpu.SemaphoreType.DMA
        hbm = pl.BlockSpec(memory_space=pltpu.HBM)
        vmem = pl.BlockSpec(memory_space=pltpu.VMEM)
        scratch = [
            pltpu.VMEM((cache * kvh, dim), BF),
            pltpu.VMEM((cache * kvh, dim), BF),
            pltpu.VMEM((tok * kvh, dim), BF),
            pltpu.VMEM((tok * kvh, dim), BF),
            pltpu.VMEM((kvh + half, cache + tok, dim), BF),
            pltpu.VMEM((kvh + half, dim, cache + dim), BF),
            pltpu.VMEM((2, cache, dim), BF),
            pltpu.VMEM((4 * half, tok, ratio, dim), BF),
            pltpu.VMEM((4 * half, dim, rows), BF),
            pltpu.VMEM((dim, rows), BF),
            pltpu.SMEM((1,), jnp.int32),
            (pltpu.VMEM((cache + tok, rows), F32),) * 4,
            (pltpu.VMEM((8, rows), F32),) * 4,
            pltpu.VMEM((4 * half, dim, rows), F32),
            pltpu.VMEM((4 * half, 1, rows), F32),
            pltpu.VMEM((4 * half, 1, rows), F32),
            pltpu.VMEM((2 * half, dim, rows), BF),
            pltpu.VMEM((2 * half, 1, rows), F32),
            pltpu.VMEM((2 * half, dim, rows), BF),
            pltpu.VMEM((2 * half, 1, rows), F32),
            pltpu.VMEM((half, tok, ratio, dim), BF),
            pltpu.VMEM((half, 1, rows), F32),
            dma((2, n_raw)), dma((3,)), dma((3 * half,)), dma((4 * half,)), dma((2, half)), dma((half,)), dma((half,)),
            dma((2, 2 * half)), dma((2, 2 * half)), dma((2, half)), dma((2, half)),
        ]
        flops = 4 * heads * tok * 4 * cache * dim
        out, lse = pl.pallas_call(
            attend_kernel,
            out_shape=(pltpu.VMEM((tok, kvh, ratio, dim), BF), pltpu.VMEM((kvh, 1, rows), F32)),
            in_specs=[hbm] * 6,
            out_specs=(vmem, vmem),
            scratch_shapes=scratch,
            compiler_params=pltpu.CompilerParams(collective_id=0, has_side_effects=True, vmem_limit_bytes=60 * 2 ** 20),
            cost_estimate=pl.CostEstimate(flops=flops, bytes_accessed=4 * cache * kvh * dim, transcendentals=heads * tok * 4 * cache),
            name='attend',
        )(queries.reshape(tok, kvh, ratio, dim), key_new.reshape(tok * kvh, dim), value_new.reshape(tok * kvh, dim),
          key_cache.reshape(cache * kvh, dim), value_cache.reshape(cache * kvh, dim), prefix_len)
        out, row_lse = pl.pallas_call(
            place_kernel,
            out_shape=(jax.ShapeDtypeStruct((tok, heads, dim), BF), jax.ShapeDtypeStruct((tok, heads), F32)),
            in_specs=[vmem, vmem],
            out_specs=(hbm, hbm),
            scratch_shapes=[pltpu.VMEM((tok, heads), F32), dma((2,))],
            compiler_params=pltpu.CompilerParams(vmem_limit_bytes=2 * 2 ** 20),
            name='place',
        )(out.reshape(tok, heads, dim), lse)
        return out, row_lse

    return jax.shard_map(local, mesh=mesh, in_specs=(tok_spec, tok_spec, tok_spec, tok_spec, tok_spec, P('dp')),
                         out_specs=(tok_spec, tok_spec), check_vma=False)
```

```python
import functools
import math

import jax
import jax.numpy as jnp
from jax import lax
from jax.experimental import pallas as pl
from jax.experimental.pallas import tpu as pltpu
from jax.sharding import PartitionSpec as P

MESH = pl.DeviceIdType.MESH
BIG = 1e30
TK = 256
PREP = 128
BF = jnp.bfloat16
SEQ = ((0, 0), (2, 0), (4, 0), (12, 0), (14, 0), (12, 1), (8, 0), (14, 1),
       (10, 0), (8, 1), (10, 1), (6, 0), (4, 1), (6, 1), (0, 1), (2, 1))
F32 = jnp.float32


def _packed(part):
    v = sum((slot // 2 + 8 * second) << (4 * k) for k, (slot, second) in enumerate(part))
    return v - (1 << 32) if v >= 1 << 31 else v


ORDER = (_packed(SEQ[:8]), _packed(SEQ[8:]))
Q_PAIRS = tuple(SEQ.index((s, 0)) for s in range(4, 16, 2))
KV_PAIRS = tuple(next(k for k, (s, f) in enumerate(SEQ) if f and s % 4 == h) for h in (0, 2))
R_PAIRS = tuple(k for k, (s, f) in enumerate(SEQ) if f and s >= 8)
L_PAIRS = tuple(k for k, (s, f) in enumerate(SEQ) if f and s < 8)


def among(i, ks):
    hit = i == ks[0]
    for k in ks[1:]:
        hit = jnp.logical_or(hit, i == k)
    return hit


def attend_kernel(q_hbm, kn_hbm, vn_hbm, kc_hbm, vc_hbm, plen_hbm, out_ref, lse_ref,
                  raw_k, raw_v, new_k, new_v, kbuf, vbuf, bias, qraw, qt, pick, plen, sbuf, mbuf,
                  st_o, st_m, st_l, ps, psl, pr, prl, fo, fl,
                  raw_sem, new_sem, q_send, q_recv, kv_send, k_recv, v_recv, p_send, p_recv, f_send, f_recv):
    tok, kvh, ratio, dim = q_hbm.shape
    cache = kc_hbm.shape[0] // kvh
    half = kvh // 2
    rows = tok * ratio
    n_raw = raw_sem.shape[1]
    raw_pos = cache // n_raw
    chunks = cache // TK
    scale2 = dim ** -0.5 * math.log2(math.e)

    me = lax.axis_index('cp')
    core = lax.rem(me, 2)
    chip2 = me - core
    mate = chip2 + 1 - core
    far = lax.rem(chip2 + 2, 4) + core
    far_other = lax.rem(chip2 + 2, 4) + 1 - core

    def raw_copy(j):
        sl = pl.ds(j * raw_pos * kvh, raw_pos * kvh)
        return (pltpu.make_async_copy(kc_hbm.at[sl], raw_k.at[sl], raw_sem.at[0, j]),
                pltpu.make_async_copy(vc_hbm.at[sl], raw_v.at[sl], raw_sem.at[1, j]))

    def own_q(h):
        return pltpu.make_async_copy(q_hbm.at[:, half * core + h], qraw.at[h], q_recv.at[h])

    for j in range(n_raw):
        a, b = raw_copy(j)
        a.start()
        b.start()
    plen_copy = pltpu.make_async_copy(plen_hbm, plen, new_sem.at[2])
    plen_copy.start()
    new_copies = (pltpu.make_async_copy(kn_hbm, new_k, new_sem.at[0]),
                  pltpu.make_async_copy(vn_hbm, new_v, new_sem.at[1]))
    for cp in new_copies:
        cp.start()
    for h in range(half):
        own_q(h).start()

    barrier = pltpu.get_barrier_semaphore()
    for peer in (mate, far, far_other):
        pl.semaphore_signal(barrier, inc=1, device_id={'cp': peer}, device_id_type=MESH)

    pick[...] = jnp.where(lax.broadcasted_iota(jnp.int32, (dim, rows), 0) == 0, 1.0, 0.0).astype(BF)
    for e in range(2):
        mbuf[e][...] = jnp.full((8, rows), -3e38, F32)

    pl.semaphore_wait(barrier, 3)

    def q_copy(k, h):
        peer, base = ((far_other, 3 * half), (far, 2 * half), (mate, half))[k]
        peer_core = (1 - core, core, 1 - core)[k]
        return pltpu.make_async_remote_copy(
            src_ref=q_hbm.at[:, half * peer_core + h], dst_ref=qraw.at[base + h],
            send_sem=q_send.at[k * half + h], recv_sem=q_recv.at[base + h],
            device_id={'cp': peer}, device_id_type=MESH)

    for k in range(3):
        for h in range(half):
            q_copy(k, h).start()

    plen_copy.wait()
    visible_len = plen[0]
    for f, owner in enumerate((me, mate)):
        @pl.loop(0, chunks)
        def _(j):
            lane = lax.broadcasted_iota(jnp.int32, (TK, dim), 1)
            pos = owner * cache + j * TK + lax.broadcasted_iota(jnp.int32, (TK, dim), 0)
            hidden = jnp.logical_and(lane == 0, pos >= visible_len)
            bias[f, pl.ds(pl.multiple_of(j * TK, TK), TK), :] = jnp.where(hidden, -BIG, 0.0).astype(BF)

    for cp in new_copies:
        cp.wait()
    kt = pltpu.einshape('phd->hpd', new_k[...].reshape(tok, kvh, dim))
    vt = pltpu.einshape('phd->hpd', new_v[...].reshape(tok, kvh, dim))
    for h in range(kvh):
        kbuf[h, pl.ds(cache, tok), :] = kt[h]
        vpad = jnp.concatenate([vt[h].astype(F32), jnp.zeros((dim - tok, dim), F32)], axis=0)
        vbuf[h, :, pl.ds(cache, dim)] = vpad.T.astype(BF)
    def kv_parts(h, lo, n):
        src = half * (1 - core) + h
        to = dict(device_id={'cp': mate}, device_id_type=MESH)
        k_rows, v_lanes = pl.ds(lo, tok if n == dim else n), pl.ds(lo, n)
        return (pltpu.make_async_remote_copy(
                    src_ref=kbuf.at[src, k_rows], dst_ref=kbuf.at[kvh + h, k_rows],
                    send_sem=kv_send.at[0, h], recv_sem=k_recv.at[h], **to),
                pltpu.make_async_remote_copy(
                    src_ref=vbuf.at[src, :, v_lanes], dst_ref=vbuf.at[kvh + h, :, v_lanes],
                    send_sem=kv_send.at[1, h], recv_sem=v_recv.at[h], **to))

    def kv_start(lo, n):
        for h in range(half):
            for cp in kv_parts(h, lo, n):
                cp.start()

    n_pairs = 4 * half

    def pair(i):
        code = lax.shift_right_logical(jnp.where(i < 8, ORDER[0], ORDER[1]), 4 * lax.rem(i, 8))
        slot = 2 * jnp.bitwise_and(code, 7)
        second = lax.div(jnp.bitwise_and(code, 15), 8)
        h = lax.rem(slot, half)
        kv = jnp.where(second == 1, kvh + h, half * core + h)
        owner = jnp.where(second == 1, mate, me)
        src = lax.div(slot, half)
        home = jnp.where(src == 0, me, jnp.where(src == 1, mate, jnp.where(src == 2, far, far_other)))
        return second, slot, kv, owner, home

    def load_q(slot):
        qt[slot] = qraw[slot].reshape(rows, dim).T

    def score_rhs(slot):
        return jnp.concatenate([qt[slot], pick[...]], axis=0)

    def qk_tile(kv, f, c, qv):
        sl = pl.ds(c * TK if isinstance(c, int) else pl.multiple_of(c * TK, TK), TK)
        lhs = jnp.concatenate([kbuf[kv, sl, :], bias[f, sl, :]], axis=1)
        return jnp.dot(lhs, qv, preferred_element_type=F32)

    def qk_new(kv, owner, home, qv):
        lhs = jnp.concatenate([kbuf[kv, pl.ds(cache, tok), :], jnp.zeros((tok, dim), BF)], axis=1)
        st = jnp.dot(lhs, qv, preferred_element_type=F32)
        key = owner * tok + lax.broadcasted_iota(jnp.int32, (tok, rows), 0)
        query = home * tok + lax.broadcasted_iota(jnp.int32, (tok, rows), 1) // ratio
        return jnp.where(key <= query, st, -BIG)

    def fold_max(mx, st):
        t = jnp.max(st.reshape(st.shape[0] // 8, 8, rows), axis=0)
        return t if mx is None else jnp.maximum(mx, t)

    f_0, slot_0, kv_0, owner_0, home_0 = pair(0)

    def first_scores(c):
        for e in range(2):
            st = qk_tile(kv_0 + e, f_0, c, score_rhs(slot_0 + e))
            sbuf[e][pl.ds(c * TK, TK), :] = st
            mbuf[e][...] = fold_max(mbuf[e][...], st)

    for j in range(n_raw):
        for cp in raw_copy(j):
            cp.wait()

        @pl.loop(0, raw_pos // PREP)
        def _(i):
            base = pl.multiple_of(j * raw_pos + i * PREP, PREP)
            src = pl.ds(pl.multiple_of(base * kvh, PREP * kvh), PREP * kvh)
            xk = pltpu.einshape('phd->hpd', raw_k[src, :].reshape(PREP, kvh, dim))
            xv = pltpu.einshape('phd->hpd', raw_v[src, :].reshape(PREP, kvh, dim))
            for h in range(kvh):
                kbuf[h, pl.ds(base, PREP), :] = xk[h]
                vbuf[h, :, pl.ds(base, PREP)] = xv[h].T

        if j == 0:
            kv_start(cache, dim)
        else:
            kv_start((j - 1) * raw_pos, raw_pos)

    for h in range(half):
        own_q(h).wait()
    for h in range(half):
        load_q(h)
    for c in range(chunks):
        first_scores(c)
    for e in range(2):
        st = qk_new(kv_0 + e, owner_0, home_0, score_rhs(slot_0 + e))
        sbuf[e][pl.ds(cache, tok), :] = st
        mbuf[e][...] = fold_max(mbuf[e][...], st)
    kv_start(cache - raw_pos, raw_pos)

    def region(i, sc, sn, mc, mn, more=True):
        nxt = lax.rem(i + 1, n_pairs)
        f_n, slot_n, kv_n, owner_n, home_n = pair(nxt)
        second, slot, kv, _, _ = pair(i)
        later = jnp.minimum(i + 2, n_pairs - 1)
        ahead = pair(later)[1]

        @pl.when(among(i + 2, Q_PAIRS))
        def _():
            for e in range(2):
                pltpu.make_async_copy(qraw.at[ahead + e], qraw.at[ahead + e], q_recv.at[ahead + e]).wait()

        @pl.when(among(i + 1, KV_PAIRS))
        def _():
            for e in range(2):
                pltpu.make_async_copy(kbuf.at[kv_n + e], kbuf.at[kv_n + e], k_recv.at[kv_n + e - kvh]).wait()
                pltpu.make_async_copy(vbuf.at[kv_n + e], vbuf.at[kv_n + e], v_recv.at[kv_n + e - kvh]).wait()

        qv, m, decay, mx, l8, o = [], [], [], [None] * 2, [], [None] * 2
        for e in range(2):
            qv.append(score_rhs(slot_n + e) if more else None)
            m_old = jnp.where(second == 1, st_m[slot + e], -1e38)
            m.append(jnp.maximum(m_old, jnp.max(mc[e][...], axis=0, keepdims=True) * scale2))
            decay.append(jnp.exp2(m_old - m[e]))
            l8.append(jnp.zeros((8, rows), F32))
        for c in range(chunks):
            sl = pl.ds(c * TK, TK)
            for e in range(2):
                st = qk_tile(kv_n + e, f_n, c, qv[e]) if more else None
                p = jnp.exp2(sc[e][sl, :] * scale2 - m[e])
                if more:
                    sn[e][sl, :] = st
                    mx[e] = fold_max(mx[e], st)
                l8[e] = l8[e] + jnp.sum(p.reshape(TK // 8, 8, rows), axis=0)
                t = jnp.dot(vbuf[kv + e, :, sl], p.astype(BF), preferred_element_type=F32)
                o[e] = t if o[e] is None else o[e] + t
        sl = pl.ds(cache, tok)
        for e in range(2):
            p = jnp.exp2(sc[e][sl, :] * scale2 - m[e])
            if more:
                st = qk_new(kv_n + e, owner_n, home_n, qv[e])
                sn[e][sl, :] = st
                mn[e][...] = fold_max(mx[e], st)
            l8[e] = l8[e] + jnp.sum(p.reshape(tok // 8, 8, rows), axis=0)
            pb = jnp.concatenate([p.astype(BF), jnp.zeros((dim - tok, rows), BF)], axis=0)
            o[e] = o[e] + jnp.dot(vbuf[kv + e, :, pl.ds(cache, dim)], pb, preferred_element_type=F32)
        for e in range(2):
            st_o[slot + e] = jnp.where(second == 1, st_o[slot + e] * decay[e], 0.0) + o[e]
            st_l[slot + e] = jnp.where(second == 1, st_l[slot + e] * decay[e], 0.0) + jnp.sum(l8[e], axis=0, keepdims=True)
            st_m[slot + e] = m[e]
            if more:
                load_q(ahead + e)

    def partial_copies(u):
        return (pltpu.make_async_remote_copy(
                    src_ref=ps.at[u], dst_ref=pr.at[u], send_sem=p_send.at[0, u], recv_sem=p_recv.at[0, u],
                    device_id={'cp': far}, device_id_type=MESH),
                pltpu.make_async_remote_copy(
                    src_ref=psl.at[u], dst_ref=prl.at[u], send_sem=p_send.at[1, u], recv_sem=p_recv.at[1, u],
                    device_id={'cp': far}, device_id_type=MESH))

    def mate_out(u):
        hh = half * core + u - half
        return (pltpu.make_async_remote_copy(
                    src_ref=fo.at[u - half], dst_ref=out_ref.at[:, hh], send_sem=f_send.at[0, u - half],
                    recv_sem=f_recv.at[0, u - half], device_id={'cp': mate}, device_id_type=MESH),
                pltpu.make_async_remote_copy(
                    src_ref=fl.at[u - half], dst_ref=lse_ref.at[hh], send_sem=f_send.at[1, u - half],
                    recv_sem=f_recv.at[1, u - half], device_id={'cp': mate}, device_id_type=MESH))

    def finish(i):
        _, slot, _, _, _ = pair(i)

        @pl.when(among(i, R_PAIRS))
        def _():
            u = slot - 2 * half
            for e in range(2):
                l = st_l[slot + e]
                ps[u + e] = (st_o[slot + e] * (1.0 / l)).astype(BF)
                psl[u + e] = st_m[slot + e] + jnp.log2(l)
            for e in range(2):
                for cp in partial_copies(u + e):
                    cp.start()

        @pl.when(among(i, L_PAIRS))
        def _():
            u = slot
            for e in range(2):
                for cp in partial_copies(u + e):
                    cp.wait_recv()
            done = []
            for e in range(2):
                m_a, m_b = st_m[u + e], prl[u + e]
                m = jnp.maximum(m_a, m_b)
                a, b = jnp.exp2(m_a - m), jnp.exp2(m_b - m)
                l = st_l[u + e] * a + b
                inv = 1.0 / l
                o = st_o[u + e] * (a * inv) + pr[u + e].astype(F32) * (b * inv)
                done.append((o.T.astype(BF).reshape(tok, ratio, dim), (m + jnp.log2(l)) * math.log(2.0)))

            @pl.when(u < half)
            def _():
                for e in range(2):
                    out_ref[:, half * core + u + e] = done[e][0]
                    lse_ref[half * core + u + e] = done[e][1]

            @pl.when(u >= half)
            def _():
                for e in range(2):
                    fo[u - half + e] = done[e][0]
                    fl[u - half + e] = done[e][1]
                for e in range(2):
                    for cp in mate_out(u + e):
                        cp.start()

    def two(i, more):
        region(2 * i, sbuf[:2], sbuf[2:], mbuf[:2], mbuf[2:])
        finish(2 * i)
        region(2 * i + 1, sbuf[2:], sbuf[:2], mbuf[2:], mbuf[:2], more)
        finish(2 * i + 1)

    @pl.loop(0, n_pairs // 2 - 1)
    def _(i):
        two(i, True)

    two(jnp.int32(n_pairs // 2 - 1), False)

    for k in range(3):
        for h in range(half):
            q_copy(k, h).wait_send()
    for h in range(half):
        pltpu.make_async_copy(kbuf.at[h], kbuf.at[h], kv_send.at[0, h]).wait()
        pltpu.make_async_copy(vbuf.at[h], vbuf.at[h], kv_send.at[1, h]).wait()
    for u in range(2 * half):
        for cp in partial_copies(u):
            cp.wait_send()
    for u in range(half):
        for cp in mate_out(u + half):
            cp.wait_send()
            cp.wait_recv()


def place_kernel(out_ref, lse_ref, out_hbm, lse_hbm, lse_buf, sem):
    kvh, _, rows = lse_ref.shape
    tok, heads = lse_buf.shape
    ratio = heads // kvh
    write = pltpu.make_async_copy(out_ref, out_hbm, sem.at[0])
    write.start()
    x = lse_ref[...].reshape(kvh, rows)
    lane = lax.broadcasted_iota(jnp.int32, (kvh, heads), 1) // ratio
    head = lax.broadcasted_iota(jnp.int32, (kvh, heads), 0)
    per = heads // ratio
    blocks = [pltpu.roll(x[:, b * heads:(b + 1) * heads], 0, 1, stride=ratio, stride_axis=0) for b in range(tok // per)]
    for t in range(tok):
        turned = pltpu.roll(blocks[t // per], (heads - (t % per) * ratio) % heads, 1)
        lse_buf[pl.ds(t, 1), :] = jnp.sum(jnp.where(lane == head, turned, 0.0), axis=0, keepdims=True)
    lse_write = pltpu.make_async_copy(lse_buf, lse_hbm, sem.at[1])
    lse_write.start()
    write.wait()
    lse_write.wait()


def solution(mesh):
    tok_spec = P(('dp', 'cp'))

    def local(queries, key_new, value_new, key_cache, value_cache, prefix_len):
        tok, heads, dim = queries.shape
        cache, kvh = key_cache.shape[:2]
        ratio = heads // kvh
        half = kvh // 2
        rows = tok * ratio
        n_raw = 6
        dma = pltpu.SemaphoreType.DMA
        hbm = pl.BlockSpec(memory_space=pltpu.HBM)
        vmem = pl.BlockSpec(memory_space=pltpu.VMEM)
        scratch = [
            pltpu.VMEM((cache * kvh, dim), BF),
            pltpu.VMEM((cache * kvh, dim), BF),
            pltpu.VMEM((tok * kvh, dim), BF),
            pltpu.VMEM((tok * kvh, dim), BF),
            pltpu.VMEM((kvh + half, cache + tok, dim), BF),
            pltpu.VMEM((kvh + half, dim, cache + dim), BF),
            pltpu.VMEM((2, cache, dim), BF),
            pltpu.VMEM((4 * half, tok, ratio, dim), BF),
            pltpu.VMEM((4 * half, dim, rows), BF),
            pltpu.VMEM((dim, rows), BF),
            pltpu.SMEM((1,), jnp.int32),
            (pltpu.VMEM((cache + tok, rows), F32),) * 4,
            (pltpu.VMEM((8, rows), F32),) * 4,
            pltpu.VMEM((4 * half, dim, rows), F32),
            pltpu.VMEM((4 * half, 1, rows), F32),
            pltpu.VMEM((4 * half, 1, rows), F32),
            pltpu.VMEM((2 * half, dim, rows), BF),
            pltpu.VMEM((2 * half, 1, rows), F32),
            pltpu.VMEM((2 * half, dim, rows), BF),
            pltpu.VMEM((2 * half, 1, rows), F32),
            pltpu.VMEM((half, tok, ratio, dim), BF),
            pltpu.VMEM((half, 1, rows), F32),
            dma((2, n_raw)), dma((3,)), dma((3 * half,)), dma((4 * half,)), dma((2, half)), dma((half,)), dma((half,)),
            dma((2, 2 * half)), dma((2, 2 * half)), dma((2, half)), dma((2, half)),
        ]
        flops = 4 * heads * tok * 4 * cache * dim
        out, lse = pl.pallas_call(
            attend_kernel,
            out_shape=(pltpu.VMEM((tok, kvh, ratio, dim), BF), pltpu.VMEM((kvh, 1, rows), F32)),
            in_specs=[hbm] * 6,
            out_specs=(vmem, vmem),
            scratch_shapes=scratch,
            compiler_params=pltpu.CompilerParams(collective_id=0, has_side_effects=True, vmem_limit_bytes=60 * 2 ** 20),
            cost_estimate=pl.CostEstimate(flops=flops, bytes_accessed=4 * cache * kvh * dim, transcendentals=heads * tok * 4 * cache),
            name='attend',
        )(queries.reshape(tok, kvh, ratio, dim), key_new.reshape(tok * kvh, dim), value_new.reshape(tok * kvh, dim),
          key_cache.reshape(cache * kvh, dim), value_cache.reshape(cache * kvh, dim), prefix_len)
        out, row_lse = pl.pallas_call(
            place_kernel,
            out_shape=(jax.ShapeDtypeStruct((tok, heads, dim), BF), jax.ShapeDtypeStruct((tok, heads), F32)),
            in_specs=[vmem, vmem],
            out_specs=(hbm, hbm),
            scratch_shapes=[pltpu.VMEM((tok, heads), F32), dma((2,))],
            compiler_params=pltpu.CompilerParams(vmem_limit_bytes=2 * 2 ** 20),
            name='place',
        )(out.reshape(tok, heads, dim), lse)
        return out, row_lse

    return jax.shard_map(local, mesh=mesh, in_specs=(tok_spec, tok_spec, tok_spec, tok_spec, tok_spec, P('dp')),
                         out_specs=(tok_spec, tok_spec), check_vma=False)
```

```python
import functools
import math

import jax
import jax.numpy as jnp
from jax import lax
from jax.experimental import pallas as pl
from jax.experimental.pallas import tpu as pltpu
from jax.sharding import PartitionSpec as P

MESH = pl.DeviceIdType.MESH
BIG = 1e30
TK = 256
PREP = 128
RAW_DEPTH = 3
BF = jnp.bfloat16
SEQ = ((0, 0), (2, 0), (4, 0), (12, 0), (14, 0), (12, 1), (8, 0), (14, 1),
       (10, 0), (8, 1), (10, 1), (6, 0), (4, 1), (6, 1), (0, 1), (2, 1))
F32 = jnp.float32


def _packed(part):
    v = sum((slot // 2 + 8 * second) << (4 * k) for k, (slot, second) in enumerate(part))
    return v - (1 << 32) if v >= 1 << 31 else v


ORDER = (_packed(SEQ[:8]), _packed(SEQ[8:]))
Q_PAIRS = tuple(SEQ.index((s, 0)) for s in range(4, 16, 2))
KV_PAIRS = tuple(next(k for k, (s, f) in enumerate(SEQ) if f and s % 4 == h) for h in (0, 2))
R_PAIRS = tuple(k for k, (s, f) in enumerate(SEQ) if f and s >= 8)
L_PAIRS = tuple(k for k, (s, f) in enumerate(SEQ) if f and s < 8)


def among(i, ks):
    hit = i == ks[0]
    for k in ks[1:]:
        hit = jnp.logical_or(hit, i == k)
    return hit


def attend_kernel(q_hbm, kn_hbm, vn_hbm, kc_hbm, vc_hbm, plen_hbm, out_ref, lse_ref,
                  raw_k, raw_v, new_k, new_v, kbuf, vbuf, bias, qraw, qt, pick, plen, sbuf, mbuf,
                  st_o, st_m, st_l, ps, psl, pr, prl, fo, fl,
                  raw_sem, new_sem, q_send, q_recv, kv_send, k_recv, v_recv, p_send, p_recv, f_send, f_recv):
    tok, kvh, ratio, dim = q_hbm.shape
    cache = kc_hbm.shape[0] // kvh
    half = kvh // 2
    rows = tok * ratio
    n_raw = raw_sem.shape[1]
    raw_pos = cache // n_raw
    chunks = cache // TK
    scale2 = dim ** -0.5 * math.log2(math.e)

    me = lax.axis_index('cp')
    core = lax.rem(me, 2)
    chip2 = me - core
    mate = chip2 + 1 - core
    far = lax.rem(chip2 + 2, 4) + core
    far_other = lax.rem(chip2 + 2, 4) + 1 - core

    def raw_copy(j):
        sl = pl.ds(j * raw_pos * kvh, raw_pos * kvh)
        return (pltpu.make_async_copy(kc_hbm.at[sl], raw_k.at[sl], raw_sem.at[0, j]),
                pltpu.make_async_copy(vc_hbm.at[sl], raw_v.at[sl], raw_sem.at[1, j]))

    def own_q(h):
        return pltpu.make_async_copy(q_hbm.at[:, half * core + h], qraw.at[h], q_recv.at[h])

    def raw_start(j):
        for cp in raw_copy(j):
            cp.start()

    for j in range(RAW_DEPTH):
        raw_start(j)
    plen_copy = pltpu.make_async_copy(plen_hbm, plen, new_sem.at[2])
    plen_copy.start()
    new_copies = (pltpu.make_async_copy(kn_hbm, new_k, new_sem.at[0]),
                  pltpu.make_async_copy(vn_hbm, new_v, new_sem.at[1]))
    for cp in new_copies:
        cp.start()
    for h in range(half):
        own_q(h).start()

    barrier = pltpu.get_barrier_semaphore()
    for peer in (mate, far, far_other):
        pl.semaphore_signal(barrier, inc=1, device_id={'cp': peer}, device_id_type=MESH)

    pick[...] = jnp.where(lax.broadcasted_iota(jnp.int32, (dim, rows), 0) == 0, 1.0, 0.0).astype(BF)
    for e in range(2):
        mbuf[e][...] = jnp.full((8, rows), -3e38, F32)

    pl.semaphore_wait(barrier, 3)

    def q_copy(k, h):
        peer, base = ((far_other, 3 * half), (far, 2 * half), (mate, half))[k]
        peer_core = (1 - core, core, 1 - core)[k]
        return pltpu.make_async_remote_copy(
            src_ref=q_hbm.at[:, half * peer_core + h], dst_ref=qraw.at[base + h],
            send_sem=q_send.at[k * half + h], recv_sem=q_recv.at[base + h],
            device_id={'cp': peer}, device_id_type=MESH)

    for k in range(3):
        for h in range(half):
            q_copy(k, h).start()

    plen_copy.wait()
    visible_len = plen[0]
    for f, owner in enumerate((me, mate)):
        @pl.loop(0, chunks)
        def _(j):
            lane = lax.broadcasted_iota(jnp.int32, (TK, dim), 1)
            pos = owner * cache + j * TK + lax.broadcasted_iota(jnp.int32, (TK, dim), 0)
            hidden = jnp.logical_and(lane == 0, pos >= visible_len)
            bias[f, pl.ds(pl.multiple_of(j * TK, TK), TK), :] = jnp.where(hidden, -BIG, 0.0).astype(BF)

    for cp in new_copies:
        cp.wait()
    kt = pltpu.einshape('phd->hpd', new_k[...].reshape(tok, kvh, dim))
    vt = pltpu.einshape('phd->hpd', new_v[...].reshape(tok, kvh, dim))
    for h in range(kvh):
        kbuf[h, pl.ds(cache, tok), :] = kt[h]
        vpad = jnp.concatenate([vt[h].astype(F32), jnp.zeros((dim - tok, dim), F32)], axis=0)
        vbuf[h, :, pl.ds(cache, dim)] = vpad.T.astype(BF)
    def kv_parts(h, lo, n):
        src = half * (1 - core) + h
        to = dict(device_id={'cp': mate}, device_id_type=MESH)
        k_rows, v_lanes = pl.ds(lo, tok if n == dim else n), pl.ds(lo, n)
        return (pltpu.make_async_remote_copy(
                    src_ref=kbuf.at[src, k_rows], dst_ref=kbuf.at[kvh + h, k_rows],
                    send_sem=kv_send.at[0, h], recv_sem=k_recv.at[h], **to),
                pltpu.make_async_remote_copy(
                    src_ref=vbuf.at[src, :, v_lanes], dst_ref=vbuf.at[kvh + h, :, v_lanes],
                    send_sem=kv_send.at[1, h], recv_sem=v_recv.at[h], **to))

    def kv_start(lo, n):
        for h in range(half):
            for cp in kv_parts(h, lo, n):
                cp.start()

    n_pairs = 4 * half

    def pair(i):
        code = lax.shift_right_logical(jnp.where(i < 8, ORDER[0], ORDER[1]), 4 * lax.rem(i, 8))
        slot = 2 * jnp.bitwise_and(code, 7)
        second = lax.div(jnp.bitwise_and(code, 15), 8)
        h = lax.rem(slot, half)
        kv = jnp.where(second == 1, kvh + h, half * core + h)
        owner = jnp.where(second == 1, mate, me)
        src = lax.div(slot, half)
        home = jnp.where(src == 0, me, jnp.where(src == 1, mate, jnp.where(src == 2, far, far_other)))
        return second, slot, kv, owner, home

    def load_q(slot):
        qt[slot] = qraw[slot].reshape(rows, dim).T

    def score_rhs(slot):
        return jnp.concatenate([qt[slot], pick[...]], axis=0)

    def qk_tile(kv, f, c, qv):
        sl = pl.ds(c * TK if isinstance(c, int) else pl.multiple_of(c * TK, TK), TK)
        lhs = jnp.concatenate([kbuf[kv, sl, :], bias[f, sl, :]], axis=1)
        return jnp.dot(lhs, qv, preferred_element_type=F32)

    def qk_new(kv, owner, home, qv):
        lhs = jnp.concatenate([kbuf[kv, pl.ds(cache, tok), :], jnp.zeros((tok, dim), BF)], axis=1)
        st = jnp.dot(lhs, qv, preferred_element_type=F32)
        key = owner * tok + lax.broadcasted_iota(jnp.int32, (tok, rows), 0)
        query = home * tok + lax.broadcasted_iota(jnp.int32, (tok, rows), 1) // ratio
        return jnp.where(key <= query, st, -BIG)

    def fold_max(mx, st):
        t = jnp.max(st.reshape(st.shape[0] // 8, 8, rows), axis=0)
        return t if mx is None else jnp.maximum(mx, t)

    f_0, slot_0, kv_0, owner_0, home_0 = pair(0)

    def first_scores(c):
        for e in range(2):
            st = qk_tile(kv_0 + e, f_0, c, score_rhs(slot_0 + e))
            sbuf[e][pl.ds(c * TK, TK), :] = st
            mbuf[e][...] = fold_max(mbuf[e][...], st)

    for j in range(n_raw):
        for cp in raw_copy(j):
            cp.wait()
        if j + RAW_DEPTH < n_raw:
            raw_start(j + RAW_DEPTH)

        @pl.loop(0, raw_pos // PREP)
        def _(i):
            base = pl.multiple_of(j * raw_pos + i * PREP, PREP)
            src = pl.ds(pl.multiple_of(base * kvh, PREP * kvh), PREP * kvh)
            xk = pltpu.einshape('phd->hpd', raw_k[src, :].reshape(PREP, kvh, dim))
            xv = pltpu.einshape('phd->hpd', raw_v[src, :].reshape(PREP, kvh, dim))
            for h in range(kvh):
                kbuf[h, pl.ds(base, PREP), :] = xk[h]
                vbuf[h, :, pl.ds(base, PREP)] = xv[h].T

        if j == 0:
            kv_start(cache, dim)
        if j % 2 and j > 1:
            kv_start((j - 3) * raw_pos, 2 * raw_pos)

    for h in range(half):
        own_q(h).wait()
    for h in range(half):
        load_q(h)
    for c in range(chunks):
        first_scores(c)
    for e in range(2):
        st = qk_new(kv_0 + e, owner_0, home_0, score_rhs(slot_0 + e))
        sbuf[e][pl.ds(cache, tok), :] = st
        mbuf[e][...] = fold_max(mbuf[e][...], st)
    kv_start(cache - 2 * raw_pos, 2 * raw_pos)

    def region(i, sc, sn, mc, mn, more=True):
        nxt = lax.rem(i + 1, n_pairs)
        f_n, slot_n, kv_n, owner_n, home_n = pair(nxt)
        second, slot, kv, _, _ = pair(i)
        later = jnp.minimum(i + 2, n_pairs - 1)
        ahead = pair(later)[1]

        @pl.when(among(i + 2, Q_PAIRS))
        def _():
            for e in range(2):
                pltpu.make_async_copy(qraw.at[ahead + e], qraw.at[ahead + e], q_recv.at[ahead + e]).wait()

        @pl.when(among(i + 1, KV_PAIRS))
        def _():
            for e in range(2):
                pltpu.make_async_copy(kbuf.at[kv_n + e], kbuf.at[kv_n + e], k_recv.at[kv_n + e - kvh]).wait()
                pltpu.make_async_copy(vbuf.at[kv_n + e], vbuf.at[kv_n + e], v_recv.at[kv_n + e - kvh]).wait()

        qv, m, decay, mx, l8, o = [], [], [], [None] * 2, [], [None] * 2
        for e in range(2):
            qv.append(score_rhs(slot_n + e) if more else None)
            m_old = jnp.where(second == 1, st_m[slot + e], -1e38)
            m.append(jnp.maximum(m_old, jnp.max(mc[e][...], axis=0, keepdims=True) * scale2))
            decay.append(jnp.exp2(m_old - m[e]))
            l8.append(jnp.zeros((8, rows), F32))
        for c in range(chunks):
            sl = pl.ds(c * TK, TK)
            for e in range(2):
                st = qk_tile(kv_n + e, f_n, c, qv[e]) if more else None
                p = jnp.exp2(sc[e][sl, :] * scale2 - m[e])
                if more:
                    sn[e][sl, :] = st
                    mx[e] = fold_max(mx[e], st)
                l8[e] = l8[e] + jnp.sum(p.reshape(TK // 8, 8, rows), axis=0)
                t = jnp.dot(vbuf[kv + e, :, sl], p.astype(BF), preferred_element_type=F32)
                o[e] = t if o[e] is None else o[e] + t
        sl = pl.ds(cache, tok)
        for e in range(2):
            p = jnp.exp2(sc[e][sl, :] * scale2 - m[e])
            if more:
                st = qk_new(kv_n + e, owner_n, home_n, qv[e])
                sn[e][sl, :] = st
                mn[e][...] = fold_max(mx[e], st)
            l8[e] = l8[e] + jnp.sum(p.reshape(tok // 8, 8, rows), axis=0)
            pb = jnp.concatenate([p.astype(BF), jnp.zeros((dim - tok, rows), BF)], axis=0)
            o[e] = o[e] + jnp.dot(vbuf[kv + e, :, pl.ds(cache, dim)], pb, preferred_element_type=F32)
        for e in range(2):
            st_o[slot + e] = jnp.where(second == 1, st_o[slot + e] * decay[e], 0.0) + o[e]
            st_l[slot + e] = jnp.where(second == 1, st_l[slot + e] * decay[e], 0.0) + jnp.sum(l8[e], axis=0, keepdims=True)
            st_m[slot + e] = m[e]
            if more:
                load_q(ahead + e)

    def partial_copies(u):
        return (pltpu.make_async_remote_copy(
                    src_ref=ps.at[u], dst_ref=pr.at[u], send_sem=p_send.at[0, u], recv_sem=p_recv.at[0, u],
                    device_id={'cp': far}, device_id_type=MESH),
                pltpu.make_async_remote_copy(
                    src_ref=psl.at[u], dst_ref=prl.at[u], send_sem=p_send.at[1, u], recv_sem=p_recv.at[1, u],
                    device_id={'cp': far}, device_id_type=MESH))

    def mate_out(u):
        hh = half * core + u - half
        return (pltpu.make_async_remote_copy(
                    src_ref=fo.at[u - half], dst_ref=out_ref.at[:, hh], send_sem=f_send.at[0, u - half],
                    recv_sem=f_recv.at[0, u - half], device_id={'cp': mate}, device_id_type=MESH),
                pltpu.make_async_remote_copy(
                    src_ref=fl.at[u - half], dst_ref=lse_ref.at[hh], send_sem=f_send.at[1, u - half],
                    recv_sem=f_recv.at[1, u - half], device_id={'cp': mate}, device_id_type=MESH))

    def finish(i):
        _, slot, _, _, _ = pair(i)

        @pl.when(among(i, R_PAIRS))
        def _():
            u = slot - 2 * half
            for e in range(2):
                l = st_l[slot + e]
                ps[u + e] = (st_o[slot + e] * (1.0 / l)).astype(BF)
                psl[u + e] = st_m[slot + e] + jnp.log2(l)
            for e in range(2):
                for cp in partial_copies(u + e):
                    cp.start()

        @pl.when(among(i, L_PAIRS))
        def _():
            u = slot
            for e in range(2):
                for cp in partial_copies(u + e):
                    cp.wait_recv()
            done = []
            for e in range(2):
                m_a, m_b = st_m[u + e], prl[u + e]
                m = jnp.maximum(m_a, m_b)
                a, b = jnp.exp2(m_a - m), jnp.exp2(m_b - m)
                l = st_l[u + e] * a + b
                inv = 1.0 / l
                o = st_o[u + e] * (a * inv) + pr[u + e].astype(F32) * (b * inv)
                done.append((o.T.astype(BF).reshape(tok, ratio, dim), (m + jnp.log2(l)) * math.log(2.0)))

            @pl.when(u < half)
            def _():
                for e in range(2):
                    out_ref[:, half * core + u + e] = done[e][0]
                    lse_ref[half * core + u + e] = done[e][1]

            @pl.when(u >= half)
            def _():
                for e in range(2):
                    fo[u - half + e] = done[e][0]
                    fl[u - half + e] = done[e][1]
                for e in range(2):
                    for cp in mate_out(u + e):
                        cp.start()

    def two(i, more):
        region(2 * i, sbuf[:2], sbuf[2:], mbuf[:2], mbuf[2:])
        finish(2 * i)
        region(2 * i + 1, sbuf[2:], sbuf[:2], mbuf[2:], mbuf[:2], more)
        finish(2 * i + 1)

    @pl.loop(0, n_pairs // 2 - 1)
    def _(i):
        two(i, True)

    two(jnp.int32(n_pairs // 2 - 1), False)

    for k in range(3):
        for h in range(half):
            q_copy(k, h).wait_send()
    for h in range(half):
        pltpu.make_async_copy(kbuf.at[h], kbuf.at[h], kv_send.at[0, h]).wait()
        pltpu.make_async_copy(vbuf.at[h], vbuf.at[h], kv_send.at[1, h]).wait()
    for u in range(2 * half):
        for cp in partial_copies(u):
            cp.wait_send()
    for u in range(half):
        for cp in mate_out(u + half):
            cp.wait_send()
            cp.wait_recv()


def place_kernel(out_ref, lse_ref, out_hbm, lse_hbm, lse_buf, sem):
    kvh, _, rows = lse_ref.shape
    tok, heads = lse_buf.shape
    ratio = heads // kvh
    write = pltpu.make_async_copy(out_ref, out_hbm, sem.at[0])
    write.start()
    x = lse_ref[...].reshape(kvh, rows)
    lane = lax.broadcasted_iota(jnp.int32, (kvh, heads), 1) // ratio
    head = lax.broadcasted_iota(jnp.int32, (kvh, heads), 0)
    per = heads // ratio
    blocks = [pltpu.roll(x[:, b * heads:(b + 1) * heads], 0, 1, stride=ratio, stride_axis=0) for b in range(tok // per)]
    for t in range(tok):
        turned = pltpu.roll(blocks[t // per], (heads - (t % per) * ratio) % heads, 1)
        lse_buf[pl.ds(t, 1), :] = jnp.sum(jnp.where(lane == head, turned, 0.0), axis=0, keepdims=True)
    lse_write = pltpu.make_async_copy(lse_buf, lse_hbm, sem.at[1])
    lse_write.start()
    write.wait()
    lse_write.wait()


def solution(mesh):
    tok_spec = P(('dp', 'cp'))

    def local(queries, key_new, value_new, key_cache, value_cache, prefix_len):
        tok, heads, dim = queries.shape
        cache, kvh = key_cache.shape[:2]
        ratio = heads // kvh
        half = kvh // 2
        rows = tok * ratio
        n_raw = cache // TK
        dma = pltpu.SemaphoreType.DMA
        hbm = pl.BlockSpec(memory_space=pltpu.HBM)
        vmem = pl.BlockSpec(memory_space=pltpu.VMEM)
        scratch = [
            pltpu.VMEM((cache * kvh, dim), BF),
            pltpu.VMEM((cache * kvh, dim), BF),
            pltpu.VMEM((tok * kvh, dim), BF),
            pltpu.VMEM((tok * kvh, dim), BF),
            pltpu.VMEM((kvh + half, cache + tok, dim), BF),
            pltpu.VMEM((kvh + half, dim, cache + dim), BF),
            pltpu.VMEM((2, cache, dim), BF),
            pltpu.VMEM((4 * half, tok, ratio, dim), BF),
            pltpu.VMEM((4 * half, dim, rows), BF),
            pltpu.VMEM((dim, rows), BF),
            pltpu.SMEM((1,), jnp.int32),
            (pltpu.VMEM((cache + tok, rows), F32),) * 4,
            (pltpu.VMEM((8, rows), F32),) * 4,
            pltpu.VMEM((4 * half, dim, rows), F32),
            pltpu.VMEM((4 * half, 1, rows), F32),
            pltpu.VMEM((4 * half, 1, rows), F32),
            pltpu.VMEM((2 * half, dim, rows), BF),
            pltpu.VMEM((2 * half, 1, rows), F32),
            pltpu.VMEM((2 * half, dim, rows), BF),
            pltpu.VMEM((2 * half, 1, rows), F32),
            pltpu.VMEM((half, tok, ratio, dim), BF),
            pltpu.VMEM((half, 1, rows), F32),
            dma((2, n_raw)), dma((3,)), dma((3 * half,)), dma((4 * half,)), dma((2, half)), dma((half,)), dma((half,)),
            dma((2, 2 * half)), dma((2, 2 * half)), dma((2, half)), dma((2, half)),
        ]
        flops = 4 * heads * tok * 4 * cache * dim
        out, lse = pl.pallas_call(
            attend_kernel,
            out_shape=(pltpu.VMEM((tok, kvh, ratio, dim), BF), pltpu.VMEM((kvh, 1, rows), F32)),
            in_specs=[hbm] * 6,
            out_specs=(vmem, vmem),
            scratch_shapes=scratch,
            compiler_params=pltpu.CompilerParams(collective_id=0, has_side_effects=True, vmem_limit_bytes=60 * 2 ** 20),
            cost_estimate=pl.CostEstimate(flops=flops, bytes_accessed=4 * cache * kvh * dim, transcendentals=heads * tok * 4 * cache),
            name='attend',
        )(queries.reshape(tok, kvh, ratio, dim), key_new.reshape(tok * kvh, dim), value_new.reshape(tok * kvh, dim),
          key_cache.reshape(cache * kvh, dim), value_cache.reshape(cache * kvh, dim), prefix_len)
        out, row_lse = pl.pallas_call(
            place_kernel,
            out_shape=(jax.ShapeDtypeStruct((tok, heads, dim), BF), jax.ShapeDtypeStruct((tok, heads), F32)),
            in_specs=[vmem, vmem],
            out_specs=(hbm, hbm),
            scratch_shapes=[pltpu.VMEM((tok, heads), F32), dma((2,))],
            compiler_params=pltpu.CompilerParams(vmem_limit_bytes=2 * 2 ** 20),
            name='place',
        )(out.reshape(tok, heads, dim), lse)
        return out, row_lse

    return jax.shard_map(local, mesh=mesh, in_specs=(tok_spec, tok_spec, tok_spec, tok_spec, tok_spec, P('dp')),
                         out_specs=(tok_spec, tok_spec), check_vma=False)
```

```python
import functools
import math

import jax
import jax.numpy as jnp
from jax import lax
from jax.experimental import pallas as pl
from jax.experimental.pallas import tpu as pltpu
from jax.sharding import PartitionSpec as P

MESH = pl.DeviceIdType.MESH
BIG = 1e30
TK = 256
PREP = 128
RAW_DEPTH = 3
BF = jnp.bfloat16
SEQ = ((0, 0), (2, 0), (4, 0), (12, 0), (14, 0), (12, 1), (8, 0), (14, 1),
       (10, 0), (8, 1), (10, 1), (6, 0), (4, 1), (6, 1), (0, 1), (2, 1))
F32 = jnp.float32


def _packed(part):
    v = sum((slot // 2 + 8 * second) << (4 * k) for k, (slot, second) in enumerate(part))
    return v - (1 << 32) if v >= 1 << 31 else v


ORDER = (_packed(SEQ[:8]), _packed(SEQ[8:]))
Q_PAIRS = tuple(SEQ.index((s, 0)) for s in range(4, 16, 2))
KV_PAIRS = tuple(next(k for k, (s, f) in enumerate(SEQ) if f and s % 4 == h) for h in (0, 2))
R_PAIRS = tuple(k for k, (s, f) in enumerate(SEQ) if f and s >= 8)
L_PAIRS = tuple(k for k, (s, f) in enumerate(SEQ) if f and s < 8)


def among(i, ks):
    hit = i == ks[0]
    for k in ks[1:]:
        hit = jnp.logical_or(hit, i == k)
    return hit


def attend_kernel(q_hbm, kn_hbm, vn_hbm, kc_hbm, vc_hbm, plen_hbm, out_ref, lse_ref,
                  raw_k, raw_v, new_k, new_v, kbuf, vbuf, bias, qraw, qt, pick, plen, sbuf, mbuf,
                  st_o, st_m, st_l, ps, psl, pr, prl, fo, fl,
                  raw_sem, new_sem, q_send, q_recv, kv_send, k_recv, v_recv, p_send, p_recv, f_send, f_recv):
    tok, kvh, ratio, dim = q_hbm.shape
    cache = kc_hbm.shape[0] // kvh
    half = kvh // 2
    rows = tok * ratio
    n_raw = raw_sem.shape[1]
    raw_pos = cache // n_raw
    chunks = cache // TK
    scale2 = dim ** -0.5 * math.log2(math.e)

    me = lax.axis_index('cp')
    core = lax.rem(me, 2)
    chip2 = me - core
    mate = chip2 + 1 - core
    far = lax.rem(chip2 + 2, 4) + core
    far_other = lax.rem(chip2 + 2, 4) + 1 - core

    def raw_copy(j):
        sl = pl.ds(j * raw_pos * kvh, raw_pos * kvh)
        return (pltpu.make_async_copy(kc_hbm.at[sl], raw_k.at[sl], raw_sem.at[0, j]),
                pltpu.make_async_copy(vc_hbm.at[sl], raw_v.at[sl], raw_sem.at[1, j]))

    def own_q(h):
        return pltpu.make_async_copy(q_hbm.at[:, half * core + h], qraw.at[h], q_recv.at[h])

    def raw_start(j):
        for cp in raw_copy(j):
            cp.start()

    for j in range(RAW_DEPTH):
        raw_start(j)
    plen_copy = pltpu.make_async_copy(plen_hbm, plen, new_sem.at[2])
    plen_copy.start()
    new_copies = (pltpu.make_async_copy(kn_hbm, new_k, new_sem.at[0]),
                  pltpu.make_async_copy(vn_hbm, new_v, new_sem.at[1]))
    for cp in new_copies:
        cp.start()
    for h in range(half):
        own_q(h).start()

    barrier = pltpu.get_barrier_semaphore()
    for peer in (mate, far, far_other):
        pl.semaphore_signal(barrier, inc=1, device_id={'cp': peer}, device_id_type=MESH)

    pick[...] = jnp.where(lax.broadcasted_iota(jnp.int32, (dim, rows), 0) == 0, 1.0, 0.0).astype(BF)
    for e in range(2):
        mbuf[e][...] = jnp.full((8, rows), -3e38, F32)

    def q_copy(k, h):
        peer, base = ((far_other, 3 * half), (far, 2 * half), (mate, half))[k]
        peer_core = (1 - core, core, 1 - core)[k]
        return pltpu.make_async_remote_copy(
            src_ref=q_hbm.at[:, half * peer_core + h], dst_ref=qraw.at[base + h],
            send_sem=q_send.at[k * half + h], recv_sem=q_recv.at[base + h],
            device_id={'cp': peer}, device_id_type=MESH)

    plen_copy.wait()
    visible_len = plen[0]
    for f, owner in enumerate((me, mate)):
        @pl.loop(0, chunks)
        def _(j):
            lane = lax.broadcasted_iota(jnp.int32, (TK, dim), 1)
            pos = owner * cache + j * TK + lax.broadcasted_iota(jnp.int32, (TK, dim), 0)
            hidden = jnp.logical_and(lane == 0, pos >= visible_len)
            bias[f, pl.ds(pl.multiple_of(j * TK, TK), TK), :] = jnp.where(hidden, -BIG, 0.0).astype(BF)

    for cp in new_copies:
        cp.wait()
    kt = pltpu.einshape('phd->hpd', new_k[...].reshape(tok, kvh, dim))
    vt = pltpu.einshape('phd->hpd', new_v[...].reshape(tok, kvh, dim))
    for h in range(kvh):
        kbuf[h, pl.ds(cache, tok), :] = kt[h]
        vpad = jnp.concatenate([vt[h].astype(F32), jnp.zeros((dim - tok, dim), F32)], axis=0)
        vbuf[h, :, pl.ds(cache, dim)] = vpad.T.astype(BF)
    def kv_parts(h, lo, n):
        src = half * (1 - core) + h
        to = dict(device_id={'cp': mate}, device_id_type=MESH)
        k_rows, v_lanes = pl.ds(lo, tok if n == dim else n), pl.ds(lo, n)
        return (pltpu.make_async_remote_copy(
                    src_ref=kbuf.at[src, k_rows], dst_ref=kbuf.at[kvh + h, k_rows],
                    send_sem=kv_send.at[0, h], recv_sem=k_recv.at[h], **to),
                pltpu.make_async_remote_copy(
                    src_ref=vbuf.at[src, :, v_lanes], dst_ref=vbuf.at[kvh + h, :, v_lanes],
                    send_sem=kv_send.at[1, h], recv_sem=v_recv.at[h], **to))

    def kv_start(lo, n):
        for h in range(half):
            for cp in kv_parts(h, lo, n):
                cp.start()

    n_pairs = 4 * half

    def pair(i):
        code = lax.shift_right_logical(jnp.where(i < 8, ORDER[0], ORDER[1]), 4 * lax.rem(i, 8))
        slot = 2 * jnp.bitwise_and(code, 7)
        second = lax.div(jnp.bitwise_and(code, 15), 8)
        h = lax.rem(slot, half)
        kv = jnp.where(second == 1, kvh + h, half * core + h)
        owner = jnp.where(second == 1, mate, me)
        src = lax.div(slot, half)
        home = jnp.where(src == 0, me, jnp.where(src == 1, mate, jnp.where(src == 2, far, far_other)))
        return second, slot, kv, owner, home

    def load_q(slot):
        qt[slot] = qraw[slot].reshape(rows, dim).T

    def score_rhs(slot):
        return jnp.concatenate([qt[slot], pick[...]], axis=0)

    def qk_tile(kv, f, c, qv):
        sl = pl.ds(c * TK if isinstance(c, int) else pl.multiple_of(c * TK, TK), TK)
        lhs = jnp.concatenate([kbuf[kv, sl, :], bias[f, sl, :]], axis=1)
        return jnp.dot(lhs, qv, preferred_element_type=F32)

    def qk_new(kv, owner, home, qv):
        lhs = jnp.concatenate([kbuf[kv, pl.ds(cache, tok), :], jnp.zeros((tok, dim), BF)], axis=1)
        st = jnp.dot(lhs, qv, preferred_element_type=F32)
        key = owner * tok + lax.broadcasted_iota(jnp.int32, (tok, rows), 0)
        query = home * tok + lax.broadcasted_iota(jnp.int32, (tok, rows), 1) // ratio
        return jnp.where(key <= query, st, -BIG)

    def fold_max(mx, st):
        t = jnp.max(st.reshape(st.shape[0] // 8, 8, rows), axis=0)
        return t if mx is None else jnp.maximum(mx, t)

    f_0, slot_0, kv_0, owner_0, home_0 = pair(0)

    def first_scores(c):
        for e in range(2):
            st = qk_tile(kv_0 + e, f_0, c, score_rhs(slot_0 + e))
            sbuf[e][pl.ds(c * TK, TK), :] = st
            mbuf[e][...] = fold_max(mbuf[e][...], st)

    for j in range(n_raw):
        for cp in raw_copy(j):
            cp.wait()
        if j + RAW_DEPTH < n_raw:
            raw_start(j + RAW_DEPTH)

        @pl.loop(0, raw_pos // PREP)
        def _(i):
            base = pl.multiple_of(j * raw_pos + i * PREP, PREP)
            src = pl.ds(pl.multiple_of(base * kvh, PREP * kvh), PREP * kvh)
            xk = pltpu.einshape('phd->hpd', raw_k[src, :].reshape(PREP, kvh, dim))
            xv = pltpu.einshape('phd->hpd', raw_v[src, :].reshape(PREP, kvh, dim))
            for h in range(kvh):
                kbuf[h, pl.ds(base, PREP), :] = xk[h]
                vbuf[h, :, pl.ds(base, PREP)] = xv[h].T

        if j == 2:
            pl.semaphore_wait(barrier, 3)
            for k in range(3):
                for h in range(half):
                    q_copy(k, h).start()
            kv_start(cache, dim)
        if j % 2 and j > 1:
            kv_start((j - 3) * raw_pos, 2 * raw_pos)

    for h in range(half):
        own_q(h).wait()
    for h in range(half):
        load_q(h)
    for c in range(chunks):
        first_scores(c)
    for e in range(2):
        st = qk_new(kv_0 + e, owner_0, home_0, score_rhs(slot_0 + e))
        sbuf[e][pl.ds(cache, tok), :] = st
        mbuf[e][...] = fold_max(mbuf[e][...], st)
    kv_start(cache - 2 * raw_pos, 2 * raw_pos)

    def region(i, sc, sn, mc, mn, more=True):
        nxt = lax.rem(i + 1, n_pairs)
        f_n, slot_n, kv_n, owner_n, home_n = pair(nxt)
        second, slot, kv, _, _ = pair(i)
        later = jnp.minimum(i + 2, n_pairs - 1)
        ahead = pair(later)[1]

        @pl.when(among(i + 2, Q_PAIRS))
        def _():
            for e in range(2):
                pltpu.make_async_copy(qraw.at[ahead + e], qraw.at[ahead + e], q_recv.at[ahead + e]).wait()

        @pl.when(among(i + 1, KV_PAIRS))
        def _():
            for e in range(2):
                pltpu.make_async_copy(kbuf.at[kv_n + e], kbuf.at[kv_n + e], k_recv.at[kv_n + e - kvh]).wait()
                pltpu.make_async_copy(vbuf.at[kv_n + e], vbuf.at[kv_n + e], v_recv.at[kv_n + e - kvh]).wait()

        qv, m, decay, mx, l8, o = [], [], [], [None] * 2, [], [None] * 2
        for e in range(2):
            qv.append(score_rhs(slot_n + e) if more else None)
            m_old = jnp.where(second == 1, st_m[slot + e], -1e38)
            m.append(jnp.maximum(m_old, jnp.max(mc[e][...], axis=0, keepdims=True) * scale2))
            decay.append(jnp.exp2(m_old - m[e]))
            l8.append(jnp.zeros((8, rows), F32))
        for c in range(chunks):
            sl = pl.ds(c * TK, TK)
            for e in range(2):
                st = qk_tile(kv_n + e, f_n, c, qv[e]) if more else None
                p = jnp.exp2(sc[e][sl, :] * scale2 - m[e])
                if more:
                    sn[e][sl, :] = st
                    mx[e] = fold_max(mx[e], st)
                l8[e] = l8[e] + jnp.sum(p.reshape(TK // 8, 8, rows), axis=0)
                t = jnp.dot(vbuf[kv + e, :, sl], p.astype(BF), preferred_element_type=F32)
                o[e] = t if o[e] is None else o[e] + t
        sl = pl.ds(cache, tok)
        for e in range(2):
            p = jnp.exp2(sc[e][sl, :] * scale2 - m[e])
            if more:
                st = qk_new(kv_n + e, owner_n, home_n, qv[e])
                sn[e][sl, :] = st
                mn[e][...] = fold_max(mx[e], st)
            l8[e] = l8[e] + jnp.sum(p.reshape(tok // 8, 8, rows), axis=0)
            pb = jnp.concatenate([p.astype(BF), jnp.zeros((dim - tok, rows), BF)], axis=0)
            o[e] = o[e] + jnp.dot(vbuf[kv + e, :, pl.ds(cache, dim)], pb, preferred_element_type=F32)
        for e in range(2):
            st_o[slot + e] = jnp.where(second == 1, st_o[slot + e] * decay[e], 0.0) + o[e]
            st_l[slot + e] = jnp.where(second == 1, st_l[slot + e] * decay[e], 0.0) + jnp.sum(l8[e], axis=0, keepdims=True)
            st_m[slot + e] = m[e]
            if more:
                load_q(ahead + e)

    def partial_copies(u):
        return (pltpu.make_async_remote_copy(
                    src_ref=ps.at[u], dst_ref=pr.at[u], send_sem=p_send.at[0, u], recv_sem=p_recv.at[0, u],
                    device_id={'cp': far}, device_id_type=MESH),
                pltpu.make_async_remote_copy(
                    src_ref=psl.at[u], dst_ref=prl.at[u], send_sem=p_send.at[1, u], recv_sem=p_recv.at[1, u],
                    device_id={'cp': far}, device_id_type=MESH))

    def mate_out(u):
        hh = half * core + u - half
        return (pltpu.make_async_remote_copy(
                    src_ref=fo.at[u - half], dst_ref=out_ref.at[:, hh], send_sem=f_send.at[0, u - half],
                    recv_sem=f_recv.at[0, u - half], device_id={'cp': mate}, device_id_type=MESH),
                pltpu.make_async_remote_copy(
                    src_ref=fl.at[u - half], dst_ref=lse_ref.at[hh], send_sem=f_send.at[1, u - half],
                    recv_sem=f_recv.at[1, u - half], device_id={'cp': mate}, device_id_type=MESH))

    def finish(i):
        _, slot, _, _, _ = pair(i)

        @pl.when(among(i, R_PAIRS))
        def _():
            u = slot - 2 * half
            for e in range(2):
                l = st_l[slot + e]
                ps[u + e] = (st_o[slot + e] * (1.0 / l)).astype(BF)
                psl[u + e] = st_m[slot + e] + jnp.log2(l)
            for e in range(2):
                for cp in partial_copies(u + e):
                    cp.start()

        @pl.when(among(i, L_PAIRS))
        def _():
            u = slot
            for e in range(2):
                for cp in partial_copies(u + e):
                    cp.wait_recv()
            done = []
            for e in range(2):
                m_a, m_b = st_m[u + e], prl[u + e]
                m = jnp.maximum(m_a, m_b)
                a, b = jnp.exp2(m_a - m), jnp.exp2(m_b - m)
                l = st_l[u + e] * a + b
                inv = 1.0 / l
                o = st_o[u + e] * (a * inv) + pr[u + e].astype(F32) * (b * inv)
                done.append((o.T.astype(BF).reshape(tok, ratio, dim), (m + jnp.log2(l)) * math.log(2.0)))

            @pl.when(u < half)
            def _():
                for e in range(2):
                    out_ref[:, half * core + u + e] = done[e][0]
                    lse_ref[half * core + u + e] = done[e][1]

            @pl.when(u >= half)
            def _():
                for e in range(2):
                    fo[u - half + e] = done[e][0]
                    fl[u - half + e] = done[e][1]
                for e in range(2):
                    for cp in mate_out(u + e):
                        cp.start()

    def two(i, more):
        region(2 * i, sbuf[:2], sbuf[2:], mbuf[:2], mbuf[2:])
        finish(2 * i)
        region(2 * i + 1, sbuf[2:], sbuf[:2], mbuf[2:], mbuf[:2], more)
        finish(2 * i + 1)

    @pl.loop(0, n_pairs // 2 - 1)
    def _(i):
        two(i, True)

    two(jnp.int32(n_pairs // 2 - 1), False)

    for k in range(3):
        for h in range(half):
            q_copy(k, h).wait_send()
    for h in range(half):
        pltpu.make_async_copy(kbuf.at[h], kbuf.at[h], kv_send.at[0, h]).wait()
        pltpu.make_async_copy(vbuf.at[h], vbuf.at[h], kv_send.at[1, h]).wait()
    for u in range(2 * half):
        for cp in partial_copies(u):
            cp.wait_send()
    for u in range(half):
        for cp in mate_out(u + half):
            cp.wait_send()
            cp.wait_recv()


def place_kernel(out_ref, lse_ref, out_hbm, lse_hbm, lse_buf, sem):
    kvh, _, rows = lse_ref.shape
    tok, heads = lse_buf.shape
    ratio = heads // kvh
    write = pltpu.make_async_copy(out_ref, out_hbm, sem.at[0])
    write.start()
    x = lse_ref[...].reshape(kvh, rows)
    lane = lax.broadcasted_iota(jnp.int32, (kvh, heads), 1) // ratio
    head = lax.broadcasted_iota(jnp.int32, (kvh, heads), 0)
    per = heads // ratio
    blocks = [pltpu.roll(x[:, b * heads:(b + 1) * heads], 0, 1, stride=ratio, stride_axis=0) for b in range(tok // per)]
    for t in range(tok):
        turned = pltpu.roll(blocks[t // per], (heads - (t % per) * ratio) % heads, 1)
        lse_buf[pl.ds(t, 1), :] = jnp.sum(jnp.where(lane == head, turned, 0.0), axis=0, keepdims=True)
    lse_write = pltpu.make_async_copy(lse_buf, lse_hbm, sem.at[1])
    lse_write.start()
    write.wait()
    lse_write.wait()


def solution(mesh):
    tok_spec = P(('dp', 'cp'))

    def local(queries, key_new, value_new, key_cache, value_cache, prefix_len):
        tok, heads, dim = queries.shape
        cache, kvh = key_cache.shape[:2]
        ratio = heads // kvh
        half = kvh // 2
        rows = tok * ratio
        n_raw = cache // TK
        dma = pltpu.SemaphoreType.DMA
        hbm = pl.BlockSpec(memory_space=pltpu.HBM)
        vmem = pl.BlockSpec(memory_space=pltpu.VMEM)
        scratch = [
            pltpu.VMEM((cache * kvh, dim), BF),
            pltpu.VMEM((cache * kvh, dim), BF),
            pltpu.VMEM((tok * kvh, dim), BF),
            pltpu.VMEM((tok * kvh, dim), BF),
            pltpu.VMEM((kvh + half, cache + tok, dim), BF),
            pltpu.VMEM((kvh + half, dim, cache + dim), BF),
            pltpu.VMEM((2, cache, dim), BF),
            pltpu.VMEM((4 * half, tok, ratio, dim), BF),
            pltpu.VMEM((4 * half, dim, rows), BF),
            pltpu.VMEM((dim, rows), BF),
            pltpu.SMEM((1,), jnp.int32),
            (pltpu.VMEM((cache + tok, rows), F32),) * 4,
            (pltpu.VMEM((8, rows), F32),) * 4,
            pltpu.VMEM((4 * half, dim, rows), F32),
            pltpu.VMEM((4 * half, 1, rows), F32),
            pltpu.VMEM((4 * half, 1, rows), F32),
            pltpu.VMEM((2 * half, dim, rows), BF),
            pltpu.VMEM((2 * half, 1, rows), F32),
            pltpu.VMEM((2 * half, dim, rows), BF),
            pltpu.VMEM((2 * half, 1, rows), F32),
            pltpu.VMEM((half, tok, ratio, dim), BF),
            pltpu.VMEM((half, 1, rows), F32),
            dma((2, n_raw)), dma((3,)), dma((3 * half,)), dma((4 * half,)), dma((2, half)), dma((half,)), dma((half,)),
            dma((2, 2 * half)), dma((2, 2 * half)), dma((2, half)), dma((2, half)),
        ]
        flops = 4 * heads * tok * 4 * cache * dim
        out, lse = pl.pallas_call(
            attend_kernel,
            out_shape=(pltpu.VMEM((tok, kvh, ratio, dim), BF), pltpu.VMEM((kvh, 1, rows), F32)),
            in_specs=[hbm] * 6,
            out_specs=(vmem, vmem),
            scratch_shapes=scratch,
            compiler_params=pltpu.CompilerParams(collective_id=0, has_side_effects=True, vmem_limit_bytes=60 * 2 ** 20),
            cost_estimate=pl.CostEstimate(flops=flops, bytes_accessed=4 * cache * kvh * dim, transcendentals=heads * tok * 4 * cache),
            name='attend',
        )(queries.reshape(tok, kvh, ratio, dim), key_new.reshape(tok * kvh, dim), value_new.reshape(tok * kvh, dim),
          key_cache.reshape(cache * kvh, dim), value_cache.reshape(cache * kvh, dim), prefix_len)
        out, row_lse = pl.pallas_call(
            place_kernel,
            out_shape=(jax.ShapeDtypeStruct((tok, heads, dim), BF), jax.ShapeDtypeStruct((tok, heads), F32)),
            in_specs=[vmem, vmem],
            out_specs=(hbm, hbm),
            scratch_shapes=[pltpu.VMEM((tok, heads), F32), dma((2,))],
            compiler_params=pltpu.CompilerParams(vmem_limit_bytes=2 * 2 ** 20),
            name='place',
        )(out.reshape(tok, heads, dim), lse)
        return out, row_lse

    return jax.shard_map(local, mesh=mesh, in_specs=(tok_spec, tok_spec, tok_spec, tok_spec, tok_spec, P('dp')),
                         out_specs=(tok_spec, tok_spec), check_vma=False)
```

```python
import functools
import math

import jax
import jax.numpy as jnp
from jax import lax
from jax.experimental import pallas as pl
from jax.experimental.pallas import tpu as pltpu
from jax.sharding import PartitionSpec as P

MESH = pl.DeviceIdType.MESH
BIG = 1e30
TK = 256
PREP = 128
RAW_DEPTH = 3
BF = jnp.bfloat16
SEQ = ((0, 0), (2, 0), (4, 0), (6, 0), (12, 0), (14, 0), (12, 1), (8, 0),
       (14, 1), (10, 0), (8, 1), (10, 1), (4, 1), (6, 1), (0, 1), (2, 1))
F32 = jnp.float32


def _packed(part):
    v = sum((slot // 2 + 8 * second) << (4 * k) for k, (slot, second) in enumerate(part))
    return v - (1 << 32) if v >= 1 << 31 else v


ORDER = (_packed(SEQ[:8]), _packed(SEQ[8:]))
Q_PAIRS = tuple(SEQ.index((s, 0)) for s in range(4, 16, 2))
KV_PAIRS = tuple(next(k for k, (s, f) in enumerate(SEQ) if f and s % 4 == h) for h in (0, 2))
R_PAIRS = tuple(k for k, (s, f) in enumerate(SEQ) if f and s >= 8)
L_PAIRS = tuple(k for k, (s, f) in enumerate(SEQ) if f and s < 8)


def among(i, ks):
    hit = i == ks[0]
    for k in ks[1:]:
        hit = jnp.logical_or(hit, i == k)
    return hit


def attend_kernel(q_hbm, kn_hbm, vn_hbm, kc_hbm, vc_hbm, plen_hbm, out_ref, lse_ref,
                  raw_k, raw_v, new_k, new_v, kbuf, vbuf, bias, qraw, qt, pick, plen, sbuf, mbuf,
                  st_o, st_m, st_l, ps, psl, pr, prl, fo, fl,
                  raw_sem, new_sem, q_send, q_recv, kv_send, k_recv, v_recv, p_send, p_recv, f_send, f_recv):
    tok, kvh, ratio, dim = q_hbm.shape
    cache = kc_hbm.shape[0] // kvh
    half = kvh // 2
    rows = tok * ratio
    n_raw = raw_sem.shape[1]
    raw_pos = cache // n_raw
    chunks = cache // TK
    scale2 = dim ** -0.5 * math.log2(math.e)

    me = lax.axis_index('cp')
    core = lax.rem(me, 2)
    chip2 = me - core
    mate = chip2 + 1 - core
    far = lax.rem(chip2 + 2, 4) + core
    far_other = lax.rem(chip2 + 2, 4) + 1 - core

    def raw_copy(j):
        sl = pl.ds(j * raw_pos * kvh, raw_pos * kvh)
        return (pltpu.make_async_copy(kc_hbm.at[sl], raw_k.at[sl], raw_sem.at[0, j]),
                pltpu.make_async_copy(vc_hbm.at[sl], raw_v.at[sl], raw_sem.at[1, j]))

    def own_q(h):
        return pltpu.make_async_copy(q_hbm.at[:, half * core + h], qraw.at[h], q_recv.at[h])

    def raw_start(j):
        for cp in raw_copy(j):
            cp.start()

    for j in range(RAW_DEPTH):
        raw_start(j)
    plen_copy = pltpu.make_async_copy(plen_hbm, plen, new_sem.at[2])
    plen_copy.start()
    new_copies = (pltpu.make_async_copy(kn_hbm, new_k, new_sem.at[0]),
                  pltpu.make_async_copy(vn_hbm, new_v, new_sem.at[1]))
    for cp in new_copies:
        cp.start()
    for h in range(half):
        own_q(h).start()

    barrier = pltpu.get_barrier_semaphore()
    for peer in (mate, far, far_other):
        pl.semaphore_signal(barrier, inc=1, device_id={'cp': peer}, device_id_type=MESH)

    pick[...] = jnp.where(lax.broadcasted_iota(jnp.int32, (dim, rows), 0) == 0, 1.0, 0.0).astype(BF)
    for e in range(2):
        mbuf[e][...] = jnp.full((8, rows), -3e38, F32)

    def q_copy(k, h):
        peer, base = ((far_other, 3 * half), (far, 2 * half), (mate, half))[k]
        peer_core = (1 - core, core, 1 - core)[k]
        return pltpu.make_async_remote_copy(
            src_ref=q_hbm.at[:, half * peer_core + h], dst_ref=qraw.at[base + h],
            send_sem=q_send.at[k * half + h], recv_sem=q_recv.at[base + h],
            device_id={'cp': peer}, device_id_type=MESH)

    plen_copy.wait()
    visible_len = plen[0]
    for f, owner in enumerate((me, mate)):
        @pl.loop(0, chunks)
        def _(j):
            lane = lax.broadcasted_iota(jnp.int32, (TK, dim), 1)
            pos = owner * cache + j * TK + lax.broadcasted_iota(jnp.int32, (TK, dim), 0)
            hidden = jnp.logical_and(lane == 0, pos >= visible_len)
            bias[f, pl.ds(pl.multiple_of(j * TK, TK), TK), :] = jnp.where(hidden, -BIG, 0.0).astype(BF)

    for cp in new_copies:
        cp.wait()
    kt = pltpu.einshape('phd->hpd', new_k[...].reshape(tok, kvh, dim))
    vt = pltpu.einshape('phd->hpd', new_v[...].reshape(tok, kvh, dim))
    for h in range(kvh):
        kbuf[h, pl.ds(cache, tok), :] = kt[h]
        vpad = jnp.concatenate([vt[h].astype(F32), jnp.zeros((dim - tok, dim), F32)], axis=0)
        vbuf[h, :, pl.ds(cache, dim)] = vpad.T.astype(BF)
    def kv_parts(h, lo, n):
        src = half * (1 - core) + h
        to = dict(device_id={'cp': mate}, device_id_type=MESH)
        k_rows, v_lanes = pl.ds(lo, tok if n == dim else n), pl.ds(lo, n)
        return (pltpu.make_async_remote_copy(
                    src_ref=kbuf.at[src, k_rows], dst_ref=kbuf.at[kvh + h, k_rows],
                    send_sem=kv_send.at[0, h], recv_sem=k_recv.at[h], **to),
                pltpu.make_async_remote_copy(
                    src_ref=vbuf.at[src, :, v_lanes], dst_ref=vbuf.at[kvh + h, :, v_lanes],
                    send_sem=kv_send.at[1, h], recv_sem=v_recv.at[h], **to))

    def kv_start(lo, n):
        for h in range(half):
            for cp in kv_parts(h, lo, n):
                cp.start()

    n_pairs = 4 * half

    def pair(i):
        code = lax.shift_right_logical(jnp.where(i < 8, ORDER[0], ORDER[1]), 4 * lax.rem(i, 8))
        slot = 2 * jnp.bitwise_and(code, 7)
        second = lax.div(jnp.bitwise_and(code, 15), 8)
        h = lax.rem(slot, half)
        kv = jnp.where(second == 1, kvh + h, half * core + h)
        owner = jnp.where(second == 1, mate, me)
        src = lax.div(slot, half)
        home = jnp.where(src == 0, me, jnp.where(src == 1, mate, jnp.where(src == 2, far, far_other)))
        return second, slot, kv, owner, home

    def load_q(slot):
        qt[slot] = qraw[slot].reshape(rows, dim).T

    def score_rhs(slot):
        return jnp.concatenate([qt[slot], pick[...]], axis=0)

    def qk_tile(kv, f, c, qv):
        sl = pl.ds(c * TK if isinstance(c, int) else pl.multiple_of(c * TK, TK), TK)
        lhs = jnp.concatenate([kbuf[kv, sl, :], bias[f, sl, :]], axis=1)
        return jnp.dot(lhs, qv, preferred_element_type=F32)

    def qk_new(kv, owner, home, qv):
        lhs = jnp.concatenate([kbuf[kv, pl.ds(cache, tok), :], jnp.zeros((tok, dim), BF)], axis=1)
        st = jnp.dot(lhs, qv, preferred_element_type=F32)
        key = owner * tok + lax.broadcasted_iota(jnp.int32, (tok, rows), 0)
        query = home * tok + lax.broadcasted_iota(jnp.int32, (tok, rows), 1) // ratio
        return jnp.where(key <= query, st, -BIG)

    def fold_max(mx, st):
        t = jnp.max(st.reshape(st.shape[0] // 8, 8, rows), axis=0)
        return t if mx is None else jnp.maximum(mx, t)

    f_0, slot_0, kv_0, owner_0, home_0 = pair(0)

    def first_scores(c):
        for e in range(2):
            st = qk_tile(kv_0 + e, f_0, c, score_rhs(slot_0 + e))
            sbuf[e][pl.ds(c * TK, TK), :] = st
            mbuf[e][...] = fold_max(mbuf[e][...], st)

    for j in range(n_raw):
        for cp in raw_copy(j):
            cp.wait()
        if j + RAW_DEPTH < n_raw:
            raw_start(j + RAW_DEPTH)

        @pl.loop(0, raw_pos // PREP)
        def _(i):
            base = pl.multiple_of(j * raw_pos + i * PREP, PREP)
            src = pl.ds(pl.multiple_of(base * kvh, PREP * kvh), PREP * kvh)
            xk = pltpu.einshape('phd->hpd', raw_k[src, :].reshape(PREP, kvh, dim))
            xv = pltpu.einshape('phd->hpd', raw_v[src, :].reshape(PREP, kvh, dim))
            for h in range(kvh):
                kbuf[h, pl.ds(base, PREP), :] = xk[h]
                vbuf[h, :, pl.ds(base, PREP)] = xv[h].T

        if j == 2:
            pl.semaphore_wait(barrier, 3)
            for k in range(3):
                for h in range(half):
                    q_copy(k, h).start()
            kv_start(cache, dim)
        if j % 2 and j > 1:
            kv_start((j - 3) * raw_pos, 2 * raw_pos)

    for h in range(half):
        own_q(h).wait()
    for h in range(half):
        load_q(h)
    for c in range(chunks):
        first_scores(c)
    for e in range(2):
        st = qk_new(kv_0 + e, owner_0, home_0, score_rhs(slot_0 + e))
        sbuf[e][pl.ds(cache, tok), :] = st
        mbuf[e][...] = fold_max(mbuf[e][...], st)
    kv_start(cache - 2 * raw_pos, 2 * raw_pos)

    def region(i, sc, sn, mc, mn, more=True):
        nxt = lax.rem(i + 1, n_pairs)
        f_n, slot_n, kv_n, owner_n, home_n = pair(nxt)
        second, slot, kv, _, _ = pair(i)
        later = jnp.minimum(i + 2, n_pairs - 1)
        ahead = pair(later)[1]

        @pl.when(among(i + 2, Q_PAIRS))
        def _():
            for e in range(2):
                pltpu.make_async_copy(qraw.at[ahead + e], qraw.at[ahead + e], q_recv.at[ahead + e]).wait()

        @pl.when(among(i + 1, KV_PAIRS))
        def _():
            for e in range(2):
                pltpu.make_async_copy(kbuf.at[kv_n + e], kbuf.at[kv_n + e], k_recv.at[kv_n + e - kvh]).wait()
                pltpu.make_async_copy(vbuf.at[kv_n + e], vbuf.at[kv_n + e], v_recv.at[kv_n + e - kvh]).wait()

        qv, m, decay, mx, l8, o = [], [], [], [None] * 2, [], [None] * 2
        for e in range(2):
            qv.append(score_rhs(slot_n + e) if more else None)
            m_old = jnp.where(second == 1, st_m[slot + e], -1e38)
            m.append(jnp.maximum(m_old, jnp.max(mc[e][...], axis=0, keepdims=True) * scale2))
            decay.append(jnp.exp2(m_old - m[e]))
            l8.append(jnp.zeros((8, rows), F32))
        for c in range(chunks):
            sl = pl.ds(c * TK, TK)
            for e in range(2):
                st = qk_tile(kv_n + e, f_n, c, qv[e]) if more else None
                p = jnp.exp2(sc[e][sl, :] * scale2 - m[e])
                if more:
                    sn[e][sl, :] = st
                    mx[e] = fold_max(mx[e], st)
                l8[e] = l8[e] + jnp.sum(p.reshape(TK // 8, 8, rows), axis=0)
                t = jnp.dot(vbuf[kv + e, :, sl], p.astype(BF), preferred_element_type=F32)
                o[e] = t if o[e] is None else o[e] + t
        sl = pl.ds(cache, tok)
        for e in range(2):
            p = jnp.exp2(sc[e][sl, :] * scale2 - m[e])
            if more:
                st = qk_new(kv_n + e, owner_n, home_n, qv[e])
                sn[e][sl, :] = st
                mn[e][...] = fold_max(mx[e], st)
            l8[e] = l8[e] + jnp.sum(p.reshape(tok // 8, 8, rows), axis=0)
            pb = jnp.concatenate([p.astype(BF), jnp.zeros((dim - tok, rows), BF)], axis=0)
            o[e] = o[e] + jnp.dot(vbuf[kv + e, :, pl.ds(cache, dim)], pb, preferred_element_type=F32)
        for e in range(2):
            st_o[slot + e] = jnp.where(second == 1, st_o[slot + e] * decay[e], 0.0) + o[e]
            st_l[slot + e] = jnp.where(second == 1, st_l[slot + e] * decay[e], 0.0) + jnp.sum(l8[e], axis=0, keepdims=True)
            st_m[slot + e] = m[e]
            if more:
                load_q(ahead + e)

    def partial_copies(u):
        return (pltpu.make_async_remote_copy(
                    src_ref=ps.at[u], dst_ref=pr.at[u], send_sem=p_send.at[0, u], recv_sem=p_recv.at[0, u],
                    device_id={'cp': far}, device_id_type=MESH),
                pltpu.make_async_remote_copy(
                    src_ref=psl.at[u], dst_ref=prl.at[u], send_sem=p_send.at[1, u], recv_sem=p_recv.at[1, u],
                    device_id={'cp': far}, device_id_type=MESH))

    def mate_out(u):
        hh = half * core + u - half
        return (pltpu.make_async_remote_copy(
                    src_ref=fo.at[u - half], dst_ref=out_ref.at[:, hh], send_sem=f_send.at[0, u - half],
                    recv_sem=f_recv.at[0, u - half], device_id={'cp': mate}, device_id_type=MESH),
                pltpu.make_async_remote_copy(
                    src_ref=fl.at[u - half], dst_ref=lse_ref.at[hh], send_sem=f_send.at[1, u - half],
                    recv_sem=f_recv.at[1, u - half], device_id={'cp': mate}, device_id_type=MESH))

    def finish(i):
        _, slot, _, _, _ = pair(i)

        @pl.when(among(i, R_PAIRS))
        def _():
            u = slot - 2 * half
            for e in range(2):
                l = st_l[slot + e]
                ps[u + e] = (st_o[slot + e] * (1.0 / l)).astype(BF)
                psl[u + e] = st_m[slot + e] + jnp.log2(l)
            for e in range(2):
                for cp in partial_copies(u + e):
                    cp.start()

        @pl.when(among(i, L_PAIRS))
        def _():
            u = slot
            for e in range(2):
                for cp in partial_copies(u + e):
                    cp.wait_recv()
            done = []
            for e in range(2):
                m_a, m_b = st_m[u + e], prl[u + e]
                m = jnp.maximum(m_a, m_b)
                a, b = jnp.exp2(m_a - m), jnp.exp2(m_b - m)
                l = st_l[u + e] * a + b
                inv = 1.0 / l
                o = st_o[u + e] * (a * inv) + pr[u + e].astype(F32) * (b * inv)
                done.append((o.T.astype(BF).reshape(tok, ratio, dim), (m + jnp.log2(l)) * math.log(2.0)))

            @pl.when(u < half)
            def _():
                for e in range(2):
                    out_ref[:, half * core + u + e] = done[e][0]
                    lse_ref[half * core + u + e] = done[e][1]

            @pl.when(u >= half)
            def _():
                for e in range(2):
                    fo[u - half + e] = done[e][0]
                    fl[u - half + e] = done[e][1]
                for e in range(2):
                    for cp in mate_out(u + e):
                        cp.start()

    def two(i, more):
        region(2 * i, sbuf[:2], sbuf[2:], mbuf[:2], mbuf[2:])
        finish(2 * i)
        region(2 * i + 1, sbuf[2:], sbuf[:2], mbuf[2:], mbuf[:2], more)
        finish(2 * i + 1)

    @pl.loop(0, n_pairs // 2 - 1)
    def _(i):
        two(i, True)

    two(jnp.int32(n_pairs // 2 - 1), False)

    for k in range(3):
        for h in range(half):
            q_copy(k, h).wait_send()
    for h in range(half):
        pltpu.make_async_copy(kbuf.at[h], kbuf.at[h], kv_send.at[0, h]).wait()
        pltpu.make_async_copy(vbuf.at[h], vbuf.at[h], kv_send.at[1, h]).wait()
    for u in range(2 * half):
        for cp in partial_copies(u):
            cp.wait_send()
    for u in range(half):
        for cp in mate_out(u + half):
            cp.wait_send()
            cp.wait_recv()


def place_kernel(out_ref, lse_ref, out_hbm, lse_hbm, lse_buf, sem):
    kvh, _, rows = lse_ref.shape
    tok, heads = lse_buf.shape
    ratio = heads // kvh
    write = pltpu.make_async_copy(out_ref, out_hbm, sem.at[0])
    write.start()
    x = lse_ref[...].reshape(kvh, rows)
    lane = lax.broadcasted_iota(jnp.int32, (kvh, heads), 1) // ratio
    head = lax.broadcasted_iota(jnp.int32, (kvh, heads), 0)
    per = heads // ratio
    blocks = [pltpu.roll(x[:, b * heads:(b + 1) * heads], 0, 1, stride=ratio, stride_axis=0) for b in range(tok // per)]
    for t in range(tok):
        turned = pltpu.roll(blocks[t // per], (heads - (t % per) * ratio) % heads, 1)
        lse_buf[pl.ds(t, 1), :] = jnp.sum(jnp.where(lane == head, turned, 0.0), axis=0, keepdims=True)
    lse_write = pltpu.make_async_copy(lse_buf, lse_hbm, sem.at[1])
    lse_write.start()
    write.wait()
    lse_write.wait()


def solution(mesh):
    tok_spec = P(('dp', 'cp'))

    def local(queries, key_new, value_new, key_cache, value_cache, prefix_len):
        tok, heads, dim = queries.shape
        cache, kvh = key_cache.shape[:2]
        ratio = heads // kvh
        half = kvh // 2
        rows = tok * ratio
        n_raw = cache // TK
        dma = pltpu.SemaphoreType.DMA
        hbm = pl.BlockSpec(memory_space=pltpu.HBM)
        vmem = pl.BlockSpec(memory_space=pltpu.VMEM)
        scratch = [
            pltpu.VMEM((cache * kvh, dim), BF),
            pltpu.VMEM((cache * kvh, dim), BF),
            pltpu.VMEM((tok * kvh, dim), BF),
            pltpu.VMEM((tok * kvh, dim), BF),
            pltpu.VMEM((kvh + half, cache + tok, dim), BF),
            pltpu.VMEM((kvh + half, dim, cache + dim), BF),
            pltpu.VMEM((2, cache, dim), BF),
            pltpu.VMEM((4 * half, tok, ratio, dim), BF),
            pltpu.VMEM((4 * half, dim, rows), BF),
            pltpu.VMEM((dim, rows), BF),
            pltpu.SMEM((1,), jnp.int32),
            (pltpu.VMEM((cache + tok, rows), F32),) * 4,
            (pltpu.VMEM((8, rows), F32),) * 4,
            pltpu.VMEM((4 * half, dim, rows), F32),
            pltpu.VMEM((4 * half, 1, rows), F32),
            pltpu.VMEM((4 * half, 1, rows), F32),
            pltpu.VMEM((2 * half, dim, rows), BF),
            pltpu.VMEM((2 * half, 1, rows), F32),
            pltpu.VMEM((2 * half, dim, rows), BF),
            pltpu.VMEM((2 * half, 1, rows), F32),
            pltpu.VMEM((half, tok, ratio, dim), BF),
            pltpu.VMEM((half, 1, rows), F32),
            dma((2, n_raw)), dma((3,)), dma((3 * half,)), dma((4 * half,)), dma((2, half)), dma((half,)), dma((half,)),
            dma((2, 2 * half)), dma((2, 2 * half)), dma((2, half)), dma((2, half)),
        ]
        flops = 4 * heads * tok * 4 * cache * dim
        out, lse = pl.pallas_call(
            attend_kernel,
            out_shape=(pltpu.VMEM((tok, kvh, ratio, dim), BF), pltpu.VMEM((kvh, 1, rows), F32)),
            in_specs=[hbm] * 6,
            out_specs=(vmem, vmem),
            scratch_shapes=scratch,
            compiler_params=pltpu.CompilerParams(collective_id=0, has_side_effects=True, vmem_limit_bytes=60 * 2 ** 20),
            cost_estimate=pl.CostEstimate(flops=flops, bytes_accessed=4 * cache * kvh * dim, transcendentals=heads * tok * 4 * cache),
            name='attend',
        )(queries.reshape(tok, kvh, ratio, dim), key_new.reshape(tok * kvh, dim), value_new.reshape(tok * kvh, dim),
          key_cache.reshape(cache * kvh, dim), value_cache.reshape(cache * kvh, dim), prefix_len)
        out, row_lse = pl.pallas_call(
            place_kernel,
            out_shape=(jax.ShapeDtypeStruct((tok, heads, dim), BF), jax.ShapeDtypeStruct((tok, heads), F32)),
            in_specs=[vmem, vmem],
            out_specs=(hbm, hbm),
            scratch_shapes=[pltpu.VMEM((tok, heads), F32), dma((2,))],
            compiler_params=pltpu.CompilerParams(vmem_limit_bytes=2 * 2 ** 20),
            name='place',
        )(out.reshape(tok, heads, dim), lse)
        return out, row_lse

    return jax.shard_map(local, mesh=mesh, in_specs=(tok_spec, tok_spec, tok_spec, tok_spec, tok_spec, P('dp')),
                         out_specs=(tok_spec, tok_spec), check_vma=False)
```

```python
import functools
import math

import jax
import jax.numpy as jnp
from jax import lax
from jax.experimental import pallas as pl
from jax.experimental.pallas import tpu as pltpu
from jax.sharding import PartitionSpec as P

MESH = pl.DeviceIdType.MESH
BIG = 1e30
TK = 256
PREP = 128
RAW_DEPTH = 3
BF = jnp.bfloat16
SEQ = ((0, 0), (2, 0), (4, 0), (12, 0), (14, 0), (12, 1), (8, 0), (14, 1),
       (10, 0), (8, 1), (10, 1), (6, 0), (4, 1), (6, 1), (0, 1), (2, 1))
F32 = jnp.float32


def _packed(part):
    v = sum((slot // 2 + 8 * second) << (4 * k) for k, (slot, second) in enumerate(part))
    return v - (1 << 32) if v >= 1 << 31 else v


ORDER = (_packed(SEQ[:8]), _packed(SEQ[8:]))
Q_PAIRS = tuple(SEQ.index((s, 0)) for s in range(4, 16, 2))
KV_PAIRS = tuple(next(k for k, (s, f) in enumerate(SEQ) if f and s % 4 == h) for h in (0, 2))
R_PAIRS = tuple(k for k, (s, f) in enumerate(SEQ) if f and s >= 8)
L_PAIRS = tuple(k for k, (s, f) in enumerate(SEQ) if f and s < 8)


def among(i, ks):
    hit = i == ks[0]
    for k in ks[1:]:
        hit = jnp.logical_or(hit, i == k)
    return hit


def attend_kernel(q_hbm, kn_hbm, vn_hbm, kc_hbm, vc_hbm, plen_hbm, out_ref, lse_ref,
                  raw_k, raw_v, new_k, new_v, kbuf, vbuf, bias, qraw, qt, pick, plen, sbuf, mbuf,
                  st_o, st_m, st_l, ps, psl, pr, prl, fo, fl,
                  raw_sem, new_sem, q_send, q_recv, kv_send, k_recv, v_recv, p_send, p_recv, f_send, f_recv):
    tok, kvh, ratio, dim = q_hbm.shape
    cache = kc_hbm.shape[0] // kvh
    half = kvh // 2
    rows = tok * ratio
    n_raw = raw_sem.shape[1]
    raw_pos = cache // n_raw
    chunks = cache // TK
    scale2 = dim ** -0.5 * math.log2(math.e)

    me = lax.axis_index('cp')
    core = lax.rem(me, 2)
    chip2 = me - core
    mate = chip2 + 1 - core
    far = lax.rem(chip2 + 2, 4) + core
    far_other = lax.rem(chip2 + 2, 4) + 1 - core

    def raw_copy(j):
        sl = pl.ds(j * raw_pos * kvh, raw_pos * kvh)
        return (pltpu.make_async_copy(kc_hbm.at[sl], raw_k.at[sl], raw_sem.at[0, j]),
                pltpu.make_async_copy(vc_hbm.at[sl], raw_v.at[sl], raw_sem.at[1, j]))

    def own_q(h):
        return pltpu.make_async_copy(q_hbm.at[:, half * core + h], qraw.at[h], q_recv.at[h])

    def raw_start(j):
        for cp in raw_copy(j):
            cp.start()

    for j in range(RAW_DEPTH):
        raw_start(j)
    plen_copy = pltpu.make_async_copy(plen_hbm, plen, new_sem.at[2])
    plen_copy.start()
    new_copies = (pltpu.make_async_copy(kn_hbm, new_k, new_sem.at[0]),
                  pltpu.make_async_copy(vn_hbm, new_v, new_sem.at[1]))
    for cp in new_copies:
        cp.start()
    for h in range(half):
        own_q(h).start()

    barrier = pltpu.get_barrier_semaphore()
    for peer in (mate, far, far_other):
        pl.semaphore_signal(barrier, inc=1, device_id={'cp': peer}, device_id_type=MESH)

    pick[...] = jnp.where(lax.broadcasted_iota(jnp.int32, (dim, rows), 0) == 0, 1.0, 0.0).astype(BF)
    for e in range(2):
        mbuf[e][...] = jnp.full((8, rows), -3e38, F32)

    def q_copy(k, h):
        peer, base = ((far_other, 3 * half), (far, 2 * half), (mate, half))[k]
        peer_core = (1 - core, core, 1 - core)[k]
        return pltpu.make_async_remote_copy(
            src_ref=q_hbm.at[:, half * peer_core + h], dst_ref=qraw.at[base + h],
            send_sem=q_send.at[k * half + h], recv_sem=q_recv.at[base + h],
            device_id={'cp': peer}, device_id_type=MESH)

    plen_copy.wait()
    visible_len = plen[0]
    for f, owner in enumerate((me, mate)):
        @pl.loop(0, chunks)
        def _(j):
            lane = lax.broadcasted_iota(jnp.int32, (TK, dim), 1)
            pos = owner * cache + j * TK + lax.broadcasted_iota(jnp.int32, (TK, dim), 0)
            hidden = jnp.logical_and(lane == 0, pos >= visible_len)
            bias[f, pl.ds(pl.multiple_of(j * TK, TK), TK), :] = jnp.where(hidden, -BIG, 0.0).astype(BF)

    for cp in new_copies:
        cp.wait()
    kt = pltpu.einshape('phd->hpd', new_k[...].reshape(tok, kvh, dim))
    vt = pltpu.einshape('phd->hpd', new_v[...].reshape(tok, kvh, dim))
    for h in range(kvh):
        kbuf[h, pl.ds(cache, tok), :] = kt[h]
        vpad = jnp.concatenate([vt[h].astype(F32), jnp.zeros((dim - tok, dim), F32)], axis=0)
        vbuf[h, :, pl.ds(cache, dim)] = vpad.T.astype(BF)
    def kv_parts(h, lo, n):
        src = half * (1 - core) + h
        to = dict(device_id={'cp': mate}, device_id_type=MESH)
        k_rows, v_lanes = pl.ds(lo, tok if n == dim else n), pl.ds(lo, n)
        return (pltpu.make_async_remote_copy(
                    src_ref=kbuf.at[src, k_rows], dst_ref=kbuf.at[kvh + h, k_rows],
                    send_sem=kv_send.at[0, h], recv_sem=k_recv.at[h], **to),
                pltpu.make_async_remote_copy(
                    src_ref=vbuf.at[src, :, v_lanes], dst_ref=vbuf.at[kvh + h, :, v_lanes],
                    send_sem=kv_send.at[1, h], recv_sem=v_recv.at[h], **to))

    def kv_start(lo, n):
        for h in range(half):
            for cp in kv_parts(h, lo, n):
                cp.start()

    n_pairs = 4 * half

    def pair(i):
        code = lax.shift_right_logical(jnp.where(i < 8, ORDER[0], ORDER[1]), 4 * lax.rem(i, 8))
        slot = 2 * jnp.bitwise_and(code, 7)
        second = lax.div(jnp.bitwise_and(code, 15), 8)
        h = lax.rem(slot, half)
        kv = jnp.where(second == 1, kvh + h, half * core + h)
        owner = jnp.where(second == 1, mate, me)
        src = lax.div(slot, half)
        home = jnp.where(src == 0, me, jnp.where(src == 1, mate, jnp.where(src == 2, far, far_other)))
        return second, slot, kv, owner, home

    def load_q(slot):
        qt[slot] = qraw[slot].reshape(rows, dim).T

    def score_rhs(slot):
        return jnp.concatenate([qt[slot], pick[...]], axis=0)

    def qk_tile(kv, f, c, qv):
        sl = pl.ds(c * TK if isinstance(c, int) else pl.multiple_of(c * TK, TK), TK)
        lhs = jnp.concatenate([kbuf[kv, sl, :], bias[f, sl, :]], axis=1)
        return jnp.dot(lhs, qv, preferred_element_type=F32)

    def qk_new(kv, owner, home, qv):
        lhs = jnp.concatenate([kbuf[kv, pl.ds(cache, tok), :], jnp.zeros((tok, dim), BF)], axis=1)
        st = jnp.dot(lhs, qv, preferred_element_type=F32)
        key = owner * tok + lax.broadcasted_iota(jnp.int32, (tok, rows), 0)
        query = home * tok + lax.broadcasted_iota(jnp.int32, (tok, rows), 1) // ratio
        return jnp.where(key <= query, st, -BIG)

    def fold_max(mx, st):
        t = jnp.max(st.reshape(st.shape[0] // 8, 8, rows), axis=0)
        return t if mx is None else jnp.maximum(mx, t)

    f_0, slot_0, kv_0, owner_0, home_0 = pair(0)

    def first_scores(c):
        for e in range(2):
            st = qk_tile(kv_0 + e, f_0, c, score_rhs(slot_0 + e))
            sbuf[e][pl.ds(c * TK, TK), :] = st
            mbuf[e][...] = fold_max(mbuf[e][...], st)

    for j in range(n_raw):
        for cp in raw_copy(j):
            cp.wait()
        if j + RAW_DEPTH < n_raw:
            raw_start(j + RAW_DEPTH)

        @pl.loop(0, raw_pos // PREP)
        def _(i):
            base = pl.multiple_of(j * raw_pos + i * PREP, PREP)
            src = pl.ds(pl.multiple_of(base * kvh, PREP * kvh), PREP * kvh)
            xk = pltpu.einshape('phd->hpd', raw_k[src, :].reshape(PREP, kvh, dim))
            xv = pltpu.einshape('phd->hpd', raw_v[src, :].reshape(PREP, kvh, dim))
            for h in range(kvh):
                kbuf[h, pl.ds(base, PREP), :] = xk[h]
                vbuf[h, :, pl.ds(base, PREP)] = xv[h].T

        if j == 1:
            pl.semaphore_wait(barrier, 3)
            for k in range(3):
                for h in range(half):
                    q_copy(k, h).start()
            kv_start(cache, dim)
        if j % 2 and j > 1:
            kv_start((j - 3) * raw_pos, 2 * raw_pos)

    for h in range(half):
        own_q(h).wait()
    for h in range(half):
        load_q(h)
    for c in range(chunks):
        first_scores(c)
    for e in range(2):
        st = qk_new(kv_0 + e, owner_0, home_0, score_rhs(slot_0 + e))
        sbuf[e][pl.ds(cache, tok), :] = st
        mbuf[e][...] = fold_max(mbuf[e][...], st)
    kv_start(cache - 2 * raw_pos, 2 * raw_pos)

    def region(i, sc, sn, mc, mn, more=True):
        nxt = lax.rem(i + 1, n_pairs)
        f_n, slot_n, kv_n, owner_n, home_n = pair(nxt)
        second, slot, kv, _, _ = pair(i)
        later = jnp.minimum(i + 2, n_pairs - 1)
        ahead = pair(later)[1]

        @pl.when(among(i + 2, Q_PAIRS))
        def _():
            for e in range(2):
                pltpu.make_async_copy(qraw.at[ahead + e], qraw.at[ahead + e], q_recv.at[ahead + e]).wait()

        @pl.when(among(i + 1, KV_PAIRS))
        def _():
            for e in range(2):
                pltpu.make_async_copy(kbuf.at[kv_n + e], kbuf.at[kv_n + e], k_recv.at[kv_n + e - kvh]).wait()
                pltpu.make_async_copy(vbuf.at[kv_n + e], vbuf.at[kv_n + e], v_recv.at[kv_n + e - kvh]).wait()

        qv, m, decay, mx, l8, o = [], [], [], [None] * 2, [], [None] * 2
        for e in range(2):
            qv.append(score_rhs(slot_n + e) if more else None)
            m_old = jnp.where(second == 1, st_m[slot + e], -1e38)
            m.append(jnp.maximum(m_old, jnp.max(mc[e][...], axis=0, keepdims=True) * scale2))
            decay.append(jnp.exp2(m_old - m[e]))
            l8.append(jnp.zeros((8, rows), F32))
        for c in range(chunks):
            sl = pl.ds(c * TK, TK)
            for e in range(2):
                st = qk_tile(kv_n + e, f_n, c, qv[e]) if more else None
                p = jnp.exp2(sc[e][sl, :] * scale2 - m[e])
                if more:
                    sn[e][sl, :] = st
                    mx[e] = fold_max(mx[e], st)
                l8[e] = l8[e] + jnp.sum(p.reshape(TK // 8, 8, rows), axis=0)
                t = jnp.dot(vbuf[kv + e, :, sl], p.astype(BF), preferred_element_type=F32)
                o[e] = t if o[e] is None else o[e] + t
        sl = pl.ds(cache, tok)
        for e in range(2):
            p = jnp.exp2(sc[e][sl, :] * scale2 - m[e])
            if more:
                st = qk_new(kv_n + e, owner_n, home_n, qv[e])
                sn[e][sl, :] = st
                mn[e][...] = fold_max(mx[e], st)
            l8[e] = l8[e] + jnp.sum(p.reshape(tok // 8, 8, rows), axis=0)
            pb = jnp.concatenate([p.astype(BF), jnp.zeros((dim - tok, rows), BF)], axis=0)
            o[e] = o[e] + jnp.dot(vbuf[kv + e, :, pl.ds(cache, dim)], pb, preferred_element_type=F32)
        for e in range(2):
            st_o[slot + e] = jnp.where(second == 1, st_o[slot + e] * decay[e], 0.0) + o[e]
            st_l[slot + e] = jnp.where(second == 1, st_l[slot + e] * decay[e], 0.0) + jnp.sum(l8[e], axis=0, keepdims=True)
            st_m[slot + e] = m[e]
            if more:
                load_q(ahead + e)

    def partial_copies(u):
        return (pltpu.make_async_remote_copy(
                    src_ref=ps.at[u], dst_ref=pr.at[u], send_sem=p_send.at[0, u], recv_sem=p_recv.at[0, u],
                    device_id={'cp': far}, device_id_type=MESH),
                pltpu.make_async_remote_copy(
                    src_ref=psl.at[u], dst_ref=prl.at[u], send_sem=p_send.at[1, u], recv_sem=p_recv.at[1, u],
                    device_id={'cp': far}, device_id_type=MESH))

    def mate_out(u):
        hh = half * core + u - half
        return (pltpu.make_async_remote_copy(
                    src_ref=fo.at[u - half], dst_ref=out_ref.at[:, hh], send_sem=f_send.at[0, u - half],
                    recv_sem=f_recv.at[0, u - half], device_id={'cp': mate}, device_id_type=MESH),
                pltpu.make_async_remote_copy(
                    src_ref=fl.at[u - half], dst_ref=lse_ref.at[hh], send_sem=f_send.at[1, u - half],
                    recv_sem=f_recv.at[1, u - half], device_id={'cp': mate}, device_id_type=MESH))

    def finish(i):
        _, slot, _, _, _ = pair(i)

        @pl.when(among(i, R_PAIRS))
        def _():
            u = slot - 2 * half
            for e in range(2):
                l = st_l[slot + e]
                ps[u + e] = (st_o[slot + e] * (1.0 / l)).astype(BF)
                psl[u + e] = st_m[slot + e] + jnp.log2(l)
            for e in range(2):
                for cp in partial_copies(u + e):
                    cp.start()

        @pl.when(among(i, L_PAIRS))
        def _():
            u = slot
            for e in range(2):
                for cp in partial_copies(u + e):
                    cp.wait_recv()
            done = []
            for e in range(2):
                m_a, m_b = st_m[u + e], prl[u + e]
                m = jnp.maximum(m_a, m_b)
                a, b = jnp.exp2(m_a - m), jnp.exp2(m_b - m)
                l = st_l[u + e] * a + b
                inv = 1.0 / l
                o = st_o[u + e] * (a * inv) + pr[u + e].astype(F32) * (b * inv)
                done.append((o.T.astype(BF).reshape(tok, ratio, dim), (m + jnp.log2(l)) * math.log(2.0)))

            @pl.when(u < half)
            def _():
                for e in range(2):
                    out_ref[:, half * core + u + e] = done[e][0]
                    lse_ref[half * core + u + e] = done[e][1]

            @pl.when(u >= half)
            def _():
                for e in range(2):
                    fo[u - half + e] = done[e][0]
                    fl[u - half + e] = done[e][1]
                for e in range(2):
                    for cp in mate_out(u + e):
                        cp.start()

    def two(i, more):
        region(2 * i, sbuf[:2], sbuf[2:], mbuf[:2], mbuf[2:])
        finish(2 * i)
        region(2 * i + 1, sbuf[2:], sbuf[:2], mbuf[2:], mbuf[:2], more)
        finish(2 * i + 1)

    @pl.loop(0, n_pairs // 2 - 1)
    def _(i):
        two(i, True)

    two(jnp.int32(n_pairs // 2 - 1), False)

    for k in range(3):
        for h in range(half):
            q_copy(k, h).wait_send()
    for h in range(half):
        pltpu.make_async_copy(kbuf.at[h], kbuf.at[h], kv_send.at[0, h]).wait()
        pltpu.make_async_copy(vbuf.at[h], vbuf.at[h], kv_send.at[1, h]).wait()
    for u in range(2 * half):
        for cp in partial_copies(u):
            cp.wait_send()
    for u in range(half):
        for cp in mate_out(u + half):
            cp.wait_send()
            cp.wait_recv()


def place_kernel(out_ref, lse_ref, out_hbm, lse_hbm, lse_buf, sem):
    kvh, _, rows = lse_ref.shape
    tok, heads = lse_buf.shape
    ratio = heads // kvh
    write = pltpu.make_async_copy(out_ref, out_hbm, sem.at[0])
    write.start()
    x = lse_ref[...].reshape(kvh, rows)
    lane = lax.broadcasted_iota(jnp.int32, (kvh, heads), 1) // ratio
    head = lax.broadcasted_iota(jnp.int32, (kvh, heads), 0)
    per = heads // ratio
    blocks = [pltpu.roll(x[:, b * heads:(b + 1) * heads], 0, 1, stride=ratio, stride_axis=0) for b in range(tok // per)]
    for t in range(tok):
        turned = pltpu.roll(blocks[t // per], (heads - (t % per) * ratio) % heads, 1)
        lse_buf[pl.ds(t, 1), :] = jnp.sum(jnp.where(lane == head, turned, 0.0), axis=0, keepdims=True)
    lse_write = pltpu.make_async_copy(lse_buf, lse_hbm, sem.at[1])
    lse_write.start()
    write.wait()
    lse_write.wait()


def solution(mesh):
    tok_spec = P(('dp', 'cp'))

    def local(queries, key_new, value_new, key_cache, value_cache, prefix_len):
        tok, heads, dim = queries.shape
        cache, kvh = key_cache.shape[:2]
        ratio = heads // kvh
        half = kvh // 2
        rows = tok * ratio
        n_raw = cache // TK
        dma = pltpu.SemaphoreType.DMA
        hbm = pl.BlockSpec(memory_space=pltpu.HBM)
        vmem = pl.BlockSpec(memory_space=pltpu.VMEM)
        scratch = [
            pltpu.VMEM((cache * kvh, dim), BF),
            pltpu.VMEM((cache * kvh, dim), BF),
            pltpu.VMEM((tok * kvh, dim), BF),
            pltpu.VMEM((tok * kvh, dim), BF),
            pltpu.VMEM((kvh + half, cache + tok, dim), BF),
            pltpu.VMEM((kvh + half, dim, cache + dim), BF),
            pltpu.VMEM((2, cache, dim), BF),
            pltpu.VMEM((4 * half, tok, ratio, dim), BF),
            pltpu.VMEM((4 * half, dim, rows), BF),
            pltpu.VMEM((dim, rows), BF),
            pltpu.SMEM((1,), jnp.int32),
            (pltpu.VMEM((cache + tok, rows), F32),) * 4,
            (pltpu.VMEM((8, rows), F32),) * 4,
            pltpu.VMEM((4 * half, dim, rows), F32),
            pltpu.VMEM((4 * half, 1, rows), F32),
            pltpu.VMEM((4 * half, 1, rows), F32),
            pltpu.VMEM((2 * half, dim, rows), BF),
            pltpu.VMEM((2 * half, 1, rows), F32),
            pltpu.VMEM((2 * half, dim, rows), BF),
            pltpu.VMEM((2 * half, 1, rows), F32),
            pltpu.VMEM((half, tok, ratio, dim), BF),
            pltpu.VMEM((half, 1, rows), F32),
            dma((2, n_raw)), dma((3,)), dma((3 * half,)), dma((4 * half,)), dma((2, half)), dma((half,)), dma((half,)),
            dma((2, 2 * half)), dma((2, 2 * half)), dma((2, half)), dma((2, half)),
        ]
        flops = 4 * heads * tok * 4 * cache * dim
        out, lse = pl.pallas_call(
            attend_kernel,
            out_shape=(pltpu.VMEM((tok, kvh, ratio, dim), BF), pltpu.VMEM((kvh, 1, rows), F32)),
            in_specs=[hbm] * 6,
            out_specs=(vmem, vmem),
            scratch_shapes=scratch,
            compiler_params=pltpu.CompilerParams(collective_id=0, has_side_effects=True, vmem_limit_bytes=60 * 2 ** 20),
            cost_estimate=pl.CostEstimate(flops=flops, bytes_accessed=4 * cache * kvh * dim, transcendentals=heads * tok * 4 * cache),
            name='attend',
        )(queries.reshape(tok, kvh, ratio, dim), key_new.reshape(tok * kvh, dim), value_new.reshape(tok * kvh, dim),
          key_cache.reshape(cache * kvh, dim), value_cache.reshape(cache * kvh, dim), prefix_len)
        out, row_lse = pl.pallas_call(
            place_kernel,
            out_shape=(jax.ShapeDtypeStruct((tok, heads, dim), BF), jax.ShapeDtypeStruct((tok, heads), F32)),
            in_specs=[vmem, vmem],
            out_specs=(hbm, hbm),
            scratch_shapes=[pltpu.VMEM((tok, heads), F32), dma((2,))],
            compiler_params=pltpu.CompilerParams(vmem_limit_bytes=2 * 2 ** 20),
            name='place',
        )(out.reshape(tok, heads, dim), lse)
        return out, row_lse

    return jax.shard_map(local, mesh=mesh, in_specs=(tok_spec, tok_spec, tok_spec, tok_spec, tok_spec, P('dp')),
                         out_specs=(tok_spec, tok_spec), check_vma=False)
```

```python
import functools
import math

import jax
import jax.numpy as jnp
from jax import lax
from jax.experimental import pallas as pl
from jax.experimental.pallas import tpu as pltpu
from jax.sharding import PartitionSpec as P

MESH = pl.DeviceIdType.MESH
BIG = 1e30
TK = 256
PREP = 128
RAW_DEPTH = 3
BF = jnp.bfloat16
SEQ = ((0, 0), (2, 0), (4, 0), (12, 0), (14, 0), (12, 1), (8, 0), (14, 1),
       (10, 0), (8, 1), (10, 1), (6, 0), (4, 1), (6, 1), (0, 1), (2, 1))
F32 = jnp.float32


def _packed(part):
    v = sum((slot // 2 + 8 * second) << (4 * k) for k, (slot, second) in enumerate(part))
    return v - (1 << 32) if v >= 1 << 31 else v


ORDER = (_packed(SEQ[:8]), _packed(SEQ[8:]))
Q_PAIRS = tuple(SEQ.index((s, 0)) for s in range(4, 16, 2))
KV_PAIRS = tuple(next(k for k, (s, f) in enumerate(SEQ) if f and s % 4 == h) for h in (0, 2))
R_PAIRS = tuple(k for k, (s, f) in enumerate(SEQ) if f and s >= 8)
L_PAIRS = tuple(k for k, (s, f) in enumerate(SEQ) if f and s < 8)


def among(i, ks):
    hit = i == ks[0]
    for k in ks[1:]:
        hit = jnp.logical_or(hit, i == k)
    return hit


def attend_kernel(q_hbm, kn_hbm, vn_hbm, kc_hbm, vc_hbm, plen_ref, out_ref, lse_ref,
                  raw_k, raw_v, new_k, new_v, kbuf, vbuf, bias, qraw, qt, pick, sbuf, mbuf,
                  st_o, st_m, st_l, ps, psl, pr, prl, fo, fl,
                  raw_sem, new_sem, q_send, q_recv, kv_send, k_recv, v_recv, p_send, p_recv, f_send, f_recv):
    tok, kvh, ratio, dim = q_hbm.shape
    cache = kc_hbm.shape[0] // kvh
    half = kvh // 2
    rows = tok * ratio
    n_raw = raw_sem.shape[1]
    raw_pos = cache // n_raw
    chunks = cache // TK
    scale2 = dim ** -0.5 * math.log2(math.e)

    me = lax.axis_index('cp')
    core = lax.rem(me, 2)
    chip2 = me - core
    mate = chip2 + 1 - core
    far = lax.rem(chip2 + 2, 4) + core
    far_other = lax.rem(chip2 + 2, 4) + 1 - core

    def raw_copy(j):
        sl = pl.ds(j * raw_pos * kvh, raw_pos * kvh)
        return (pltpu.make_async_copy(kc_hbm.at[sl], raw_k.at[sl], raw_sem.at[0, j]),
                pltpu.make_async_copy(vc_hbm.at[sl], raw_v.at[sl], raw_sem.at[1, j]))

    def own_q(h):
        return pltpu.make_async_copy(q_hbm.at[:, half * core + h], qraw.at[h], q_recv.at[h])

    def raw_start(j):
        for cp in raw_copy(j):
            cp.start()

    for j in range(RAW_DEPTH):
        raw_start(j)
    new_copies = (pltpu.make_async_copy(kn_hbm, new_k, new_sem.at[0]),
                  pltpu.make_async_copy(vn_hbm, new_v, new_sem.at[1]))
    for cp in new_copies:
        cp.start()
    for h in range(half):
        own_q(h).start()

    barrier = pltpu.get_barrier_semaphore()
    for peer in (mate, far, far_other):
        pl.semaphore_signal(barrier, inc=1, device_id={'cp': peer}, device_id_type=MESH)

    pick[...] = jnp.where(lax.broadcasted_iota(jnp.int32, (dim, rows), 0) == 0, 1.0, 0.0).astype(BF)
    for e in range(2):
        mbuf[e][...] = jnp.full((8, rows), -3e38, F32)

    def q_copy(k, h):
        peer, base = ((far_other, 3 * half), (far, 2 * half), (mate, half))[k]
        peer_core = (1 - core, core, 1 - core)[k]
        return pltpu.make_async_remote_copy(
            src_ref=q_hbm.at[:, half * peer_core + h], dst_ref=qraw.at[base + h],
            send_sem=q_send.at[k * half + h], recv_sem=q_recv.at[base + h],
            device_id={'cp': peer}, device_id_type=MESH)

    visible_len = plen_ref[0]
    for f, owner in enumerate((me, mate)):
        @pl.loop(0, chunks)
        def _(j):
            lane = lax.broadcasted_iota(jnp.int32, (TK, dim), 1)
            pos = owner * cache + j * TK + lax.broadcasted_iota(jnp.int32, (TK, dim), 0)
            hidden = jnp.logical_and(lane == 0, pos >= visible_len)
            bias[f, pl.ds(pl.multiple_of(j * TK, TK), TK), :] = jnp.where(hidden, -BIG, 0.0).astype(BF)

    for cp in new_copies:
        cp.wait()
    kt = pltpu.einshape('phd->hpd', new_k[...].reshape(tok, kvh, dim))
    vt = pltpu.einshape('phd->hpd', new_v[...].reshape(tok, kvh, dim))
    for h in range(kvh):
        kbuf[h, pl.ds(cache, tok), :] = kt[h]
        vpad = jnp.concatenate([vt[h].astype(F32), jnp.zeros((dim - tok, dim), F32)], axis=0)
        vbuf[h, :, pl.ds(cache, dim)] = vpad.T.astype(BF)
    def kv_parts(h, lo, n):
        src = half * (1 - core) + h
        to = dict(device_id={'cp': mate}, device_id_type=MESH)
        k_rows, v_lanes = pl.ds(lo, tok if n == dim else n), pl.ds(lo, n)
        return (pltpu.make_async_remote_copy(
                    src_ref=kbuf.at[src, k_rows], dst_ref=kbuf.at[kvh + h, k_rows],
                    send_sem=kv_send.at[0, h], recv_sem=k_recv.at[h], **to),
                pltpu.make_async_remote_copy(
                    src_ref=vbuf.at[src, :, v_lanes], dst_ref=vbuf.at[kvh + h, :, v_lanes],
                    send_sem=kv_send.at[1, h], recv_sem=v_recv.at[h], **to))

    def kv_start(lo, n):
        for h in range(half):
            for cp in kv_parts(h, lo, n):
                cp.start()

    n_pairs = 4 * half

    def pair(i):
        code = lax.shift_right_logical(jnp.where(i < 8, ORDER[0], ORDER[1]), 4 * lax.rem(i, 8))
        slot = 2 * jnp.bitwise_and(code, 7)
        second = lax.div(jnp.bitwise_and(code, 15), 8)
        h = lax.rem(slot, half)
        kv = jnp.where(second == 1, kvh + h, half * core + h)
        owner = jnp.where(second == 1, mate, me)
        src = lax.div(slot, half)
        home = jnp.where(src == 0, me, jnp.where(src == 1, mate, jnp.where(src == 2, far, far_other)))
        return second, slot, kv, owner, home

    def load_q(slot):
        qt[slot] = qraw[slot].reshape(rows, dim).T

    def score_rhs(slot):
        return jnp.concatenate([qt[slot], pick[...]], axis=0)

    def qk_tile(kv, f, c, qv):
        sl = pl.ds(c * TK if isinstance(c, int) else pl.multiple_of(c * TK, TK), TK)
        lhs = jnp.concatenate([kbuf[kv, sl, :], bias[f, sl, :]], axis=1)
        return jnp.dot(lhs, qv, preferred_element_type=F32)

    def qk_new(kv, owner, home, qv):
        lhs = jnp.concatenate([kbuf[kv, pl.ds(cache, tok), :], jnp.zeros((tok, dim), BF)], axis=1)
        st = jnp.dot(lhs, qv, preferred_element_type=F32)
        key = owner * tok + lax.broadcasted_iota(jnp.int32, (tok, rows), 0)
        query = home * tok + lax.broadcasted_iota(jnp.int32, (tok, rows), 1) // ratio
        return jnp.where(key <= query, st, -BIG)

    def fold_max(mx, st):
        t = jnp.max(st.reshape(st.shape[0] // 8, 8, rows), axis=0)
        return t if mx is None else jnp.maximum(mx, t)

    f_0, slot_0, kv_0, owner_0, home_0 = pair(0)

    def first_scores(c):
        for e in range(2):
            st = qk_tile(kv_0 + e, f_0, c, score_rhs(slot_0 + e))
            sbuf[e][pl.ds(c * TK, TK), :] = st
            mbuf[e][...] = fold_max(mbuf[e][...], st)

    for j in range(n_raw):
        for cp in raw_copy(j):
            cp.wait()
        if j + RAW_DEPTH < n_raw:
            raw_start(j + RAW_DEPTH)

        @pl.loop(0, raw_pos // PREP)
        def _(i):
            base = pl.multiple_of(j * raw_pos + i * PREP, PREP)
            src = pl.ds(pl.multiple_of(base * kvh, PREP * kvh), PREP * kvh)
            xk = pltpu.einshape('phd->hpd', raw_k[src, :].reshape(PREP, kvh, dim))
            xv = pltpu.einshape('phd->hpd', raw_v[src, :].reshape(PREP, kvh, dim))
            for h in range(kvh):
                kbuf[h, pl.ds(base, PREP), :] = xk[h]
                vbuf[h, :, pl.ds(base, PREP)] = xv[h].T

        if j == 1:
            pl.semaphore_wait(barrier, 3)
            for k in range(3):
                for h in range(half):
                    q_copy(k, h).start()
            kv_start(cache, dim)
        if j % 2 and j > 1:
            kv_start((j - 3) * raw_pos, 2 * raw_pos)

    for h in range(half):
        own_q(h).wait()
    for h in range(half):
        load_q(h)
    for c in range(chunks):
        first_scores(c)
    for e in range(2):
        st = qk_new(kv_0 + e, owner_0, home_0, score_rhs(slot_0 + e))
        sbuf[e][pl.ds(cache, tok), :] = st
        mbuf[e][...] = fold_max(mbuf[e][...], st)
    kv_start(cache - 2 * raw_pos, 2 * raw_pos)

    def region(i, sc, sn, mc, mn, more=True):
        nxt = lax.rem(i + 1, n_pairs)
        f_n, slot_n, kv_n, owner_n, home_n = pair(nxt)
        second, slot, kv, _, _ = pair(i)
        later = jnp.minimum(i + 2, n_pairs - 1)
        ahead = pair(later)[1]

        @pl.when(among(i + 2, Q_PAIRS))
        def _():
            for e in range(2):
                pltpu.make_async_copy(qraw.at[ahead + e], qraw.at[ahead + e], q_recv.at[ahead + e]).wait()

        @pl.when(among(i + 1, KV_PAIRS))
        def _():
            for e in range(2):
                pltpu.make_async_copy(kbuf.at[kv_n + e], kbuf.at[kv_n + e], k_recv.at[kv_n + e - kvh]).wait()
                pltpu.make_async_copy(vbuf.at[kv_n + e], vbuf.at[kv_n + e], v_recv.at[kv_n + e - kvh]).wait()

        qv, m, decay, mx, l8, o = [], [], [], [None] * 2, [], [None] * 2
        for e in range(2):
            qv.append(score_rhs(slot_n + e) if more else None)
            m_old = jnp.where(second == 1, st_m[slot + e], -1e38)
            m.append(jnp.maximum(m_old, jnp.max(mc[e][...], axis=0, keepdims=True) * scale2))
            decay.append(jnp.exp2(m_old - m[e]))
            l8.append(jnp.zeros((8, rows), F32))
        for c in range(chunks):
            sl = pl.ds(c * TK, TK)
            for e in range(2):
                st = qk_tile(kv_n + e, f_n, c, qv[e]) if more else None
                p = jnp.exp2(sc[e][sl, :] * scale2 - m[e])
                if more:
                    sn[e][sl, :] = st
                    mx[e] = fold_max(mx[e], st)
                l8[e] = l8[e] + jnp.sum(p.reshape(TK // 8, 8, rows), axis=0)
                t = jnp.dot(vbuf[kv + e, :, sl], p.astype(BF), preferred_element_type=F32)
                o[e] = t if o[e] is None else o[e] + t
        sl = pl.ds(cache, tok)
        for e in range(2):
            p = jnp.exp2(sc[e][sl, :] * scale2 - m[e])
            if more:
                st = qk_new(kv_n + e, owner_n, home_n, qv[e])
                sn[e][sl, :] = st
                mn[e][...] = fold_max(mx[e], st)
            l8[e] = l8[e] + jnp.sum(p.reshape(tok // 8, 8, rows), axis=0)
            pb = jnp.concatenate([p.astype(BF), jnp.zeros((dim - tok, rows), BF)], axis=0)
            o[e] = o[e] + jnp.dot(vbuf[kv + e, :, pl.ds(cache, dim)], pb, preferred_element_type=F32)
        for e in range(2):
            st_o[slot + e] = jnp.where(second == 1, st_o[slot + e] * decay[e], 0.0) + o[e]
            st_l[slot + e] = jnp.where(second == 1, st_l[slot + e] * decay[e], 0.0) + jnp.sum(l8[e], axis=0, keepdims=True)
            st_m[slot + e] = m[e]
            if more:
                load_q(ahead + e)

    def partial_copies(u):
        return (pltpu.make_async_remote_copy(
                    src_ref=ps.at[u], dst_ref=pr.at[u], send_sem=p_send.at[0, u], recv_sem=p_recv.at[0, u],
                    device_id={'cp': far}, device_id_type=MESH),
                pltpu.make_async_remote_copy(
                    src_ref=psl.at[u], dst_ref=prl.at[u], send_sem=p_send.at[1, u], recv_sem=p_recv.at[1, u],
                    device_id={'cp': far}, device_id_type=MESH))

    def mate_out(u):
        hh = half * core + u - half
        return (pltpu.make_async_remote_copy(
                    src_ref=fo.at[u - half], dst_ref=out_ref.at[:, hh], send_sem=f_send.at[0, u - half],
                    recv_sem=f_recv.at[0, u - half], device_id={'cp': mate}, device_id_type=MESH),
                pltpu.make_async_remote_copy(
                    src_ref=fl.at[u - half], dst_ref=lse_ref.at[hh], send_sem=f_send.at[1, u - half],
                    recv_sem=f_recv.at[1, u - half], device_id={'cp': mate}, device_id_type=MESH))

    def finish(i):
        _, slot, _, _, _ = pair(i)

        @pl.when(among(i, R_PAIRS))
        def _():
            u = slot - 2 * half
            for e in range(2):
                l = st_l[slot + e]
                ps[u + e] = (st_o[slot + e] * (1.0 / l)).astype(BF)
                psl[u + e] = st_m[slot + e] + jnp.log2(l)
            for e in range(2):
                for cp in partial_copies(u + e):
                    cp.start()

        @pl.when(among(i, L_PAIRS))
        def _():
            u = slot
            for e in range(2):
                for cp in partial_copies(u + e):
                    cp.wait_recv()
            done = []
            for e in range(2):
                m_a, m_b = st_m[u + e], prl[u + e]
                m = jnp.maximum(m_a, m_b)
                a, b = jnp.exp2(m_a - m), jnp.exp2(m_b - m)
                l = st_l[u + e] * a + b
                inv = 1.0 / l
                o = st_o[u + e] * (a * inv) + pr[u + e].astype(F32) * (b * inv)
                done.append((o.T.astype(BF).reshape(tok, ratio, dim), (m + jnp.log2(l)) * math.log(2.0)))

            @pl.when(u < half)
            def _():
                for e in range(2):
                    out_ref[:, half * core + u + e] = done[e][0]
                    lse_ref[half * core + u + e] = done[e][1]

            @pl.when(u >= half)
            def _():
                for e in range(2):
                    fo[u - half + e] = done[e][0]
                    fl[u - half + e] = done[e][1]
                for e in range(2):
                    for cp in mate_out(u + e):
                        cp.start()

    def two(i, more):
        region(2 * i, sbuf[:2], sbuf[2:], mbuf[:2], mbuf[2:])
        finish(2 * i)
        region(2 * i + 1, sbuf[2:], sbuf[:2], mbuf[2:], mbuf[:2], more)
        finish(2 * i + 1)

    @pl.loop(0, n_pairs // 2 - 1)
    def _(i):
        two(i, True)

    two(jnp.int32(n_pairs // 2 - 1), False)

    for k in range(3):
        for h in range(half):
            q_copy(k, h).wait_send()
    for h in range(half):
        pltpu.make_async_copy(kbuf.at[h], kbuf.at[h], kv_send.at[0, h]).wait()
        pltpu.make_async_copy(vbuf.at[h], vbuf.at[h], kv_send.at[1, h]).wait()
    for u in range(2 * half):
        for cp in partial_copies(u):
            cp.wait_send()
    for u in range(half):
        for cp in mate_out(u + half):
            cp.wait_send()
            cp.wait_recv()


def place_kernel(out_ref, lse_ref, out_hbm, lse_hbm, lse_buf, sem):
    kvh, _, rows = lse_ref.shape
    tok, heads = lse_buf.shape
    ratio = heads // kvh
    write = pltpu.make_async_copy(out_ref, out_hbm, sem.at[0])
    write.start()
    x = lse_ref[...].reshape(kvh, rows)
    lane = lax.broadcasted_iota(jnp.int32, (kvh, heads), 1) // ratio
    head = lax.broadcasted_iota(jnp.int32, (kvh, heads), 0)
    per = heads // ratio
    blocks = [pltpu.roll(x[:, b * heads:(b + 1) * heads], 0, 1, stride=ratio, stride_axis=0) for b in range(tok // per)]
    for t in range(tok):
        turned = pltpu.roll(blocks[t // per], (heads - (t % per) * ratio) % heads, 1)
        lse_buf[pl.ds(t, 1), :] = jnp.sum(jnp.where(lane == head, turned, 0.0), axis=0, keepdims=True)
    lse_write = pltpu.make_async_copy(lse_buf, lse_hbm, sem.at[1])
    lse_write.start()
    write.wait()
    lse_write.wait()


def solution(mesh):
    tok_spec = P(('dp', 'cp'))

    def local(queries, key_new, value_new, key_cache, value_cache, prefix_len):
        tok, heads, dim = queries.shape
        cache, kvh = key_cache.shape[:2]
        ratio = heads // kvh
        half = kvh // 2
        rows = tok * ratio
        n_raw = cache // TK
        dma = pltpu.SemaphoreType.DMA
        hbm = pl.BlockSpec(memory_space=pltpu.HBM)
        vmem = pl.BlockSpec(memory_space=pltpu.VMEM)
        scratch = [
            pltpu.VMEM((cache * kvh, dim), BF),
            pltpu.VMEM((cache * kvh, dim), BF),
            pltpu.VMEM((tok * kvh, dim), BF),
            pltpu.VMEM((tok * kvh, dim), BF),
            pltpu.VMEM((kvh + half, cache + tok, dim), BF),
            pltpu.VMEM((kvh + half, dim, cache + dim), BF),
            pltpu.VMEM((2, cache, dim), BF),
            pltpu.VMEM((4 * half, tok, ratio, dim), BF),
            pltpu.VMEM((4 * half, dim, rows), BF),
            pltpu.VMEM((dim, rows), BF),
            (pltpu.VMEM((cache + tok, rows), F32),) * 4,
            (pltpu.VMEM((8, rows), F32),) * 4,
            pltpu.VMEM((4 * half, dim, rows), F32),
            pltpu.VMEM((4 * half, 1, rows), F32),
            pltpu.VMEM((4 * half, 1, rows), F32),
            pltpu.VMEM((2 * half, dim, rows), BF),
            pltpu.VMEM((2 * half, 1, rows), F32),
            pltpu.VMEM((2 * half, dim, rows), BF),
            pltpu.VMEM((2 * half, 1, rows), F32),
            pltpu.VMEM((half, tok, ratio, dim), BF),
            pltpu.VMEM((half, 1, rows), F32),
            dma((2, n_raw)), dma((2,)), dma((3 * half,)), dma((4 * half,)), dma((2, half)), dma((half,)), dma((half,)),
            dma((2, 2 * half)), dma((2, 2 * half)), dma((2, half)), dma((2, half)),
        ]
        flops = 4 * heads * tok * 4 * cache * dim
        out, lse = pl.pallas_call(
            attend_kernel,
            out_shape=(pltpu.VMEM((tok, kvh, ratio, dim), BF), pltpu.VMEM((kvh, 1, rows), F32)),
            in_specs=[hbm] * 5 + [pl.BlockSpec(memory_space=pltpu.SMEM)],
            out_specs=(vmem, vmem),
            scratch_shapes=scratch,
            compiler_params=pltpu.CompilerParams(collective_id=0, has_side_effects=True, vmem_limit_bytes=60 * 2 ** 20),
            cost_estimate=pl.CostEstimate(flops=flops, bytes_accessed=4 * cache * kvh * dim, transcendentals=heads * tok * 4 * cache),
            name='attend',
        )(queries.reshape(tok, kvh, ratio, dim), key_new.reshape(tok * kvh, dim), value_new.reshape(tok * kvh, dim),
          key_cache.reshape(cache * kvh, dim), value_cache.reshape(cache * kvh, dim), prefix_len)
        out, row_lse = pl.pallas_call(
            place_kernel,
            out_shape=(jax.ShapeDtypeStruct((tok, heads, dim), BF), jax.ShapeDtypeStruct((tok, heads), F32)),
            in_specs=[vmem, vmem],
            out_specs=(hbm, hbm),
            scratch_shapes=[pltpu.VMEM((tok, heads), F32), dma((2,))],
            compiler_params=pltpu.CompilerParams(vmem_limit_bytes=2 * 2 ** 20),
            name='place',
        )(out.reshape(tok, heads, dim), lse)
        return out, row_lse

    return jax.shard_map(local, mesh=mesh, in_specs=(tok_spec, tok_spec, tok_spec, tok_spec, tok_spec, P('dp')),
                         out_specs=(tok_spec, tok_spec), check_vma=False)
```

```python
import functools
import math

import jax
import jax.numpy as jnp
from jax import lax
from jax.experimental import pallas as pl
from jax.experimental.pallas import tpu as pltpu
from jax.sharding import PartitionSpec as P

MESH = pl.DeviceIdType.MESH
BIG = 1e30
TK = 256
PREP = 128
RAW_DEPTH = 3
BF = jnp.bfloat16
SEQ = ((0, 0), (2, 0), (4, 0), (12, 0), (14, 0), (12, 1), (8, 0), (14, 1),
       (10, 0), (8, 1), (10, 1), (6, 0), (4, 1), (6, 1), (0, 1), (2, 1))
F32 = jnp.float32


def _packed(part):
    v = sum((slot // 2 + 8 * second) << (4 * k) for k, (slot, second) in enumerate(part))
    return v - (1 << 32) if v >= 1 << 31 else v


ORDER = (_packed(SEQ[:8]), _packed(SEQ[8:]))
Q_PAIRS = tuple(SEQ.index((s, 0)) for s in range(4, 16, 2))
KV_PAIRS = tuple(next(k for k, (s, f) in enumerate(SEQ) if f and s % 4 == h) for h in (0, 2))
R_PAIRS = tuple(k for k, (s, f) in enumerate(SEQ) if f and s >= 8)
L_PAIRS = tuple(k for k, (s, f) in enumerate(SEQ) if f and s < 8)


def among(i, ks):
    hit = i == ks[0]
    for k in ks[1:]:
        hit = jnp.logical_or(hit, i == k)
    return hit


def attend_kernel(q_hbm, kn_hbm, vn_hbm, kc_hbm, vc_hbm, plen_ref, out_ref, lse_ref,
                  raw_k, raw_v, new_k, new_v, kbuf, vbuf, bias, qraw, qt, pick, sbuf, mbuf,
                  st_o, st_m, st_l, ps, psl, pr, prl, fo, fl,
                  raw_sem, new_sem, q_send, q_recv, kv_send, k_recv, v_recv, p_send, p_recv, f_send, f_recv):
    tok, kvh, ratio, dim = q_hbm.shape
    cache = kc_hbm.shape[0] // kvh
    half = kvh // 2
    rows = tok * ratio
    n_raw = raw_sem.shape[1]
    raw_pos = cache // n_raw
    chunks = cache // TK
    scale2 = dim ** -0.5 * math.log2(math.e)

    me = lax.axis_index('cp')
    core = lax.rem(me, 2)
    chip2 = me - core
    mate = chip2 + 1 - core
    far = lax.rem(chip2 + 2, 4) + core
    far_other = lax.rem(chip2 + 2, 4) + 1 - core

    def raw_copy(j):
        sl = pl.ds(j * raw_pos * kvh, raw_pos * kvh)
        return (pltpu.make_async_copy(kc_hbm.at[sl], raw_k.at[sl], raw_sem.at[0, j]),
                pltpu.make_async_copy(vc_hbm.at[sl], raw_v.at[sl], raw_sem.at[1, j]))

    def own_q(h):
        return pltpu.make_async_copy(q_hbm.at[:, half * core + h], qraw.at[h], q_recv.at[h])

    def raw_start(j):
        for cp in raw_copy(j):
            cp.start()

    raw_start(0)
    new_copies = (pltpu.make_async_copy(kn_hbm, new_k, new_sem.at[0]),
                  pltpu.make_async_copy(vn_hbm, new_v, new_sem.at[1]))
    for cp in new_copies:
        cp.start()
    for h in range(half):
        own_q(h).start()

    barrier = pltpu.get_barrier_semaphore()
    for peer in (mate, far, far_other):
        pl.semaphore_signal(barrier, inc=1, device_id={'cp': peer}, device_id_type=MESH)

    pick[...] = jnp.where(lax.broadcasted_iota(jnp.int32, (dim, rows), 0) == 0, 1.0, 0.0).astype(BF)
    for e in range(2):
        mbuf[e][...] = jnp.full((8, rows), -3e38, F32)
    raw_start(1)

    def q_copy(k, h):
        peer, base = ((far_other, 3 * half), (far, 2 * half), (mate, half))[k]
        peer_core = (1 - core, core, 1 - core)[k]
        return pltpu.make_async_remote_copy(
            src_ref=q_hbm.at[:, half * peer_core + h], dst_ref=qraw.at[base + h],
            send_sem=q_send.at[k * half + h], recv_sem=q_recv.at[base + h],
            device_id={'cp': peer}, device_id_type=MESH)

    visible_len = plen_ref[0]
    for f, owner in enumerate((me, mate)):
        @pl.loop(0, chunks)
        def _(j):
            lane = lax.broadcasted_iota(jnp.int32, (TK, dim), 1)
            pos = owner * cache + j * TK + lax.broadcasted_iota(jnp.int32, (TK, dim), 0)
            hidden = jnp.logical_and(lane == 0, pos >= visible_len)
            bias[f, pl.ds(pl.multiple_of(j * TK, TK), TK), :] = jnp.where(hidden, -BIG, 0.0).astype(BF)

        if f == 0:
            raw_start(2)

    for cp in new_copies:
        cp.wait()
    kt = pltpu.einshape('phd->hpd', new_k[...].reshape(tok, kvh, dim))
    vt = pltpu.einshape('phd->hpd', new_v[...].reshape(tok, kvh, dim))
    for h in range(kvh):
        kbuf[h, pl.ds(cache, tok), :] = kt[h]
        vpad = jnp.concatenate([vt[h].astype(F32), jnp.zeros((dim - tok, dim), F32)], axis=0)
        vbuf[h, :, pl.ds(cache, dim)] = vpad.T.astype(BF)
    def kv_parts(h, lo, n):
        src = half * (1 - core) + h
        to = dict(device_id={'cp': mate}, device_id_type=MESH)
        k_rows, v_lanes = pl.ds(lo, tok if n == dim else n), pl.ds(lo, n)
        return (pltpu.make_async_remote_copy(
                    src_ref=kbuf.at[src, k_rows], dst_ref=kbuf.at[kvh + h, k_rows],
                    send_sem=kv_send.at[0, h], recv_sem=k_recv.at[h], **to),
                pltpu.make_async_remote_copy(
                    src_ref=vbuf.at[src, :, v_lanes], dst_ref=vbuf.at[kvh + h, :, v_lanes],
                    send_sem=kv_send.at[1, h], recv_sem=v_recv.at[h], **to))

    def kv_start(lo, n):
        for h in range(half):
            for cp in kv_parts(h, lo, n):
                cp.start()

    n_pairs = 4 * half

    def pair(i):
        code = lax.shift_right_logical(jnp.where(i < 8, ORDER[0], ORDER[1]), 4 * lax.rem(i, 8))
        slot = 2 * jnp.bitwise_and(code, 7)
        second = lax.div(jnp.bitwise_and(code, 15), 8)
        h = lax.rem(slot, half)
        kv = jnp.where(second == 1, kvh + h, half * core + h)
        owner = jnp.where(second == 1, mate, me)
        src = lax.div(slot, half)
        home = jnp.where(src == 0, me, jnp.where(src == 1, mate, jnp.where(src == 2, far, far_other)))
        return second, slot, kv, owner, home

    def load_q(slot):
        qt[slot] = qraw[slot].reshape(rows, dim).T

    def score_rhs(slot):
        return jnp.concatenate([qt[slot], pick[...]], axis=0)

    def qk_tile(kv, f, c, qv):
        sl = pl.ds(c * TK if isinstance(c, int) else pl.multiple_of(c * TK, TK), TK)
        lhs = jnp.concatenate([kbuf[kv, sl, :], bias[f, sl, :]], axis=1)
        return jnp.dot(lhs, qv, preferred_element_type=F32)

    def qk_new(kv, owner, home, qv):
        lhs = jnp.concatenate([kbuf[kv, pl.ds(cache, tok), :], jnp.zeros((tok, dim), BF)], axis=1)
        st = jnp.dot(lhs, qv, preferred_element_type=F32)
        key = owner * tok + lax.broadcasted_iota(jnp.int32, (tok, rows), 0)
        query = home * tok + lax.broadcasted_iota(jnp.int32, (tok, rows), 1) // ratio
        return jnp.where(key <= query, st, -BIG)

    def fold_max(mx, st):
        t = jnp.max(st.reshape(st.shape[0] // 8, 8, rows), axis=0)
        return t if mx is None else jnp.maximum(mx, t)

    f_0, slot_0, kv_0, owner_0, home_0 = pair(0)

    def first_scores(c):
        for e in range(2):
            st = qk_tile(kv_0 + e, f_0, c, score_rhs(slot_0 + e))
            sbuf[e][pl.ds(c * TK, TK), :] = st
            mbuf[e][...] = fold_max(mbuf[e][...], st)

    for j in range(n_raw):
        for cp in raw_copy(j):
            cp.wait()
        if j + RAW_DEPTH < n_raw:
            raw_start(j + RAW_DEPTH)

        @pl.loop(0, raw_pos // PREP)
        def _(i):
            base = pl.multiple_of(j * raw_pos + i * PREP, PREP)
            src = pl.ds(pl.multiple_of(base * kvh, PREP * kvh), PREP * kvh)
            xk = pltpu.einshape('phd->hpd', raw_k[src, :].reshape(PREP, kvh, dim))
            xv = pltpu.einshape('phd->hpd', raw_v[src, :].reshape(PREP, kvh, dim))
            for h in range(kvh):
                kbuf[h, pl.ds(base, PREP), :] = xk[h]
                vbuf[h, :, pl.ds(base, PREP)] = xv[h].T

        if j == 1:
            pl.semaphore_wait(barrier, 3)
            for k in range(3):
                for h in range(half):
                    q_copy(k, h).start()
            kv_start(cache, dim)
        if j % 2 and j > 1:
            kv_start((j - 3) * raw_pos, 2 * raw_pos)

    for h in range(half):
        own_q(h).wait()
    for h in range(half):
        load_q(h)
    for c in range(chunks):
        first_scores(c)
    for e in range(2):
        st = qk_new(kv_0 + e, owner_0, home_0, score_rhs(slot_0 + e))
        sbuf[e][pl.ds(cache, tok), :] = st
        mbuf[e][...] = fold_max(mbuf[e][...], st)
    kv_start(cache - 2 * raw_pos, 2 * raw_pos)

    def region(i, sc, sn, mc, mn, more=True):
        nxt = lax.rem(i + 1, n_pairs)
        f_n, slot_n, kv_n, owner_n, home_n = pair(nxt)
        second, slot, kv, _, _ = pair(i)
        later = jnp.minimum(i + 2, n_pairs - 1)
        ahead = pair(later)[1]

        @pl.when(among(i + 2, Q_PAIRS))
        def _():
            for e in range(2):
                pltpu.make_async_copy(qraw.at[ahead + e], qraw.at[ahead + e], q_recv.at[ahead + e]).wait()

        @pl.when(among(i + 1, KV_PAIRS))
        def _():
            for e in range(2):
                pltpu.make_async_copy(kbuf.at[kv_n + e], kbuf.at[kv_n + e], k_recv.at[kv_n + e - kvh]).wait()
                pltpu.make_async_copy(vbuf.at[kv_n + e], vbuf.at[kv_n + e], v_recv.at[kv_n + e - kvh]).wait()

        qv, m, decay, mx, l8, o = [], [], [], [None] * 2, [], [None] * 2
        for e in range(2):
            qv.append(score_rhs(slot_n + e) if more else None)
            m_old = jnp.where(second == 1, st_m[slot + e], -1e38)
            m.append(jnp.maximum(m_old, jnp.max(mc[e][...], axis=0, keepdims=True) * scale2))
            decay.append(jnp.exp2(m_old - m[e]))
            l8.append(jnp.zeros((8, rows), F32))
        for c in range(chunks):
            sl = pl.ds(c * TK, TK)
            for e in range(2):
                st = qk_tile(kv_n + e, f_n, c, qv[e]) if more else None
                p = jnp.exp2(sc[e][sl, :] * scale2 - m[e])
                if more:
                    sn[e][sl, :] = st
                    mx[e] = fold_max(mx[e], st)
                l8[e] = l8[e] + jnp.sum(p.reshape(TK // 8, 8, rows), axis=0)
                t = jnp.dot(vbuf[kv + e, :, sl], p.astype(BF), preferred_element_type=F32)
                o[e] = t if o[e] is None else o[e] + t
        sl = pl.ds(cache, tok)
        for e in range(2):
            p = jnp.exp2(sc[e][sl, :] * scale2 - m[e])
            if more:
                st = qk_new(kv_n + e, owner_n, home_n, qv[e])
                sn[e][sl, :] = st
                mn[e][...] = fold_max(mx[e], st)
            l8[e] = l8[e] + jnp.sum(p.reshape(tok // 8, 8, rows), axis=0)
            pb = jnp.concatenate([p.astype(BF), jnp.zeros((dim - tok, rows), BF)], axis=0)
            o[e] = o[e] + jnp.dot(vbuf[kv + e, :, pl.ds(cache, dim)], pb, preferred_element_type=F32)
        for e in range(2):
            st_o[slot + e] = jnp.where(second == 1, st_o[slot + e] * decay[e], 0.0) + o[e]
            st_l[slot + e] = jnp.where(second == 1, st_l[slot + e] * decay[e], 0.0) + jnp.sum(l8[e], axis=0, keepdims=True)
            st_m[slot + e] = m[e]
            if more:
                load_q(ahead + e)

    def partial_copies(u):
        return (pltpu.make_async_remote_copy(
                    src_ref=ps.at[u], dst_ref=pr.at[u], send_sem=p_send.at[0, u], recv_sem=p_recv.at[0, u],
                    device_id={'cp': far}, device_id_type=MESH),
                pltpu.make_async_remote_copy(
                    src_ref=psl.at[u], dst_ref=prl.at[u], send_sem=p_send.at[1, u], recv_sem=p_recv.at[1, u],
                    device_id={'cp': far}, device_id_type=MESH))

    def mate_out(u):
        hh = half * core + u - half
        return (pltpu.make_async_remote_copy(
                    src_ref=fo.at[u - half], dst_ref=out_ref.at[:, hh], send_sem=f_send.at[0, u - half],
                    recv_sem=f_recv.at[0, u - half], device_id={'cp': mate}, device_id_type=MESH),
                pltpu.make_async_remote_copy(
                    src_ref=fl.at[u - half], dst_ref=lse_ref.at[hh], send_sem=f_send.at[1, u - half],
                    recv_sem=f_recv.at[1, u - half], device_id={'cp': mate}, device_id_type=MESH))

    def finish(i):
        _, slot, _, _, _ = pair(i)

        @pl.when(among(i, R_PAIRS))
        def _():
            u = slot - 2 * half
            for e in range(2):
                l = st_l[slot + e]
                ps[u + e] = (st_o[slot + e] * (1.0 / l)).astype(BF)
                psl[u + e] = st_m[slot + e] + jnp.log2(l)
            for e in range(2):
                for cp in partial_copies(u + e):
                    cp.start()

        @pl.when(among(i, L_PAIRS))
        def _():
            u = slot
            for e in range(2):
                for cp in partial_copies(u + e):
                    cp.wait_recv()
            done = []
            for e in range(2):
                m_a, m_b = st_m[u + e], prl[u + e]
                m = jnp.maximum(m_a, m_b)
                a, b = jnp.exp2(m_a - m), jnp.exp2(m_b - m)
                l = st_l[u + e] * a + b
                inv = 1.0 / l
                o = st_o[u + e] * (a * inv) + pr[u + e].astype(F32) * (b * inv)
                done.append((o.T.astype(BF).reshape(tok, ratio, dim), (m + jnp.log2(l)) * math.log(2.0)))

            @pl.when(u < half)
            def _():
                for e in range(2):
                    out_ref[:, half * core + u + e] = done[e][0]
                    lse_ref[half * core + u + e] = done[e][1]

            @pl.when(u >= half)
            def _():
                for e in range(2):
                    fo[u - half + e] = done[e][0]
                    fl[u - half + e] = done[e][1]
                for e in range(2):
                    for cp in mate_out(u + e):
                        cp.start()

    def two(i, more):
        region(2 * i, sbuf[:2], sbuf[2:], mbuf[:2], mbuf[2:])
        finish(2 * i)
        region(2 * i + 1, sbuf[2:], sbuf[:2], mbuf[2:], mbuf[:2], more)
        finish(2 * i + 1)

    @pl.loop(0, n_pairs // 2 - 1)
    def _(i):
        two(i, True)

    two(jnp.int32(n_pairs // 2 - 1), False)

    for k in range(3):
        for h in range(half):
            q_copy(k, h).wait_send()
    for h in range(half):
        pltpu.make_async_copy(kbuf.at[h], kbuf.at[h], kv_send.at[0, h]).wait()
        pltpu.make_async_copy(vbuf.at[h], vbuf.at[h], kv_send.at[1, h]).wait()
    for u in range(2 * half):
        for cp in partial_copies(u):
            cp.wait_send()
    for u in range(half):
        for cp in mate_out(u + half):
            cp.wait_send()
            cp.wait_recv()


def place_kernel(out_ref, lse_ref, out_hbm, lse_hbm, lse_buf, sem):
    kvh, _, rows = lse_ref.shape
    tok, heads = lse_buf.shape
    ratio = heads // kvh
    write = pltpu.make_async_copy(out_ref, out_hbm, sem.at[0])
    write.start()
    x = lse_ref[...].reshape(kvh, rows)
    lane = lax.broadcasted_iota(jnp.int32, (kvh, heads), 1) // ratio
    head = lax.broadcasted_iota(jnp.int32, (kvh, heads), 0)
    per = heads // ratio
    blocks = [pltpu.roll(x[:, b * heads:(b + 1) * heads], 0, 1, stride=ratio, stride_axis=0) for b in range(tok // per)]
    for t in range(tok):
        turned = pltpu.roll(blocks[t // per], (heads - (t % per) * ratio) % heads, 1)
        lse_buf[pl.ds(t, 1), :] = jnp.sum(jnp.where(lane == head, turned, 0.0), axis=0, keepdims=True)
    lse_write = pltpu.make_async_copy(lse_buf, lse_hbm, sem.at[1])
    lse_write.start()
    write.wait()
    lse_write.wait()


def solution(mesh):
    tok_spec = P(('dp', 'cp'))

    def local(queries, key_new, value_new, key_cache, value_cache, prefix_len):
        tok, heads, dim = queries.shape
        cache, kvh = key_cache.shape[:2]
        ratio = heads // kvh
        half = kvh // 2
        rows = tok * ratio
        n_raw = cache // TK
        dma = pltpu.SemaphoreType.DMA
        hbm = pl.BlockSpec(memory_space=pltpu.HBM)
        vmem = pl.BlockSpec(memory_space=pltpu.VMEM)
        scratch = [
            pltpu.VMEM((cache * kvh, dim), BF),
            pltpu.VMEM((cache * kvh, dim), BF),
            pltpu.VMEM((tok * kvh, dim), BF),
            pltpu.VMEM((tok * kvh, dim), BF),
            pltpu.VMEM((kvh + half, cache + tok, dim), BF),
            pltpu.VMEM((kvh + half, dim, cache + dim), BF),
            pltpu.VMEM((2, cache, dim), BF),
            pltpu.VMEM((4 * half, tok, ratio, dim), BF),
            pltpu.VMEM((4 * half, dim, rows), BF),
            pltpu.VMEM((dim, rows), BF),
            (pltpu.VMEM((cache + tok, rows), F32),) * 4,
            (pltpu.VMEM((8, rows), F32),) * 4,
            pltpu.VMEM((4 * half, dim, rows), F32),
            pltpu.VMEM((4 * half, 1, rows), F32),
            pltpu.VMEM((4 * half, 1, rows), F32),
            pltpu.VMEM((2 * half, dim, rows), BF),
            pltpu.VMEM((2 * half, 1, rows), F32),
            pltpu.VMEM((2 * half, dim, rows), BF),
            pltpu.VMEM((2 * half, 1, rows), F32),
            pltpu.VMEM((half, tok, ratio, dim), BF),
            pltpu.VMEM((half, 1, rows), F32),
            dma((2, n_raw)), dma((2,)), dma((3 * half,)), dma((4 * half,)), dma((2, half)), dma((half,)), dma((half,)),
            dma((2, 2 * half)), dma((2, 2 * half)), dma((2, half)), dma((2, half)),
        ]
        flops = 4 * heads * tok * 4 * cache * dim
        out, lse = pl.pallas_call(
            attend_kernel,
            out_shape=(pltpu.VMEM((tok, kvh, ratio, dim), BF), pltpu.VMEM((kvh, 1, rows), F32)),
            in_specs=[hbm] * 5 + [pl.BlockSpec(memory_space=pltpu.SMEM)],
            out_specs=(vmem, vmem),
            scratch_shapes=scratch,
            compiler_params=pltpu.CompilerParams(collective_id=0, has_side_effects=True, vmem_limit_bytes=60 * 2 ** 20),
            cost_estimate=pl.CostEstimate(flops=flops, bytes_accessed=4 * cache * kvh * dim, transcendentals=heads * tok * 4 * cache),
            name='attend',
        )(queries.reshape(tok, kvh, ratio, dim), key_new.reshape(tok * kvh, dim), value_new.reshape(tok * kvh, dim),
          key_cache.reshape(cache * kvh, dim), value_cache.reshape(cache * kvh, dim), prefix_len)
        out, row_lse = pl.pallas_call(
            place_kernel,
            out_shape=(jax.ShapeDtypeStruct((tok, heads, dim), BF), jax.ShapeDtypeStruct((tok, heads), F32)),
            in_specs=[vmem, vmem],
            out_specs=(hbm, hbm),
            scratch_shapes=[pltpu.VMEM((tok, heads), F32), dma((2,))],
            compiler_params=pltpu.CompilerParams(vmem_limit_bytes=2 * 2 ** 20),
            name='place',
        )(out.reshape(tok, heads, dim), lse)
        return out, row_lse

    return jax.shard_map(local, mesh=mesh, in_specs=(tok_spec, tok_spec, tok_spec, tok_spec, tok_spec, P('dp')),
                         out_specs=(tok_spec, tok_spec), check_vma=False)
```
